128 devices in a mesh: lat: 2 (over x_lo), lon: 8 (over z_lo, x_hi, core), lev: 8 (over z_hi, y).
Axes of the slice: x: 4 (x_hi: 2, x_lo: 2; x = x_hi * 2 + x_lo), y: 4, z: 4 (z_hi: 2, z_lo: 2; z = z_hi * 2 + z_lo), core: 2. Of those that a mesh axis runs over, the one named last changes fastest.
Arguments:
- initial_state: float32 [16, 256, 512, 128], P('lat', 'lon', 'lev'), may hold values from 0.2 to 1.8
- scaled_diffusivity: float32 [16, 256, 512, 128], P('lat', 'lon', 'lev'), may hold values from 0.03 to 0.15
- scaled_forcing: float32 [16, 256, 512, 128], P('lat', 'lon', 'lev'), may hold values from -0.2 to 0.2
Outputs:
- cumulative_totals: float32 [16, 256, 512, 128], P('lat', 'lon', 'lev')
- temperature_end: float32 [16, 256, 512, 128], P('lat', 'lon', 'lev')
The draws below stay inside these ranges and needn't reach their ends.
All inputs are finite; a program needn't handle non-finite values.
Results may differ from the reference program's by a relative error of at most 0.00002.
Values sent between devices are 32-bit elements; how exact they have to be, the bound alone decides.
No kernel may reach another device: no remote copies, remote signals or barrier semaphores. Data moves between devices by JAX's collectives and lax.ppermute only.
A program may use at most 128 MiB of HBM per device.

```python
import jax
import jax.numpy as jnp
from jax import lax

SECOND_EXTENT = 16
FIRST_EXTENT = 256
THIRD_EXTENT = 512
MEMBER_TALLY = 128
STEPS = 4


def level_of(rng, extent, cuts, smallest, top_value):
    def one(axis_at, shards_of):
        draws = jax.random.uniform(jax.random.fold_in(jax.random.fold_in(rng, 6), axis_at), (shards_of,), jnp.float32, smallest / len(cuts), top_value / len(cuts))
        return jnp.repeat(jnp.exp(draws), extent[axis_at] // shards_of).reshape((-1,) + (1,) * (len(extent) - axis_at - 1))

    level = one(*cuts[0])
    for cut in cuts[1:]:
        level = level * one(*cut)
    return level


def setup_inputs(seed: int = 0) -> dict:
    seeds = jax.random.split(jax.random.key(seed), 4)
    initial_state = jnp.clip(0.2 + 1.5999999 * jax.random.uniform(seeds[0], (SECOND_EXTENT, FIRST_EXTENT, THIRD_EXTENT, MEMBER_TALLY), jnp.float32) ** level_of(seeds[0], (SECOND_EXTENT, FIRST_EXTENT, THIRD_EXTENT, MEMBER_TALLY), ((0, 2), (1, 8), (2, 8)), -0.2, 0.2), 0.2, 1.8)
    scaled_diffusivity = jnp.clip(0.03 + 0.120000007 * jax.random.uniform(seeds[1], (SECOND_EXTENT, FIRST_EXTENT, THIRD_EXTENT, MEMBER_TALLY), jnp.float32) ** level_of(seeds[1], (SECOND_EXTENT, FIRST_EXTENT, THIRD_EXTENT, MEMBER_TALLY), ((0, 2), (1, 8), (2, 8)), -0.2, 0.2), 0.03, 0.15)
    scaled_forcing = jnp.clip(jax.random.uniform(seeds[2], (SECOND_EXTENT, FIRST_EXTENT, THIRD_EXTENT, MEMBER_TALLY), jnp.float32, -0.2, 0.2) * level_of(seeds[2], (SECOND_EXTENT, FIRST_EXTENT, THIRD_EXTENT, MEMBER_TALLY), ((0, 2), (1, 8), (2, 8)), -0.4, 0.0), -0.2, 0.2)
    return dict(initial_state=initial_state, scaled_diffusivity=scaled_diffusivity, scaled_forcing=scaled_forcing)


def strip_edges(values, dims):
    for dim in dims:
        values = lax.slice_in_dim(values, 1, values.shape[dim] - 1, axis=dim)
    return values


def neighbour(values, dim, start, dims):
    others = [other for other in dims if other != dim]
    values = strip_edges(values, others)
    return lax.slice_in_dim(values, start, start + values.shape[dim] - 2, axis=dim)


def explicit_update(haloed_values, scaled_diffusivity, scaled_forcing):
    middle = strip_edges(haloed_values, (0, 1, 2))
    lower = [neighbour(haloed_values, dim, 0, (0, 1, 2)) for dim in (0, 1, 2)]
    upper = [neighbour(haloed_values, dim, 2, (0, 1, 2)) for dim in (0, 1, 2)]
    spread = lower[0] + upper[0] + lower[1] + upper[1] + lower[2] + upper[2] - 6.0 * middle
    return middle + scaled_diffusivity * spread + scaled_forcing


def reference(initial_state, scaled_diffusivity, scaled_forcing):
    for step in range(STEPS):
        initial_state = explicit_update(jnp.pad(initial_state, ((1, 1), (1, 1), (1, 1), (0, 0)), mode="constant"), scaled_diffusivity, scaled_forcing)
    cumulative_totals = jnp.cumsum(initial_state, axis=1) / FIRST_EXTENT
    return cumulative_totals, initial_state
```

```python
import functools

import jax
import jax.numpy as jnp
from jax import lax
from jax.experimental import pallas as pl
from jax.experimental.pallas import tpu as pltpu
from jax.sharding import PartitionSpec as P


STEPS = 4
BLOCK = 4
VMEM = pl.BlockSpec(memory_space=pltpu.VMEM)
HBM = pl.BlockSpec(memory_space=pltpu.HBM)
ANY = pl.BlockSpec(memory_space=pl.ANY)


def in_vmem(x):
    return pltpu.with_memory_space_constraint(x, pltpu.VMEM)


def in_hbm(x):
    return pltpu.with_memory_space_constraint(x, pltpu.HBM)


def new_rows(c, im, ip, nb, klo, khi, d, f):
    km = jnp.concatenate([klo, c[:-1]], axis=0)
    kp = jnp.concatenate([c[1:], khi], axis=0)
    spread = (im + ip) + nb + (km + kp) - 6.0 * c
    return c + d * spread + f


def sweep(lo, hi, row, below, above, nb, klo, khi, d, f, put, carry=None):
    def block(first, bottom, top, carry):
        rows = [bottom() if bottom else row(first - 1)]
        rows += [row(first + r) for r in range(BLOCK)]
        rows += [top() if top else row(first + BLOCK)]
        for r in range(BLOCK):
            i = first + r
            new = new_rows(rows[r + 1], rows[r], rows[r + 2], nb(i), klo(i), khi(i), d(i), f(i))
            carry = put(i, new, carry)
        return carry

    carry = block(lo, below, None, carry)

    def body(b, carry):
        return block(lo + b * BLOCK, None, None, carry)

    n = (hi - lo) // BLOCK
    carry = lax.fori_loop(1, n - 1, body, carry)
    return block(hi - BLOCK, None, above, carry)


def plane_at(depth, n):
    low = lax.axis_index("lat") == 0
    return jnp.where(low, n - 1 - depth, depth)


def faces_kernel(u, lon_lo, lon_hi, lev_lo, lev_hi):
    nj, ni, nk, _ = u.shape
    for j in range(nj):
        lon_lo[j] = u[j, 0]
        lon_hi[j] = u[j, ni - 1]
        lev_lo[j] = u[j, :, 0, :]
        lev_hi[j] = u[j, :, nk - 1, :]


def load_kernel(u_in, d_in, f_in, u, d_edge, f_edge, lon_lo, lon_hi, lev_lo, lev_hi, sem):
    nj = u.shape[0]
    pj = plane_at(0, nj)
    copies = [pltpu.make_async_copy(u_in.at[j], u.at[j], sem.at[j]) for j in range(nj)]
    copies += [
        pltpu.make_async_copy(d_in.at[pj], d_edge, sem.at[nj]),
        pltpu.make_async_copy(f_in.at[pj], f_edge, sem.at[nj + 1]),
    ]
    for copy in copies:
        copy.start()
    for copy in copies:
        copy.wait()
    faces_kernel(u, lon_lo, lon_hi, lev_lo, lev_hi)


def edge_kernel(part, u, pa, pb, lat, lon_lo, lon_hi, lev_lo, lev_hi, d, f, *rest):
    nj, ni, nk, _ = u.shape
    half = ni // 2
    pj, pn = plane_at(0, nj), plane_at(1, nj)
    mine = (pa, pb)[part]
    base = part * half
    if part == 0:
        (out,) = rest
        below = lambda: lon_lo[pj]
        above = lambda: pb[0]
    else:
        nu, npa, out, s_lon_lo, s_lon_hi, s_lev_lo, s_lev_hi = rest
        below = lambda: pa[half - 1]
        above = lambda: lon_hi[pj]

    def put(i, new, carry):
        out[i] = new
        return carry

    sweep(
        0,
        half,
        lambda i: mine[i],
        below,
        above,
        lambda i: u[pn, base + i] + lat[i],
        lambda i: lev_lo[pj, pl.ds(base + i, 1), :],
        lambda i: lev_hi[pj, pl.ds(base + i, 1), :],
        lambda i: d[base + i],
        lambda i: f[base + i],
        put,
        jnp.int32(0),
    )
    if part == 1:
        faces_kernel(nu, s_lon_lo, s_lon_hi, s_lev_lo, s_lev_hi)
        s_lon_lo[pj] = npa[0]
        s_lon_hi[pj] = out[half - 1]
        s_lev_lo[pj, :half] = npa[:, 0, :]
        s_lev_lo[pj, half:] = out[:, 0, :]
        s_lev_hi[pj, :half] = npa[:, nk - 1, :]
        s_lev_hi[pj, half:] = out[:, nk - 1, :]


def bulk_planes(u, pa, pb, lon_lo, lon_hi, lev_lo, lev_hi, d, f, put, start, finish):
    nj, ni, _, _ = u.shape
    half = ni // 2

    def run(j, lo, hi, nb, carry):
        return sweep(
            lo,
            hi,
            lambda i: u[j, i],
            (lambda: lon_lo[j]) if lo == 0 else None,
            (lambda: lon_hi[j]) if hi == ni else None,
            nb,
            lambda i: lev_lo[j, pl.ds(i, 1), :],
            lambda i: lev_hi[j, pl.ds(i, 1), :],
            lambda i: d[j, i],
            lambda i: f[j, i],
            functools.partial(put, j),
            carry,
        )

    j, inner = plane_at(1, nj), plane_at(2, nj)
    start(j, 1)
    carry = run(j, 0, half, lambda i: u[inner, i] + pa[i], zero_carry(u))
    carry = run(j, half, ni, lambda i: u[inner, i] + pb[i - half], carry)
    finish(j, 1, carry)

    def body(depth, _):
        j, outer, inner = plane_at(depth, nj), plane_at(depth - 1, nj), plane_at(depth + 1, nj)
        start(j, depth)
        carry = run(j, 0, ni, lambda i: u[outer, i] + u[inner, i], zero_carry(u))
        finish(j, depth, carry)
        return 0

    lax.fori_loop(2, nj - 1, body, 0)
    j, outer = plane_at(nj - 1, nj), plane_at(nj - 2, nj)
    start(j, nj - 1)
    carry = run(j, 0, ni, lambda i: u[outer, i], zero_carry(u))
    finish(j, nj - 1, carry)


def zero_carry(u):
    return jnp.zeros(u.shape[2:], u.dtype)


def nothing(*_):
    pass


def plain_put(out):
    def put(j, i, new, carry):
        out[j, i] = new
        return carry

    return put


def first_bulk_kernel(u, pa, pb, lon_lo, lon_hi, lev_lo, lev_hi, d_in, f_in, after, out, d, f, sem):
    del after
    nj = u.shape[0]

    def copies(j, depth):
        return (
            pltpu.make_async_copy(d_in.at[j], d.at[j], sem.at[0, depth]),
            pltpu.make_async_copy(f_in.at[j], f.at[j], sem.at[1, depth]),
        )

    for depth in range(1, nj):
        for copy in copies(plane_at(depth, nj), depth):
            copy.start()

    def start(j, depth):
        for copy in copies(j, depth):
            copy.wait()

    bulk_planes(u, pa, pb, lon_lo, lon_hi, lev_lo, lev_hi, d, f, plain_put(out), start, nothing)


def bulk_kernel(u, pa, pb, lon_lo, lon_hi, lev_lo, lev_hi, d, f, after, out):
    del after
    bulk_planes(u, pa, pb, lon_lo, lon_hi, lev_lo, lev_hi, d, f, plain_put(out), nothing, nothing)


def last_bulk_kernel(u, pa, pb, lon_lo, lon_hi, lev_lo, lev_hi, d_in, f_in, end, d, f, total, sem):
    del d_in, f_in
    nj = u.shape[0]

    def copy_out(j, depth):
        return pltpu.make_async_copy(f.at[j], end.at[j], sem.at[depth])

    def put(j, i, new, carry):
        f[j, i] = new
        carry = carry + new
        d[j, i] = carry
        return carry

    def finish(j, depth, carry):
        total[j] = carry
        copy_out(j, depth).start()

    bulk_planes(u, pa, pb, lon_lo, lon_hi, lev_lo, lev_hi, d, f, put, nothing, finish)
    pj = plane_at(0, nj)
    total[pj] = jnp.zeros(total.shape[1:], total.dtype)
    for depth in range(1, nj):
        copy_out(plane_at(depth, nj), depth).wait()


def last_edge_kernel(u, pa, pb, lata, latb, lon_lo, lon_hi, lev_lo, lev_hi, d, f, end_in, end, sums, total, stage, sem):
    del end_in
    nj, ni, nk, nm = u.shape
    half = ni // 2
    pj, pn = plane_at(0, nj), plane_at(1, nj)
    carry = jnp.zeros((nk, nm), u.dtype)
    for part in (0, 1):
        mine, lat, base = (pa, pb)[part], (lata, latb)[part], part * half

        def put(i, new, carry):
            stage[base + i] = new
            carry = carry + new
            sums[base + i] = carry
            return carry

        carry = sweep(
            0,
            half,
            lambda i: mine[i],
            (lambda: lon_lo[pj]) if part == 0 else (lambda: pa[half - 1]),
            (lambda: pb[0]) if part == 0 else (lambda: lon_hi[pj]),
            lambda i: u[pn, base + i] + lat[i],
            lambda i: lev_lo[pj, pl.ds(base + i, 1), :],
            lambda i: lev_hi[pj, pl.ds(base + i, 1), :],
            lambda i: d[base + i],
            lambda i: f[base + i],
            put,
            carry,
        )
    total[...] = carry
    copy = pltpu.make_async_copy(stage, end.at[pj], sem)
    copy.start()
    copy.wait()


def earlier(others):
    lon = lax.axis_index("lon")
    before = 0.0
    for bit, other in enumerate(others):
        before += jnp.where(lon & (1 << bit) != 0, other, 0.0)
    return before


def totals_kernel(scale, sums, *rest):
    *others, out, stage, sem = rest
    nj, ni = sums.shape[:2]

    def copy_out(j, depth):
        slot = depth % 2
        return pltpu.make_async_copy(stage.at[slot], out.at[j], sem.at[slot])

    def body(depth, _):
        j, slot = plane_at(depth, nj), depth % 2

        @pl.when(depth > 2)
        def _():
            copy_out(j, depth).wait()

        b = earlier([other[j] for other in others])

        def row(r, _):
            for q in range(BLOCK):
                i = r * BLOCK + q
                stage[slot, i] = (sums[j, i] + b) * scale
            return 0

        lax.fori_loop(0, ni // BLOCK, row, 0)
        copy_out(j, depth).start()
        return 0

    lax.fori_loop(1, nj, body, 0)
    copy_out(0, 0).wait()
    copy_out(0, 1).wait()


def last_totals_kernel(scale, sums, *rest):
    *others, _, out, stage, sem = rest
    ni = sums.shape[0]
    nj = out.shape[0]
    b = earlier([other[...] for other in others])

    def row(r, _):
        for q in range(BLOCK):
            i = r * BLOCK + q
            stage[i] = (sums[i] + b) * scale
        return 0

    lax.fori_loop(0, ni // BLOCK, row, 0)
    copy = pltpu.make_async_copy(stage, out.at[plane_at(0, nj)], sem)
    copy.start()
    copy.wait()


def call(kernel, out_shape, out_specs, in_specs, limit=2, scratch=(), aliases=None, flops=0):
    return pl.pallas_call(
        kernel,
        out_shape=out_shape,
        in_specs=in_specs,
        out_specs=out_specs,
        scratch_shapes=scratch,
        input_output_aliases=aliases or {},
        compiler_params=pltpu.CompilerParams(vmem_limit_bytes=limit * 2**20),
        cost_estimate=pl.CostEstimate(flops=flops, transcendentals=0, bytes_accessed=0),
    )


def per_device(lon_size, lev_size, initial_state, scaled_diffusivity, scaled_forcing):
    dtype = initial_state.dtype
    nj, ni, nk, nm = initial_state.shape
    half = ni // 2
    V = lambda *shape: pltpu.VMEM(shape, dtype)
    H = lambda *shape: pltpu.HBM(shape, dtype)

    swap = [(0, 1), (1, 0)]
    lon_up = [(i, i + 1) for i in range(lon_size - 1)]
    lev_up = [(i, i + 1) for i in range(lev_size - 1)]
    down = lambda pairs: [(b, a) for a, b in pairs]

    faces_out = (V(nj, nk, nm), V(nj, nk, nm), V(nj, ni, nm), V(nj, ni, nm))

    def exchange(faces):
        lon_lo, lon_hi, lev_lo, lev_hi = faces
        return (
            lax.ppermute(lon_hi, "lon", lon_up),
            lax.ppermute(lon_lo, "lon", down(lon_up)),
            lax.ppermute(lev_hi, "lev", lev_up),
            lax.ppermute(lev_lo, "lev", down(lev_up)),
        )

    pj = jnp.where(lax.axis_index("lat") == 0, nj - 1, 0)
    pa = lax.dynamic_slice(initial_state, (pj, 0, 0, 0), (1, half, nk, nm))[0]
    pb = lax.dynamic_slice(initial_state, (pj, half, 0, 0), (1, half, nk, nm))[0]
    lat_a = lax.ppermute(pa, "lat", swap)
    lat_b = lax.ppermute(pb, "lat", swap)

    u, d_edge, f_edge, *faces = call(
        load_kernel,
        (V(nj, ni, nk, nm), V(ni, nk, nm), V(ni, nk, nm)) + faces_out,
        (VMEM,) * 7,
        (HBM,) * 3,
        scratch=(pltpu.SemaphoreType.DMA((nj + 2,)),),
        flops=10**6,
    )(*map(in_hbm, (initial_state, scaled_diffusivity, scaled_forcing)))
    halo = exchange(faces)
    d_edge, f_edge = in_vmem(d_edge), in_vmem(f_edge)
    d, f = in_hbm(scaled_diffusivity), in_hbm(scaled_forcing)

    for step in range(STEPS - 1):
        halo = tuple(map(in_vmem, halo))
        u, pa, pb = map(in_vmem, (u, pa, pb))
        n_pa = call(
            functools.partial(edge_kernel, 0), V(half, nk, nm), VMEM, (VMEM,) * 10, flops=10**6
        )(u, pa, pb, in_vmem(lat_a), *halo, d_edge, f_edge)
        n_lat_a = lax.ppermute(n_pa, "lat", swap)
        if step == 0:
            n_u, d, f = call(
                first_bulk_kernel,
                (V(nj, ni, nk, nm),) * 3,
                (VMEM,) * 3,
                (VMEM,) * 7 + (HBM,) * 2 + (ANY,),
                scratch=(pltpu.SemaphoreType.DMA((2, nj)),),
                flops=2 * 10**7,
            )(u, pa, pb, *halo, d, f, n_pa)
        else:
            n_u = call(
                bulk_kernel, V(nj, ni, nk, nm), VMEM, (VMEM,) * 9 + (ANY,), flops=2 * 10**7
            )(u, pa, pb, *halo, in_vmem(d), in_vmem(f), n_pa)
        n_pb, *faces = call(
            functools.partial(edge_kernel, 1),
            (V(half, nk, nm),) + faces_out,
            (VMEM,) * 5,
            (VMEM,) * 12,
            flops=10**6,
        )(u, pa, pb, in_vmem(lat_b), *halo, d_edge, f_edge, in_vmem(n_u), in_vmem(n_pa))
        lat_b = lax.ppermute(n_pb, "lat", swap)
        halo = exchange(faces)
        u, pa, pb, lat_a = n_u, n_pa, n_pb, n_lat_a

    halo = tuple(map(in_vmem, halo))
    u, pa, pb = map(in_vmem, (u, pa, pb))
    end, sums, _, total = call(
        last_bulk_kernel,
        (H(nj, ni, nk, nm), V(nj, ni, nk, nm), V(nj, ni, nk, nm), V(nj, nk, nm)),
        (HBM, VMEM, VMEM, VMEM),
        (VMEM,) * 9,
        scratch=(pltpu.SemaphoreType.DMA((nj,)),),
        aliases={7: 1, 8: 2},
        flops=2 * 10**7,
    )(u, pa, pb, *halo, in_vmem(d), in_vmem(f))

    def partners(total):
        others = []
        for bit in range(lon_size.bit_length() - 1):
            pairs = [(i, i ^ (1 << bit)) for i in range(lon_size)]
            if others:
                total = total + others[-1]
            if 2 << bit == lon_size:
                pairs = [(a, b) for a, b in pairs if a < b]
            others.append(lax.ppermute(total, "lon", pairs))
        return tuple(map(in_vmem, others))

    scale = 1.0 / (ni * lon_size)
    out = call(
        functools.partial(totals_kernel, scale),
        H(nj, ni, nk, nm),
        HBM,
        (VMEM,) * lon_size.bit_length(),
        limit=4,
        scratch=(V(2, ni, nk, nm), pltpu.SemaphoreType.DMA((2,))),
        flops=10**6,
    )(in_vmem(sums), *partners(total))

    end, edge_sums, edge_total = call(
        last_edge_kernel,
        (H(nj, ni, nk, nm), V(ni, nk, nm), V(nk, nm)),
        (HBM, VMEM, VMEM),
        (VMEM,) * 11 + (HBM,),
        limit=4,
        scratch=(V(ni, nk, nm), pltpu.SemaphoreType.DMA),
        aliases={11: 0},
        flops=2 * 10**6,
    )(u, pa, pb, in_vmem(lat_a), in_vmem(lat_b), *halo, d_edge, f_edge, in_hbm(end))
    out = call(
        functools.partial(last_totals_kernel, scale),
        H(nj, ni, nk, nm),
        HBM,
        (VMEM,) * lon_size.bit_length() + (HBM,),
        limit=4,
        scratch=(V(ni, nk, nm), pltpu.SemaphoreType.DMA),
        aliases={lon_size.bit_length(): 0},
        flops=10**6,
    )(in_vmem(edge_sums), *partners(edge_total), in_hbm(out))
    return out, end


def solution(mesh):
    spec = P("lat", "lon", "lev", None)
    return jax.shard_map(
        functools.partial(per_device, mesh.shape["lon"], mesh.shape["lev"]),
        mesh=mesh,
        in_specs=(spec, spec, spec),
        out_specs=(spec, spec),
        check_vma=False,
    )
```

```python
import functools

import jax
import jax.numpy as jnp
from jax import lax
from jax.experimental import pallas as pl
from jax.experimental.pallas import tpu as pltpu
from jax.sharding import PartitionSpec as P


STEPS = 4
BLOCK = 4
VMEM = pl.BlockSpec(memory_space=pltpu.VMEM)
HBM = pl.BlockSpec(memory_space=pltpu.HBM)
ANY = pl.BlockSpec(memory_space=pl.ANY)


def in_vmem(x):
    return pltpu.with_memory_space_constraint(x, pltpu.VMEM)


def in_hbm(x):
    return pltpu.with_memory_space_constraint(x, pltpu.HBM)


def new_rows(c, im, ip, nb, klo, khi, d, f):
    km = jnp.concatenate([klo, c[:-1]], axis=0)
    kp = jnp.concatenate([c[1:], khi], axis=0)
    spread = (im + ip) + nb + (km + kp) - 6.0 * c
    return c + d * spread + f


def sweep(lo, hi, row, below, above, nb, klo, khi, d, f, put, carry=None):
    def block(first, bottom, top, carry):
        rows = [bottom() if bottom else row(first - 1)]
        rows += [row(first + r) for r in range(BLOCK)]
        rows += [top() if top else row(first + BLOCK)]
        for r in range(BLOCK):
            i = first + r
            new = new_rows(rows[r + 1], rows[r], rows[r + 2], nb(i), klo(i), khi(i), d(i), f(i))
            carry = put(i, new, carry)
        return carry

    carry = block(lo, below, None, carry)

    def body(b, carry):
        return block(lo + b * BLOCK, None, None, carry)

    n = (hi - lo) // BLOCK
    carry = lax.fori_loop(1, n - 1, body, carry)
    return block(hi - BLOCK, None, above, carry)


def plane_at(depth, n):
    low = lax.axis_index("lat") == 0
    return jnp.where(low, n - 1 - depth, depth)


def faces_kernel(u, lon_lo, lon_hi, lev_lo, lev_hi):
    nj, ni, nk, _ = u.shape
    for j in range(nj):
        lon_lo[j] = u[j, 0]
        lon_hi[j] = u[j, ni - 1]
        lev_lo[j] = u[j, :, 0, :]
        lev_hi[j] = u[j, :, nk - 1, :]


def load_kernel(u_in, d_in, f_in, u, pb, d_edge, f_edge, lon_lo, lon_hi, lev_lo, lev_hi, sem):
    nj, ni = u.shape[:2]
    q = ni // 4
    pj = plane_at(0, nj)
    copies = [pltpu.make_async_copy(u_in.at[j], u.at[j], sem.at[j]) for j in range(nj)]
    copies += [
        pltpu.make_async_copy(d_in.at[pj], d_edge, sem.at[nj]),
        pltpu.make_async_copy(f_in.at[pj], f_edge, sem.at[nj + 1]),
        pltpu.make_async_copy(u_in.at[pj, pl.ds(0, q)], pb.at[pl.ds(0, q)], sem.at[nj + 2]),
        pltpu.make_async_copy(u_in.at[pj, pl.ds(ni - q, q)], pb.at[pl.ds(q, q)], sem.at[nj + 3]),
    ]
    for copy in copies:
        copy.start()
    for copy in copies:
        copy.wait()
    faces_kernel(u, lon_lo, lon_hi, lev_lo, lev_hi)


def edge_rows(lo, hi, base, mine, below, above, u, lat, lev_lo, lev_hi, d, f, put):
    nj = u.shape[0]
    pj, pn = plane_at(0, nj), plane_at(1, nj)
    sweep(
        lo,
        hi,
        lambda i: mine[i],
        below,
        above,
        lambda i: u[pn, base + i] + lat[i],
        lambda i: lev_lo[pj, pl.ds(base + i, 1), :],
        lambda i: lev_hi[pj, pl.ds(base + i, 1), :],
        lambda i: d[base + i],
        lambda i: f[base + i],
        put,
        jnp.int32(0),
    )


def edge_a_kernel(u, pa, pb, lat, lev_lo, lev_hi, d, f, out):
    def put(i, new, carry):
        out[i] = new
        return carry

    n = pa.shape[0]
    edge_rows(0, n, n // 2, pa, lambda: pb[n // 2 - 1], lambda: pb[n // 2], u, lat, lev_lo, lev_hi, d, f, put)


def edge_b_kernel(u, pa, pb, lat, lon_lo, lon_hi, lev_lo, lev_hi, d, f, *rest):
    nj, ni, nk, _ = u.shape
    q = ni // 4
    pj = plane_at(0, nj)
    out = rest[2] if len(rest) > 1 else rest[0]

    def put(i, new, carry):
        out[i] = new
        return carry

    args = (u, lat, lev_lo, lev_hi, d, f, put)
    edge_rows(0, q, 0, pb, lambda: lon_lo[pj], lambda: pa[0], *args)
    edge_rows(q, 2 * q, 2 * q, pb, lambda: pa[2 * q - 1], lambda: lon_hi[pj], *args)
    if len(rest) > 1:
        nu, npa, _, s_lon_lo, s_lon_hi, s_lev_lo, s_lev_hi = rest
        faces_kernel(nu, s_lon_lo, s_lon_hi, s_lev_lo, s_lev_hi)
        s_lon_lo[pj] = out[0]
        s_lon_hi[pj] = out[2 * q - 1]
        for s_lev, k in ((s_lev_lo, 0), (s_lev_hi, nk - 1)):
            s_lev[pj, :q] = out[:q, k, :]
            s_lev[pj, q : 3 * q] = npa[:, k, :]
            s_lev[pj, 3 * q :] = out[q:, k, :]


def bulk_planes(u, pa, pb, lon_lo, lon_hi, lev_lo, lev_hi, d, f, put, start, finish):
    nj, ni, _, _ = u.shape
    q = ni // 4

    def run(j, lo, hi, nb, carry):
        return sweep(
            lo,
            hi,
            lambda i: u[j, i],
            (lambda: lon_lo[j]) if lo == 0 else None,
            (lambda: lon_hi[j]) if hi == ni else None,
            nb,
            lambda i: lev_lo[j, pl.ds(i, 1), :],
            lambda i: lev_hi[j, pl.ds(i, 1), :],
            lambda i: d[j, i],
            lambda i: f[j, i],
            functools.partial(put, j),
            carry,
        )

    j, inner = plane_at(1, nj), plane_at(2, nj)
    start(j, 1)
    carry = run(j, 0, q, lambda i: u[inner, i] + pb[i], zero_carry(u))
    carry = run(j, q, 3 * q, lambda i: u[inner, i] + pa[i - q], carry)
    carry = run(j, 3 * q, ni, lambda i: u[inner, i] + pb[i - 2 * q], carry)
    finish(j, 1, carry)

    def body(depth, _):
        j, outer, inner = plane_at(depth, nj), plane_at(depth - 1, nj), plane_at(depth + 1, nj)
        start(j, depth)
        carry = run(j, 0, ni, lambda i: u[outer, i] + u[inner, i], zero_carry(u))
        finish(j, depth, carry)
        return 0

    lax.fori_loop(2, nj - 1, body, 0)
    j, outer = plane_at(nj - 1, nj), plane_at(nj - 2, nj)
    start(j, nj - 1)
    carry = run(j, 0, ni, lambda i: u[outer, i], zero_carry(u))
    finish(j, nj - 1, carry)


def zero_carry(u):
    return jnp.zeros(u.shape[2:], u.dtype)


def nothing(*_):
    pass


def plain_put(out):
    def put(j, i, new, carry):
        out[j, i] = new
        return carry

    return put


def first_bulk_kernel(u, pa, pb, lon_lo, lon_hi, lev_lo, lev_hi, d_in, f_in, after, out, d, f, sem):
    del after
    nj = u.shape[0]

    def copies(j, depth):
        return (
            pltpu.make_async_copy(d_in.at[j], d.at[j], sem.at[0, depth]),
            pltpu.make_async_copy(f_in.at[j], f.at[j], sem.at[1, depth]),
        )

    for depth in range(1, nj):
        for copy in copies(plane_at(depth, nj), depth):
            copy.start()

    def start(j, depth):
        for copy in copies(j, depth):
            copy.wait()

    bulk_planes(u, pa, pb, lon_lo, lon_hi, lev_lo, lev_hi, d, f, plain_put(out), start, nothing)


def bulk_kernel(u, pa, pb, lon_lo, lon_hi, lev_lo, lev_hi, d, f, after, out):
    del after
    bulk_planes(u, pa, pb, lon_lo, lon_hi, lev_lo, lev_hi, d, f, plain_put(out), nothing, nothing)


def last_bulk_kernel(u, pa, pb, lon_lo, lon_hi, lev_lo, lev_hi, d_in, f_in, after, end, d, f, total, sem):
    del d_in, f_in, after
    nj = u.shape[0]

    def copy_out(j, depth):
        return pltpu.make_async_copy(f.at[j], end.at[j], sem.at[depth])

    def put(j, i, new, carry):
        f[j, i] = new
        carry = carry + new
        d[j, i] = carry
        return carry

    def finish(j, depth, carry):
        total[depth - 1] = carry
        copy_out(j, depth).start()

    bulk_planes(u, pa, pb, lon_lo, lon_hi, lev_lo, lev_hi, d, f, put, nothing, finish)
    for depth in range(1, nj):
        copy_out(plane_at(depth, nj), depth).wait()


def last_edge_kernel(u, pa, pb, lat, lon_lo, lon_hi, lev_lo, lev_hi, d, f, npa, npb, sums, total):
    edge_b_kernel(u, pa, pb, lat, lon_lo, lon_hi, lev_lo, lev_hi, d, f, npb)
    ni = sums.shape[0]
    q = ni // 4
    carry = zero_carry(u)
    for part, lo, n, base in ((npb, 0, q, 0), (npa, 0, 2 * q, q), (npb, q, q, 3 * q)):

        def row(r, carry):
            carry = carry + part[lo + r]
            sums[base + r] = carry
            return carry

        carry = lax.fori_loop(0, n, row, carry, unroll=4)
    total[...] = carry


def earlier(others):
    lon = lax.axis_index("lon")
    before = 0.0
    for bit, other in enumerate(others):
        before += jnp.where(lon & (1 << bit) != 0, other, 0.0)
    return before


def totals_kernel(scale, sums, *rest):
    *others, out, stage, sem = rest
    nj, ni = sums.shape[:2]

    def copy_out(j, depth):
        slot = depth % 2
        return pltpu.make_async_copy(stage.at[slot], out.at[j], sem.at[slot])

    def body(depth, _):
        j, slot = plane_at(depth, nj), depth % 2

        @pl.when(depth > 2)
        def _():
            copy_out(j, depth).wait()

        b = earlier([other[depth - 1] for other in others])

        def row(r, _):
            for q in range(BLOCK):
                i = r * BLOCK + q
                stage[slot, i] = (sums[j, i] + b) * scale
            return 0

        lax.fori_loop(0, ni // BLOCK, row, 0)
        copy_out(j, depth).start()
        return 0

    lax.fori_loop(1, nj, body, 0)
    copy_out(0, 0).wait()
    copy_out(0, 1).wait()


def last_totals_kernel(scale, sums, npa, npb, *rest):
    *others, _, _, end, out, stage, sem = rest
    ni = sums.shape[0]
    nj = out.shape[0]
    q = ni // 4
    pj = plane_at(0, nj)
    copies = [
        pltpu.make_async_copy(npb.at[pl.ds(0, q)], end.at[pj, pl.ds(0, q)], sem.at[0]),
        pltpu.make_async_copy(npa, end.at[pj, pl.ds(q, 2 * q)], sem.at[1]),
        pltpu.make_async_copy(npb.at[pl.ds(q, q)], end.at[pj, pl.ds(3 * q, q)], sem.at[2]),
    ]
    for copy in copies:
        copy.start()
    b = earlier([other[...] for other in others])

    def row(r, _):
        for p in range(BLOCK):
            i = r * BLOCK + p
            stage[i] = (sums[i] + b) * scale
        return 0

    for half in range(2):
        lax.fori_loop(half * ni // 2 // BLOCK, (half + 1) * ni // 2 // BLOCK, row, 0)
        rows = pl.ds(half * ni // 2, ni // 2)
        copies.append(pltpu.make_async_copy(stage.at[rows], out.at[pj, rows], sem.at[3 + half]))
        copies[-1].start()
    for copy in copies:
        copy.wait()


def call(kernel, out_shape, out_specs, in_specs, limit=2, scratch=(), aliases=None, flops=0):
    return pl.pallas_call(
        kernel,
        out_shape=out_shape,
        in_specs=in_specs,
        out_specs=out_specs,
        scratch_shapes=scratch,
        input_output_aliases=aliases or {},
        compiler_params=pltpu.CompilerParams(vmem_limit_bytes=limit * 2**20),
        cost_estimate=pl.CostEstimate(flops=flops, transcendentals=0, bytes_accessed=0),
    )


def per_device(lon_size, lev_size, initial_state, scaled_diffusivity, scaled_forcing):
    dtype = initial_state.dtype
    nj, ni, nk, nm = initial_state.shape
    half = ni // 2
    V = lambda *shape: pltpu.VMEM(shape, dtype)
    H = lambda *shape: pltpu.HBM(shape, dtype)

    swap = [(0, 1), (1, 0)]
    lon_up = [(i, i + 1) for i in range(lon_size - 1)]
    lev_up = [(i, i + 1) for i in range(lev_size - 1)]
    down = lambda pairs: [(b, a) for a, b in pairs]

    faces_out = (V(nj, nk, nm), V(nj, nk, nm), V(nj, ni, nm), V(nj, ni, nm))

    def lon_exchange(lon_lo, lon_hi):
        return lax.ppermute(lon_hi, "lon", lon_up), lax.ppermute(lon_lo, "lon", down(lon_up))

    def lev_exchange(lev_lo, lev_hi):
        return lax.ppermute(lev_hi, "lev", lev_up), lax.ppermute(lev_lo, "lev", down(lev_up))

    def partners(total):
        others = []
        for bit in range(lon_size.bit_length() - 1):
            pairs = [(i, i ^ (1 << bit)) for i in range(lon_size)]
            if others:
                total = total + others[-1]
            if 2 << bit == lon_size:
                pairs = [(a, b) for a, b in pairs if a < b]
            others.append(lax.ppermute(total, "lon", pairs))
        return tuple(map(in_vmem, others))

    pj = jnp.where(lax.axis_index("lat") == 0, nj - 1, 0)
    pa = lax.dynamic_slice(initial_state, (pj, ni // 4, 0, 0), (1, half, nk, nm))[0]
    lat_a = lax.ppermute(pa, "lat", swap)
    u, pb, d_edge, f_edge, *faces = call(
        load_kernel,
        (V(nj, ni, nk, nm), V(half, nk, nm), V(ni, nk, nm), V(ni, nk, nm)) + faces_out,
        (VMEM,) * 8,
        (HBM,) * 3,
        scratch=(pltpu.SemaphoreType.DMA((nj + 4,)),),
        flops=10**6,
    )(*map(in_hbm, (initial_state, scaled_diffusivity, scaled_forcing)))
    lon = lon_exchange(*faces[:2])
    lat_b = lax.ppermute(pb, "lat", swap)
    lev = lev_exchange(*faces[2:])
    d_edge, f_edge = in_vmem(d_edge), in_vmem(f_edge)
    d, f = in_hbm(scaled_diffusivity), in_hbm(scaled_forcing)

    for step in range(STEPS):
        last = step == STEPS - 1
        u, pa, pb, lat_a, lat_b = map(in_vmem, (u, pa, pb, lat_a, lat_b))
        lon, lev = tuple(map(in_vmem, lon)), tuple(map(in_vmem, lev))
        n_pa = call(edge_a_kernel, V(half, nk, nm), VMEM, (VMEM,) * 8, flops=10**6)(
            u, pa, pb, lat_a, *lev, d_edge, f_edge
        )
        if last:
            break
        lat_a = lax.ppermute(n_pa, "lat", swap)
        if step == 0:
            n_u, d, f = call(
                first_bulk_kernel,
                (V(nj, ni, nk, nm),) * 3,
                (VMEM,) * 3,
                (VMEM,) * 7 + (HBM,) * 2 + (ANY,),
                scratch=(pltpu.SemaphoreType.DMA((2, nj)),),
                flops=2 * 10**7,
            )(u, pa, pb, *lon, *lev, d, f, n_pa)
        else:
            n_u = call(
                bulk_kernel, V(nj, ni, nk, nm), VMEM, (VMEM,) * 9 + (ANY,), flops=2 * 10**7
            )(u, pa, pb, *lon, *lev, in_vmem(d), in_vmem(f), n_pa)
        n_pb, *faces = call(
            edge_b_kernel, (V(half, nk, nm),) + faces_out, (VMEM,) * 5, (VMEM,) * 12, flops=10**6
        )(u, pa, pb, lat_b, *lon, *lev, d_edge, f_edge, in_vmem(n_u), in_vmem(n_pa))
        lon = lon_exchange(*faces[:2])
        lat_b = lax.ppermute(n_pb, "lat", swap)
        lev = lev_exchange(*faces[2:])
        u, pa, pb = n_u, n_pa, n_pb

    scale = 1.0 / (ni * lon_size)
    n = lon_size.bit_length()
    end, sums, _, total = call(
        last_bulk_kernel,
        (H(nj, ni, nk, nm), V(nj, ni, nk, nm), V(nj, ni, nk, nm), V(nj - 1, nk, nm)),
        (HBM, VMEM, VMEM, VMEM),
        (VMEM,) * 9 + (ANY,),
        scratch=(pltpu.SemaphoreType.DMA((nj,)),),
        aliases={7: 1, 8: 2},
        flops=2 * 10**7,
    )(u, pa, pb, *lon, *lev, in_vmem(d), in_vmem(f), n_pa)
    others = partners(total)
    out = call(
        functools.partial(totals_kernel, scale),
        H(nj, ni, nk, nm),
        HBM,
        (VMEM,) * n,
        limit=4,
        scratch=(V(2, ni, nk, nm), pltpu.SemaphoreType.DMA((2,))),
        flops=10**6,
    )(in_vmem(sums), *others)
    n_pa = in_vmem(n_pa)
    n_pb, edge_sums, edge_total = call(
        last_edge_kernel, (V(half, nk, nm), V(ni, nk, nm), V(nk, nm)), (VMEM,) * 3, (VMEM,) * 11, flops=2 * 10**6
    )(u, pa, pb, lat_b, *lon, *lev, d_edge, f_edge, n_pa)
    others = partners(edge_total)
    end, out = call(
        functools.partial(last_totals_kernel, scale),
        (H(nj, ni, nk, nm),) * 2,
        (HBM, HBM),
        (VMEM,) * (n + 2) + (HBM, HBM),
        scratch=(V(ni, nk, nm), pltpu.SemaphoreType.DMA((5,))),
        limit=4,
        aliases={n + 2: 0, n + 3: 1},
        flops=10**6,
    )(in_vmem(edge_sums), n_pa, in_vmem(n_pb), *others, in_hbm(end), in_hbm(out))
    return out, end


def solution(mesh):
    spec = P("lat", "lon", "lev", None)
    return jax.shard_map(
        functools.partial(per_device, mesh.shape["lon"], mesh.shape["lev"]),
        mesh=mesh,
        in_specs=(spec, spec, spec),
        out_specs=(spec, spec),
        check_vma=False,
    )
```

```python
import functools

import jax
import jax.numpy as jnp
from jax import lax
from jax.experimental import pallas as pl
from jax.experimental.pallas import tpu as pltpu
from jax.sharding import PartitionSpec as P


STEPS = 4
BLOCK = 4
VMEM = pl.BlockSpec(memory_space=pltpu.VMEM)
HBM = pl.BlockSpec(memory_space=pltpu.HBM)
ANY = pl.BlockSpec(memory_space=pl.ANY)


def in_vmem(x):
    return pltpu.with_memory_space_constraint(x, pltpu.VMEM)


def in_hbm(x):
    return pltpu.with_memory_space_constraint(x, pltpu.HBM)


def new_rows(c, im, ip, nb, klo, khi, d, f):
    km = jnp.concatenate([klo, c[:-1]], axis=0)
    kp = jnp.concatenate([c[1:], khi], axis=0)
    spread = (im + ip) + nb + (km + kp) - 6.0 * c
    return c + d * spread + f


def sweep(lo, hi, row, below, above, nb, klo, khi, d, f, put, carry=None):
    def block(first, bottom, top, carry):
        rows = [bottom() if bottom else row(first - 1)]
        rows += [row(first + r) for r in range(BLOCK)]
        rows += [top() if top else row(first + BLOCK)]
        for r in range(BLOCK):
            i = first + r
            new = new_rows(rows[r + 1], rows[r], rows[r + 2], nb(i), klo(i), khi(i), d(i), f(i))
            carry = put(i, new, carry)
        return carry

    carry = block(lo, below, None, carry)

    def body(b, carry):
        return block(lo + b * BLOCK, None, None, carry)

    n = (hi - lo) // BLOCK
    carry = lax.fori_loop(1, n - 1, body, carry)
    return block(hi - BLOCK, None, above, carry)


def plane_at(depth, n):
    low = lax.axis_index("lat") == 0
    return jnp.where(low, n - 1 - depth, depth)


def odd(axis):
    return lax.axis_index(axis) % 2 == 1


def lower(axis, e, o):
    return jnp.where(odd(axis), e, o)


def upper(axis, e, o):
    return jnp.where(odd(axis), o, e)


def faces_kernel(u, lon_e, lon_o, lev_e, lev_o):
    nj, ni, nk, _ = u.shape
    at_e = jnp.where(odd("lon"), 0, ni - 1)
    for j in range(nj):
        lon_e[j] = u[j, at_e]
        lon_o[j] = u[j, ni - 1 - at_e]
        lo, hi = u[j, :, 0, :], u[j, :, nk - 1, :]
        lev_e[j] = lower("lev", lo, hi)
        lev_o[j] = upper("lev", lo, hi)


def load_kernel(u_in, d_in, f_in, u, pb, d_edge, f_edge, lon_e, lon_o, lev_e, lev_o, sem):
    nj, ni = u.shape[:2]
    q = ni // 4
    pj = plane_at(0, nj)
    copies = [pltpu.make_async_copy(u_in.at[j], u.at[j], sem.at[j]) for j in range(nj)]
    copies += [
        pltpu.make_async_copy(d_in.at[pj], d_edge, sem.at[nj]),
        pltpu.make_async_copy(f_in.at[pj], f_edge, sem.at[nj + 1]),
        pltpu.make_async_copy(u_in.at[pj, pl.ds(0, q)], pb.at[pl.ds(0, q)], sem.at[nj + 2]),
        pltpu.make_async_copy(u_in.at[pj, pl.ds(ni - q, q)], pb.at[pl.ds(q, q)], sem.at[nj + 3]),
    ]
    for copy in copies:
        copy.start()
    for copy in copies:
        copy.wait()
    faces_kernel(u, lon_e, lon_o, lev_e, lev_o)


def lev_rows(lev_e, lev_o, j, base):
    def get(side):
        def row(i):
            at = pl.ds(base + i, 1)
            return side("lev", lev_e[j, at, :], lev_o[j, at, :])

        return row

    return get(lower), get(upper)


def edge_rows(lo, hi, base, mine, below, above, u, lat, lev_e, lev_o, d, f, put):
    nj = u.shape[0]
    pj, pn = plane_at(0, nj), plane_at(1, nj)
    sweep(
        lo,
        hi,
        lambda i: mine[i],
        below,
        above,
        lambda i: u[pn, base + i] + lat[i],
        *lev_rows(lev_e, lev_o, pj, base),
        lambda i: d[base + i],
        lambda i: f[base + i],
        put,
        jnp.int32(0),
    )


def edge_a_kernel(u, pa, pb, lat, lev_e, lev_o, d, f, out):
    def put(i, new, carry):
        out[i] = new
        return carry

    n = pa.shape[0]
    edge_rows(0, n, n // 2, pa, lambda: pb[n // 2 - 1], lambda: pb[n // 2], u, lat, lev_e, lev_o, d, f, put)


def edge_b_kernel(u, pa, pb, lat, lon_e, lon_o, lev_e, lev_o, d, f, *rest):
    nj, ni, nk, _ = u.shape
    q = ni // 4
    pj = plane_at(0, nj)
    out = rest[2] if len(rest) > 1 else rest[0]

    def put(i, new, carry):
        out[i] = new
        return carry

    args = (u, lat, lev_e, lev_o, d, f, put)
    edge_rows(0, q, 0, pb, lambda: lower("lon", lon_e[pj], lon_o[pj]), lambda: pa[0], *args)
    edge_rows(q, 2 * q, 2 * q, pb, lambda: pa[2 * q - 1], lambda: upper("lon", lon_e[pj], lon_o[pj]), *args)
    if len(rest) > 1:
        nu, npa, _, s_lon_e, s_lon_o, s_lev_e, s_lev_o = rest
        faces_kernel(nu, s_lon_e, s_lon_o, s_lev_e, s_lev_o)
        s_lon_e[pj] = lower("lon", out[0], out[2 * q - 1])
        s_lon_o[pj] = upper("lon", out[0], out[2 * q - 1])
        for s_lev, side in ((s_lev_e, lower), (s_lev_o, upper)):
            s_lev[pj, :q] = side("lev", out[:q, 0, :], out[:q, nk - 1, :])
            s_lev[pj, q : 3 * q] = side("lev", npa[:, 0, :], npa[:, nk - 1, :])
            s_lev[pj, 3 * q :] = side("lev", out[q:, 0, :], out[q:, nk - 1, :])


def bulk_planes(u, pa, pb, lon_e, lon_o, lev_e, lev_o, d, f, put, start, finish):
    nj, ni, _, _ = u.shape
    q = ni // 4

    def run(j, lo, hi, nb, carry):
        return sweep(
            lo,
            hi,
            lambda i: u[j, i],
            (lambda: lower("lon", lon_e[j], lon_o[j])) if lo == 0 else None,
            (lambda: upper("lon", lon_e[j], lon_o[j])) if hi == ni else None,
            nb,
            *lev_rows(lev_e, lev_o, j, 0),
            lambda i: d[j, i],
            lambda i: f[j, i],
            functools.partial(put, j),
            carry,
        )

    j, inner = plane_at(1, nj), plane_at(2, nj)
    start(j, 1)
    carry = run(j, 0, q, lambda i: u[inner, i] + pb[i], zero_carry(u))
    carry = run(j, q, 3 * q, lambda i: u[inner, i] + pa[i - q], carry)
    carry = run(j, 3 * q, ni, lambda i: u[inner, i] + pb[i - 2 * q], carry)
    finish(j, 1, carry)

    def body(depth, _):
        j, outer, inner = plane_at(depth, nj), plane_at(depth - 1, nj), plane_at(depth + 1, nj)
        start(j, depth)
        carry = run(j, 0, ni, lambda i: u[outer, i] + u[inner, i], zero_carry(u))
        finish(j, depth, carry)
        return 0

    lax.fori_loop(2, nj - 1, body, 0)
    j, outer = plane_at(nj - 1, nj), plane_at(nj - 2, nj)
    start(j, nj - 1)
    carry = run(j, 0, ni, lambda i: u[outer, i], zero_carry(u))
    finish(j, nj - 1, carry)


def zero_carry(u):
    return jnp.zeros(u.shape[2:], u.dtype)


def nothing(*_):
    pass


def plain_put(out):
    def put(j, i, new, carry):
        out[j, i] = new
        return carry

    return put


def first_bulk_kernel(u, pa, pb, lon_e, lon_o, lev_e, lev_o, d_in, f_in, after, out, d, f, sem):
    del after
    nj = u.shape[0]

    def copies(j, depth):
        return (
            pltpu.make_async_copy(d_in.at[j], d.at[j], sem.at[0, depth]),
            pltpu.make_async_copy(f_in.at[j], f.at[j], sem.at[1, depth]),
        )

    for depth in range(1, nj):
        for copy in copies(plane_at(depth, nj), depth):
            copy.start()

    def start(j, depth):
        for copy in copies(j, depth):
            copy.wait()

    bulk_planes(u, pa, pb, lon_e, lon_o, lev_e, lev_o, d, f, plain_put(out), start, nothing)


def bulk_kernel(u, pa, pb, lon_e, lon_o, lev_e, lev_o, d, f, after, out):
    del after
    bulk_planes(u, pa, pb, lon_e, lon_o, lev_e, lev_o, d, f, plain_put(out), nothing, nothing)


def last_bulk_kernel(u, pa, pb, lon_e, lon_o, lev_e, lev_o, d_in, f_in, after, end, d, f, total, sem):
    del d_in, f_in, after
    nj = u.shape[0]

    def copy_out(j, depth):
        return pltpu.make_async_copy(f.at[j], end.at[j], sem.at[depth])

    def put(j, i, new, carry):
        f[j, i] = new
        carry = carry + new
        d[j, i] = carry
        return carry

    def finish(j, depth, carry):
        total[depth - 1] = carry
        copy_out(j, depth).start()

    bulk_planes(u, pa, pb, lon_e, lon_o, lev_e, lev_o, d, f, put, nothing, finish)
    for depth in range(1, nj):
        copy_out(plane_at(depth, nj), depth).wait()


def last_edge_kernel(u, pa, pb, lat, lon_e, lon_o, lev_e, lev_o, d, f, npa, npb, sums, total):
    edge_b_kernel(u, pa, pb, lat, lon_e, lon_o, lev_e, lev_o, d, f, npb)
    ni = sums.shape[0]
    q = ni // 4
    carry = zero_carry(u)
    for part, lo, n, base in ((npb, 0, q, 0), (npa, 0, 2 * q, q), (npb, q, q, 3 * q)):

        def row(r, carry):
            carry = carry + part[lo + r]
            sums[base + r] = carry
            return carry

        carry = lax.fori_loop(0, n, row, carry, unroll=4)
    total[...] = carry


def earlier(others, first=0):
    lon = lax.axis_index("lon")
    before = 0.0
    for bit, other in enumerate(others):
        before += jnp.where(lon & (1 << (first + bit)) != 0, other, 0.0)
    return before


def half_kernel(total, other, out):
    n = out.shape[1]
    at = pl.ds(pl.multiple_of(jnp.where(odd("lon"), n, 0), n), n)
    for p in range(out.shape[0]):
        out[p] = total[p, at] + other[p, at]


def before_kernel(*refs):
    *others, out = refs
    for p in range(out.shape[0]):
        out[p] = earlier([other[p] for other in others], 1)


def totals_kernel(scale, sums, other, mine, partners, out, stage, sem):
    nj, ni = sums.shape[:2]

    def copy_out(j, depth):
        slot = depth % 2
        return pltpu.make_async_copy(stage.at[slot], out.at[j], sem.at[slot])

    def body(depth, _):
        j, slot = plane_at(depth, nj), depth % 2

        @pl.when(depth > 2)
        def _():
            copy_out(j, depth).wait()

        a, b = mine[depth - 1], partners[depth - 1]
        b = jnp.concatenate([jnp.where(odd("lon"), b, a), jnp.where(odd("lon"), a, b)], axis=0)
        b += earlier([other[depth - 1]])

        def row(r, _):
            for q in range(BLOCK):
                i = r * BLOCK + q
                stage[slot, i] = (sums[j, i] + b) * scale
            return 0

        lax.fori_loop(0, ni // BLOCK, row, 0)
        copy_out(j, depth).start()
        return 0

    lax.fori_loop(1, nj, body, 0)
    copy_out(0, 0).wait()
    copy_out(0, 1).wait()


def last_totals_kernel(scale, sums, npa, npb, *rest):
    *others, _, _, end, out, stage, sem = rest
    ni = sums.shape[0]
    nj = out.shape[0]
    q = ni // 4
    pj = plane_at(0, nj)
    copies = [
        pltpu.make_async_copy(npb.at[pl.ds(0, q)], end.at[pj, pl.ds(0, q)], sem.at[0]),
        pltpu.make_async_copy(npa, end.at[pj, pl.ds(q, 2 * q)], sem.at[1]),
        pltpu.make_async_copy(npb.at[pl.ds(q, q)], end.at[pj, pl.ds(3 * q, q)], sem.at[2]),
    ]
    for copy in copies:
        copy.start()
    b = earlier([other[...] for other in others])

    def row(r, _):
        for p in range(BLOCK):
            i = r * BLOCK + p
            stage[i] = (sums[i] + b) * scale
        return 0

    for half in range(2):
        lax.fori_loop(half * ni // 2 // BLOCK, (half + 1) * ni // 2 // BLOCK, row, 0)
        rows = pl.ds(half * ni // 2, ni // 2)
        copies.append(pltpu.make_async_copy(stage.at[rows], out.at[pj, rows], sem.at[3 + half]))
        copies[-1].start()
    for copy in copies:
        copy.wait()


def call(kernel, out_shape, out_specs, in_specs, limit=2, scratch=(), aliases=None, flops=0):
    return pl.pallas_call(
        kernel,
        out_shape=out_shape,
        in_specs=in_specs,
        out_specs=out_specs,
        scratch_shapes=scratch,
        input_output_aliases=aliases or {},
        compiler_params=pltpu.CompilerParams(vmem_limit_bytes=limit * 2**20),
        cost_estimate=pl.CostEstimate(flops=flops, transcendentals=0, bytes_accessed=0),
    )


def per_device(lon_size, lev_size, initial_state, scaled_diffusivity, scaled_forcing):
    dtype = initial_state.dtype
    nj, ni, nk, nm = initial_state.shape
    half = ni // 2
    V = lambda *shape: pltpu.VMEM(shape, dtype)
    H = lambda *shape: pltpu.HBM(shape, dtype)

    swap = [(0, 1), (1, 0)]
    faces_out = (V(nj, nk, nm), V(nj, nk, nm), V(nj, ni, nm), V(nj, ni, nm))

    def exchange(axis, size, e, o):
        def swaps(first):
            return [(a, b) for i in range(first, size - 1, 2) for a, b in ((i, i + 1), (i + 1, i))]

        return lax.ppermute(e, axis, swaps(0)), lax.ppermute(o, axis, swaps(1))

    def lon_exchange(e, o):
        return exchange("lon", lon_size, e, o)

    def lev_exchange(e, o):
        return exchange("lev", lev_size, e, o)

    def partner(bit, total):
        pairs = [(i, i ^ (1 << bit)) for i in range(lon_size)]
        if 2 << bit == lon_size:
            pairs = [(a, b) for a, b in pairs if a < b]
        return lax.ppermute(total, "lon", pairs)

    bits = lon_size.bit_length() - 1

    pj = jnp.where(lax.axis_index("lat") == 0, nj - 1, 0)
    pa = lax.dynamic_slice(initial_state, (pj, ni // 4, 0, 0), (1, half, nk, nm))[0]
    lat_a = lax.ppermute(pa, "lat", swap)
    u, pb, d_edge, f_edge, *faces = call(
        load_kernel,
        (V(nj, ni, nk, nm), V(half, nk, nm), V(ni, nk, nm), V(ni, nk, nm)) + faces_out,
        (VMEM,) * 8,
        (HBM,) * 3,
        scratch=(pltpu.SemaphoreType.DMA((nj + 4,)),),
        flops=10**6,
    )(*map(in_hbm, (initial_state, scaled_diffusivity, scaled_forcing)))
    lev = lev_exchange(*faces[2:])
    lon = lon_exchange(*faces[:2])
    lat_b = lax.ppermute(pb, "lat", swap)
    d_edge, f_edge = in_vmem(d_edge), in_vmem(f_edge)
    d, f = in_hbm(scaled_diffusivity), in_hbm(scaled_forcing)

    for step in range(STEPS):
        last = step == STEPS - 1
        u, pa, pb, lat_a, lat_b = map(in_vmem, (u, pa, pb, lat_a, lat_b))
        lon, lev = tuple(map(in_vmem, lon)), tuple(map(in_vmem, lev))
        n_pa = call(edge_a_kernel, V(half, nk, nm), VMEM, (VMEM,) * 8, flops=10**6)(
            u, pa, pb, lat_a, *lev, d_edge, f_edge
        )
        if last:
            break
        lat_a = lax.ppermute(n_pa, "lat", swap)
        if step == 0:
            n_u, d, f = call(
                first_bulk_kernel,
                (V(nj, ni, nk, nm),) * 3,
                (VMEM,) * 3,
                (VMEM,) * 7 + (HBM,) * 2 + (ANY,),
                scratch=(pltpu.SemaphoreType.DMA((2, nj)),),
                flops=2 * 10**7,
            )(u, pa, pb, *lon, *lev, d, f, n_pa)
        else:
            n_u = call(
                bulk_kernel, V(nj, ni, nk, nm), VMEM, (VMEM,) * 9 + (ANY,), flops=2 * 10**7
            )(u, pa, pb, *lon, *lev, in_vmem(d), in_vmem(f), n_pa)
        n_pb, *faces = call(
            edge_b_kernel, (V(half, nk, nm),) + faces_out, (VMEM,) * 5, (VMEM,) * 12, flops=10**6
        )(u, pa, pb, lat_b, *lon, *lev, d_edge, f_edge, in_vmem(n_u), in_vmem(n_pa))
        lon = lon_exchange(*faces[:2])
        lat_b = lax.ppermute(n_pb, "lat", swap)
        lev = lev_exchange(*faces[2:])
        u, pa, pb = n_u, n_pa, n_pb

    scale = 1.0 / (ni * lon_size)
    n = bits + 1
    end, sums, _, total = call(
        last_bulk_kernel,
        (H(nj, ni, nk, nm), V(nj, ni, nk, nm), V(nj, ni, nk, nm), V(nj - 1, nk, nm)),
        (HBM, VMEM, VMEM, VMEM),
        (VMEM,) * 9 + (ANY,),
        scratch=(pltpu.SemaphoreType.DMA((nj,)),),
        aliases={7: 1, 8: 2},
        flops=2 * 10**7,
    )(u, pa, pb, *lon, *lev, in_vmem(d), in_vmem(f), n_pa)
    other = partner(0, total)
    mine = call(half_kernel, V(nj - 1, nk // 2, nm), VMEM, (VMEM,) * 2, flops=10**5)(in_vmem(total), in_vmem(other))
    others = []
    for bit in range(1, bits):
        others.append(partner(bit, mine))
        mine = mine + others[-1]
    mine = call(before_kernel, V(nj - 1, nk // 2, nm), VMEM, (VMEM,) * (bits - 1), flops=10**5)(*map(in_vmem, others))
    back = lax.ppermute(mine, "lon", [(i, i ^ 1) for i in range(lon_size)])
    out = call(
        functools.partial(totals_kernel, scale),
        H(nj, ni, nk, nm),
        HBM,
        (VMEM,) * 4,
        limit=4,
        scratch=(V(2, ni, nk, nm), pltpu.SemaphoreType.DMA((2,))),
        flops=10**6,
    )(*map(in_vmem, (sums, other, mine, back)))
    n_pa = in_vmem(n_pa)
    n_pb, edge_sums, edge_total = call(
        last_edge_kernel, (V(half, nk, nm), V(ni, nk, nm), V(nk, nm)), (VMEM,) * 3, (VMEM,) * 11, flops=2 * 10**6
    )(u, pa, pb, lat_b, *lon, *lev, d_edge, f_edge, n_pa)
    others = []
    for bit in range(bits):
        others.append(partner(bit, edge_total))
        edge_total = edge_total + others[-1]
    others = tuple(map(in_vmem, others))
    end, out = call(
        functools.partial(last_totals_kernel, scale),
        (H(nj, ni, nk, nm),) * 2,
        (HBM, HBM),
        (VMEM,) * (n + 2) + (HBM, HBM),
        scratch=(V(ni, nk, nm), pltpu.SemaphoreType.DMA((5,))),
        limit=4,
        aliases={n + 2: 0, n + 3: 1},
        flops=10**6,
    )(in_vmem(edge_sums), n_pa, in_vmem(n_pb), *others, in_hbm(end), in_hbm(out))
    return out, end


def solution(mesh):
    spec = P("lat", "lon", "lev", None)
    return jax.shard_map(
        functools.partial(per_device, mesh.shape["lon"], mesh.shape["lev"]),
        mesh=mesh,
        in_specs=(spec, spec, spec),
        out_specs=(spec, spec),
        check_vma=False,
    )
```

```python
import functools

import jax
import jax.numpy as jnp
from jax import lax
from jax.experimental import pallas as pl
from jax.experimental.pallas import tpu as pltpu
from jax.sharding import PartitionSpec as P


STEPS = 4
BLOCK = 4
VMEM = pl.BlockSpec(memory_space=pltpu.VMEM)
HBM = pl.BlockSpec(memory_space=pltpu.HBM)
ANY = pl.BlockSpec(memory_space=pl.ANY)


def in_vmem(x):
    return pltpu.with_memory_space_constraint(x, pltpu.VMEM)


def in_hbm(x):
    return pltpu.with_memory_space_constraint(x, pltpu.HBM)


def new_rows(c, im, ip, nb, klo, khi, d, f):
    km = jnp.concatenate([klo, c[:-1]], axis=0)
    kp = jnp.concatenate([c[1:], khi], axis=0)
    spread = (im + ip) + nb + (km + kp) - 6.0 * c
    return c + d * spread + f


def sweep(lo, hi, row, below, above, nb, klo, khi, d, f, put, carry=None):
    def block(first, bottom, top, carry):
        rows = [bottom() if bottom else row(first - 1)]
        rows += [row(first + r) for r in range(BLOCK)]
        rows += [top() if top else row(first + BLOCK)]
        for r in range(BLOCK):
            i = first + r
            new = new_rows(rows[r + 1], rows[r], rows[r + 2], nb(i), klo(i), khi(i), d(i), f(i))
            carry = put(i, new, carry)
        return carry

    carry = block(lo, below, None, carry)

    def body(b, carry):
        return block(lo + b * BLOCK, None, None, carry)

    n = (hi - lo) // BLOCK
    carry = lax.fori_loop(1, n - 1, body, carry)
    return block(hi - BLOCK, None, above, carry)


def plane_at(depth, n):
    low = lax.axis_index("lat") == 0
    return jnp.where(low, n - 1 - depth, depth)


def odd(axis):
    return lax.axis_index(axis) % 2 == 1


def lower(axis, e, o):
    return jnp.where(odd(axis), e, o)


def upper(axis, e, o):
    return jnp.where(odd(axis), o, e)


def faces_kernel(u, lon_e, lon_o, lev_e, lev_o):
    nj, ni, nk, _ = u.shape
    at_e = jnp.where(odd("lon"), 0, ni - 1)
    for j in range(nj):
        lon_e[j] = u[j, at_e]
        lon_o[j] = u[j, ni - 1 - at_e]
        lo, hi = u[j, :, 0, :], u[j, :, nk - 1, :]
        lev_e[j] = lower("lev", lo, hi)
        lev_o[j] = upper("lev", lo, hi)


def load_kernel(u_in, d_in, f_in, u, pb, d_edge, f_edge, lon_e, lon_o, lev_e, lev_o, sem):
    nj, ni = u.shape[:2]
    q = ni // 4
    pj = plane_at(0, nj)
    copies = [pltpu.make_async_copy(u_in.at[j], u.at[j], sem.at[j]) for j in range(nj)]
    copies += [
        pltpu.make_async_copy(d_in.at[pj], d_edge, sem.at[nj]),
        pltpu.make_async_copy(f_in.at[pj], f_edge, sem.at[nj + 1]),
        pltpu.make_async_copy(u_in.at[pj, pl.ds(0, q)], pb.at[pl.ds(0, q)], sem.at[nj + 2]),
        pltpu.make_async_copy(u_in.at[pj, pl.ds(ni - q, q)], pb.at[pl.ds(q, q)], sem.at[nj + 3]),
    ]
    for copy in copies:
        copy.start()
    for copy in copies:
        copy.wait()
    faces_kernel(u, lon_e, lon_o, lev_e, lev_o)


def lev_rows(lev_e, lev_o, j, base):
    def get(side):
        def row(i):
            at = pl.ds(base + i, 1)
            return side("lev", lev_e[j, at, :], lev_o[j, at, :])

        return row

    return get(lower), get(upper)


def edge_rows(lo, hi, base, mine, lat, below, above, u, lev_e, lev_o, d, f, put):
    nj = u.shape[0]
    pj, pn = plane_at(0, nj), plane_at(1, nj)
    sweep(
        lo,
        hi,
        lambda i: mine[i],
        below,
        above,
        lambda i: u[pn, base + i] + lat(i),
        *lev_rows(lev_e, lev_o, pj, base),
        lambda i: d[base + i],
        lambda i: f[base + i],
        put,
        jnp.int32(0),
    )


def edge_a_kernel(parts, u, pa, pb, *rest):
    lats, (lev_e, lev_o, d, f, out) = rest[:parts], rest[parts:]

    def put(i, new, carry):
        out[i] = new
        return carry

    n = pa.shape[0]
    m = n // parts
    for part, lat in enumerate(lats):
        edge_rows(
            part * m,
            (part + 1) * m,
            n // 2,
            pa,
            lambda i: lat[i - part * m],
            (lambda: pb[n // 2 - 1]) if part == 0 else None,
            (lambda: pb[n // 2]) if part == parts - 1 else None,
            u,
            lev_e,
            lev_o,
            d,
            f,
            put,
        )


def edge_b_kernel(u, pa, pb, lat, lon_e, lon_o, lev_e, lev_o, d, f, *rest):
    nj, ni, nk, _ = u.shape
    q = ni // 4
    pj = plane_at(0, nj)
    out = rest[2] if len(rest) > 1 else rest[0]

    def put(i, new, carry):
        out[i] = new
        return carry

    lat_lo, lat_hi = lat if isinstance(lat, tuple) else (lat, lat.at[pl.ds(q, q)])
    args = (u, lev_e, lev_o, d, f, put)
    edge_rows(0, q, 0, pb, lambda i: lat_lo[i], lambda: lower("lon", lon_e[pj], lon_o[pj]), lambda: pa[0], *args)
    above = lambda: upper("lon", lon_e[pj], lon_o[pj])
    edge_rows(q, 2 * q, 2 * q, pb, lambda i: lat_hi[i - q], lambda: pa[2 * q - 1], above, *args)
    if len(rest) > 1:
        nu, npa, _, s_lon_e, s_lon_o, s_lev_e, s_lev_o = rest
        faces_kernel(nu, s_lon_e, s_lon_o, s_lev_e, s_lev_o)
        s_lon_e[pj] = lower("lon", out[0], out[2 * q - 1])
        s_lon_o[pj] = upper("lon", out[0], out[2 * q - 1])
        for s_lev, side in ((s_lev_e, lower), (s_lev_o, upper)):
            s_lev[pj, :q] = side("lev", out[:q, 0, :], out[:q, nk - 1, :])
            s_lev[pj, q : 3 * q] = side("lev", npa[:, 0, :], npa[:, nk - 1, :])
            s_lev[pj, 3 * q :] = side("lev", out[q:, 0, :], out[q:, nk - 1, :])


def bulk_planes(u, pa, pb, lon_e, lon_o, lev_e, lev_o, d, f, put, start, finish):
    nj, ni, _, _ = u.shape
    q = ni // 4

    def run(j, lo, hi, nb, carry):
        return sweep(
            lo,
            hi,
            lambda i: u[j, i],
            (lambda: lower("lon", lon_e[j], lon_o[j])) if lo == 0 else None,
            (lambda: upper("lon", lon_e[j], lon_o[j])) if hi == ni else None,
            nb,
            *lev_rows(lev_e, lev_o, j, 0),
            lambda i: d[j, i],
            lambda i: f[j, i],
            functools.partial(put, j),
            carry,
        )

    j, inner = plane_at(1, nj), plane_at(2, nj)
    start(j, 1)
    carry = run(j, 0, q, lambda i: u[inner, i] + pb[i], zero_carry(u))
    carry = run(j, q, 3 * q, lambda i: u[inner, i] + pa[i - q], carry)
    carry = run(j, 3 * q, ni, lambda i: u[inner, i] + pb[i - 2 * q], carry)
    finish(j, 1, carry)

    def body(depth, _):
        j, outer, inner = plane_at(depth, nj), plane_at(depth - 1, nj), plane_at(depth + 1, nj)
        start(j, depth)
        carry = run(j, 0, ni, lambda i: u[outer, i] + u[inner, i], zero_carry(u))
        finish(j, depth, carry)
        return 0

    lax.fori_loop(2, nj - 1, body, 0)
    j, outer = plane_at(nj - 1, nj), plane_at(nj - 2, nj)
    start(j, nj - 1)
    carry = run(j, 0, ni, lambda i: u[outer, i], zero_carry(u))
    finish(j, nj - 1, carry)


def zero_carry(u):
    return jnp.zeros(u.shape[2:], u.dtype)


def nothing(*_):
    pass


def plain_put(out):
    def put(j, i, new, carry):
        out[j, i] = new
        return carry

    return put


def first_bulk_kernel(u, pa, pb, lon_e, lon_o, lev_e, lev_o, d_in, f_in, after, out, d, f, sem):
    del after
    nj = u.shape[0]

    def copies(j, depth):
        return (
            pltpu.make_async_copy(d_in.at[j], d.at[j], sem.at[0, depth]),
            pltpu.make_async_copy(f_in.at[j], f.at[j], sem.at[1, depth]),
        )

    for depth in range(1, nj):
        for copy in copies(plane_at(depth, nj), depth):
            copy.start()

    def start(j, depth):
        for copy in copies(j, depth):
            copy.wait()

    bulk_planes(u, pa, pb, lon_e, lon_o, lev_e, lev_o, d, f, plain_put(out), start, nothing)


def bulk_kernel(u, pa, pb, lon_e, lon_o, lev_e, lev_o, d, f, after, out):
    del after
    bulk_planes(u, pa, pb, lon_e, lon_o, lev_e, lev_o, d, f, plain_put(out), nothing, nothing)


def last_bulk_kernel(u, pa, pb, lon_e, lon_o, lev_e, lev_o, d_in, f_in, end, d, f, total, sem):
    del d_in, f_in
    nj = u.shape[0]

    def copy_out(j, depth):
        return pltpu.make_async_copy(f.at[j], end.at[j], sem.at[depth])

    def put(j, i, new, carry):
        f[j, i] = new
        carry = carry + new
        d[j, i] = carry
        return carry

    def finish(j, depth, carry):
        total[depth - 1] = carry
        copy_out(j, depth).start()

    bulk_planes(u, pa, pb, lon_e, lon_o, lev_e, lev_o, d, f, put, nothing, finish)
    for depth in range(1, nj):
        copy_out(plane_at(depth, nj), depth).wait()


def last_edge_kernel(u, pa, pb, lat_lo, lat_hi, lon_e, lon_o, lev_e, lev_o, d, f, npa, npb, sums, total):
    edge_b_kernel(u, pa, pb, (lat_lo, lat_hi), lon_e, lon_o, lev_e, lev_o, d, f, npb)
    ni = sums.shape[0]
    q = ni // 4
    carry = zero_carry(u)
    for part, lo, n, base in ((npb, 0, q, 0), (npa, 0, 2 * q, q), (npb, q, q, 3 * q)):

        def row(r, carry):
            carry = carry + part[lo + r]
            sums[base + r] = carry
            return carry

        carry = lax.fori_loop(0, n, row, carry, unroll=4)
    total[...] = carry


def earlier(others, first=0):
    lon = lax.axis_index("lon")
    before = 0.0
    for bit, other in enumerate(others):
        before += jnp.where(lon & (1 << (first + bit)) != 0, other, 0.0)
    return before


def half_kernel(total, other, out):
    n = out.shape[1]
    at = pl.ds(pl.multiple_of(jnp.where(odd("lon"), n, 0), n), n)
    for p in range(out.shape[0]):
        out[p] = total[p, at] + other[p, at]


def before_kernel(*refs):
    *others, out = refs
    for p in range(out.shape[0]):
        out[p] = earlier([other[p] for other in others], 1)


def totals_kernel(scale, sums, other, mine, partners, out, stage, sem):
    nj, ni = sums.shape[:2]

    def copy_out(j, depth):
        slot = depth % 2
        return pltpu.make_async_copy(stage.at[slot], out.at[j], sem.at[slot])

    def body(depth, _):
        j, slot = plane_at(depth, nj), depth % 2

        @pl.when(depth > 2)
        def _():
            copy_out(j, depth).wait()

        a, b = mine[depth - 1], partners[depth - 1]
        b = jnp.concatenate([jnp.where(odd("lon"), b, a), jnp.where(odd("lon"), a, b)], axis=0)
        b += earlier([other[depth - 1]])

        def row(r, _):
            for q in range(BLOCK):
                i = r * BLOCK + q
                stage[slot, i] = (sums[j, i] + b) * scale
            return 0

        lax.fori_loop(0, ni // BLOCK, row, 0)
        copy_out(j, depth).start()
        return 0

    lax.fori_loop(1, nj, body, 0)
    copy_out(0, 0).wait()
    copy_out(0, 1).wait()


def last_totals_kernel(scale, sums, npa, npb, *rest):
    *others, _, _, end, out, stage, sem = rest
    ni = sums.shape[0]
    nj = out.shape[0]
    q = ni // 4
    pj = plane_at(0, nj)
    copies = [
        pltpu.make_async_copy(npb.at[pl.ds(0, q)], end.at[pj, pl.ds(0, q)], sem.at[0]),
        pltpu.make_async_copy(npa, end.at[pj, pl.ds(q, 2 * q)], sem.at[1]),
        pltpu.make_async_copy(npb.at[pl.ds(q, q)], end.at[pj, pl.ds(3 * q, q)], sem.at[2]),
    ]
    for copy in copies:
        copy.start()
    b = earlier([other[...] for other in others])

    def row(r, _):
        for p in range(BLOCK):
            i = r * BLOCK + p
            stage[i] = (sums[i] + b) * scale
        return 0

    for half in range(2):
        lax.fori_loop(half * ni // 2 // BLOCK, (half + 1) * ni // 2 // BLOCK, row, 0)
        rows = pl.ds(half * ni // 2, ni // 2)
        copies.append(pltpu.make_async_copy(stage.at[rows], out.at[pj, rows], sem.at[3 + half]))
        copies[-1].start()
    for copy in copies:
        copy.wait()


def call(kernel, out_shape, out_specs, in_specs, limit=2, scratch=(), aliases=None, flops=0):
    return pl.pallas_call(
        kernel,
        out_shape=out_shape,
        in_specs=in_specs,
        out_specs=out_specs,
        scratch_shapes=scratch,
        input_output_aliases=aliases or {},
        compiler_params=pltpu.CompilerParams(vmem_limit_bytes=limit * 2**20),
        cost_estimate=pl.CostEstimate(flops=flops, transcendentals=0, bytes_accessed=0),
    )


def per_device(lon_size, lev_size, initial_state, scaled_diffusivity, scaled_forcing):
    dtype = initial_state.dtype
    nj, ni, nk, nm = initial_state.shape
    half = ni // 2
    V = lambda *shape: pltpu.VMEM(shape, dtype)
    H = lambda *shape: pltpu.HBM(shape, dtype)

    swap = [(0, 1), (1, 0)]
    faces_out = (V(nj, nk, nm), V(nj, nk, nm), V(nj, ni, nm), V(nj, ni, nm))

    def exchange(axis, size, e, o):
        def swaps(first):
            return [(a, b) for i in range(first, size - 1, 2) for a, b in ((i, i + 1), (i + 1, i))]

        return lax.ppermute(e, axis, swaps(0)), lax.ppermute(o, axis, swaps(1))

    def lon_exchange(e, o):
        return exchange("lon", lon_size, e, o)

    def lev_exchange(e, o):
        return exchange("lev", lev_size, e, o)

    def partner(bit, total):
        pairs = [(i, i ^ (1 << bit)) for i in range(lon_size)]
        if 2 << bit == lon_size:
            pairs = [(a, b) for a, b in pairs if a < b]
        return lax.ppermute(total, "lon", pairs)

    bits = lon_size.bit_length() - 1

    pj = jnp.where(lax.axis_index("lat") == 0, nj - 1, 0)
    pa = lax.dynamic_slice(initial_state, (pj, ni // 4, 0, 0), (1, half, nk, nm))[0]
    lat_a = lax.ppermute(pa, "lat", swap)
    u, pb, d_edge, f_edge, *faces = call(
        load_kernel,
        (V(nj, ni, nk, nm), V(half, nk, nm), V(ni, nk, nm), V(ni, nk, nm)) + faces_out,
        (VMEM,) * 8,
        (HBM,) * 3,
        scratch=(pltpu.SemaphoreType.DMA((nj + 4,)),),
        flops=10**6,
    )(*map(in_hbm, (initial_state, scaled_diffusivity, scaled_forcing)))
    lev = lev_exchange(*faces[2:])
    lon = lon_exchange(*faces[:2])
    lat_b = lax.ppermute(pb, "lat", swap)
    d_edge, f_edge = in_vmem(d_edge), in_vmem(f_edge)
    d, f = in_hbm(scaled_diffusivity), in_hbm(scaled_forcing)

    lat_a = (lat_a,)
    for step in range(STEPS):
        next_is_last = step == STEPS - 2
        u, pa, pb = map(in_vmem, (u, pa, pb))
        lat_a = tuple(map(in_vmem, lat_a))
        lon, lev = tuple(map(in_vmem, lon)), tuple(map(in_vmem, lev))
        parts = len(lat_a)
        n_pa = call(
            functools.partial(edge_a_kernel, parts), V(half, nk, nm), VMEM, (VMEM,) * (7 + parts), flops=10**6
        )(u, pa, pb, *lat_a, *lev, d_edge, f_edge)
        if step == STEPS - 1:
            break
        lat_a = (lax.ppermute(n_pa[: half // 2] if next_is_last else n_pa, "lat", swap),)
        if step == 0:
            n_u, d, f = call(
                first_bulk_kernel,
                (V(nj, ni, nk, nm),) * 3,
                (VMEM,) * 3,
                (VMEM,) * 7 + (HBM,) * 2 + (ANY,),
                scratch=(pltpu.SemaphoreType.DMA((2, nj)),),
                flops=2 * 10**7,
            )(u, pa, pb, *lon, *lev, d, f, n_pa)
        else:
            n_u = call(
                bulk_kernel, V(nj, ni, nk, nm), VMEM, (VMEM,) * 9 + (ANY,), flops=2 * 10**7
            )(u, pa, pb, *lon, *lev, in_vmem(d), in_vmem(f), n_pa)
        n_pb, *faces = call(
            edge_b_kernel, (V(half, nk, nm),) + faces_out, (VMEM,) * 5, (VMEM,) * 12, flops=10**6
        )(u, pa, pb, in_vmem(lat_b), *lon, *lev, d_edge, f_edge, in_vmem(n_u), in_vmem(n_pa))
        lon = lon_exchange(*faces[:2])
        if next_is_last:
            lat_a += (lax.ppermute(n_pa[half // 2 :], "lat", swap),)
            lat_b = lax.ppermute(n_pb[: half // 2], "lat", swap)
            final = n_pb[half // 2 :]
        else:
            lat_b = lax.ppermute(n_pb, "lat", swap)
        lev = lev_exchange(*faces[2:])
        u, pa, pb = n_u, n_pa, n_pb

    scale = 1.0 / (ni * lon_size)
    n = bits + 1
    lat_c = lax.ppermute(final, "lat", swap)
    end, sums, _, total = call(
        last_bulk_kernel,
        (H(nj, ni, nk, nm), V(nj, ni, nk, nm), V(nj, ni, nk, nm), V(nj - 1, nk, nm)),
        (HBM, VMEM, VMEM, VMEM),
        (VMEM,) * 9,
        scratch=(pltpu.SemaphoreType.DMA((nj,)),),
        aliases={7: 1, 8: 2},
        flops=2 * 10**7,
    )(u, pa, pb, *lon, *lev, in_vmem(d), in_vmem(f))
    other = partner(0, total)
    mine = call(half_kernel, V(nj - 1, nk // 2, nm), VMEM, (VMEM,) * 2, flops=10**5)(in_vmem(total), in_vmem(other))
    others = []
    for bit in range(1, bits):
        others.append(partner(bit, mine))
        mine = mine + others[-1]
    mine = call(before_kernel, V(nj - 1, nk // 2, nm), VMEM, (VMEM,) * (bits - 1), flops=10**5)(*map(in_vmem, others))
    back = lax.ppermute(mine, "lon", [(i, i ^ 1) for i in range(lon_size)])
    out = call(
        functools.partial(totals_kernel, scale),
        H(nj, ni, nk, nm),
        HBM,
        (VMEM,) * 4,
        limit=4,
        scratch=(V(2, ni, nk, nm), pltpu.SemaphoreType.DMA((2,))),
        flops=10**6,
    )(*map(in_vmem, (sums, other, mine, back)))
    n_pa = in_vmem(n_pa)
    n_pb, edge_sums, edge_total = call(
        last_edge_kernel, (V(half, nk, nm), V(ni, nk, nm), V(nk, nm)), (VMEM,) * 3, (VMEM,) * 12, flops=2 * 10**6
    )(u, pa, pb, in_vmem(lat_b), in_vmem(lat_c), *lon, *lev, d_edge, f_edge, n_pa)
    others = []
    for bit in range(bits):
        others.append(partner(bit, edge_total))
        edge_total = edge_total + others[-1]
    others = tuple(map(in_vmem, others))
    end, out = call(
        functools.partial(last_totals_kernel, scale),
        (H(nj, ni, nk, nm),) * 2,
        (HBM, HBM),
        (VMEM,) * (n + 2) + (HBM, HBM),
        scratch=(V(ni, nk, nm), pltpu.SemaphoreType.DMA((5,))),
        limit=4,
        aliases={n + 2: 0, n + 3: 1},
        flops=10**6,
    )(in_vmem(edge_sums), n_pa, in_vmem(n_pb), *others, in_hbm(end), in_hbm(out))
    return out, end


def solution(mesh):
    spec = P("lat", "lon", "lev", None)
    return jax.shard_map(
        functools.partial(per_device, mesh.shape["lon"], mesh.shape["lev"]),
        mesh=mesh,
        in_specs=(spec, spec, spec),
        out_specs=(spec, spec),
        check_vma=False,
    )
```

```python
import functools

import jax
import jax.numpy as jnp
from jax import lax
from jax.experimental import pallas as pl
from jax.experimental.pallas import tpu as pltpu
from jax.sharding import PartitionSpec as P


STEPS = 4
BLOCK = 4
VMEM = pl.BlockSpec(memory_space=pltpu.VMEM)
HBM = pl.BlockSpec(memory_space=pltpu.HBM)
ANY = pl.BlockSpec(memory_space=pl.ANY)


def in_vmem(x):
    return pltpu.with_memory_space_constraint(x, pltpu.VMEM)


def in_hbm(x):
    return pltpu.with_memory_space_constraint(x, pltpu.HBM)


def new_rows(c, im, ip, nb, klo, khi, d, f):
    km = jnp.concatenate([klo, c[:-1]], axis=0)
    kp = jnp.concatenate([c[1:], khi], axis=0)
    spread = (im + ip) + nb + (km + kp) - 6.0 * c
    return c + d * spread + f


def sweep(lo, hi, row, below, above, nb, klo, khi, d, f, put, carry=None):
    def block(first, bottom, top, carry):
        rows = [bottom() if bottom else row(first - 1)]
        rows += [row(first + r) for r in range(BLOCK)]
        rows += [top() if top else row(first + BLOCK)]
        for r in range(BLOCK):
            i = first + r
            new = new_rows(rows[r + 1], rows[r], rows[r + 2], nb(i), klo(i), khi(i), d(i), f(i))
            carry = put(i, new, carry)
        return carry

    carry = block(lo, below, None, carry)

    def body(b, carry):
        return block(lo + b * BLOCK, None, None, carry)

    n = (hi - lo) // BLOCK
    carry = lax.fori_loop(1, n - 1, body, carry)
    return block(hi - BLOCK, None, above, carry)


def plane_at(depth, n):
    low = lax.axis_index("lat") == 0
    return jnp.where(low, n - 1 - depth, depth)


def odd(axis):
    return lax.axis_index(axis) % 2 == 1


def lower(axis, e, o):
    return jnp.where(odd(axis), e, o)


def upper(axis, e, o):
    return jnp.where(odd(axis), o, e)


def faces_kernel(u, lon_e, lon_o, lev_e, lev_o):
    nj, ni, nk, _ = u.shape
    at_e = jnp.where(odd("lon"), 0, ni - 1)
    for j in range(nj):
        lon_e[j] = u[j, at_e]
        lon_o[j] = u[j, ni - 1 - at_e]
        lo, hi = u[j, :, 0, :], u[j, :, nk - 1, :]
        lev_e[j] = lower("lev", lo, hi)
        lev_o[j] = upper("lev", lo, hi)


def load_kernel(u_in, d_in, f_in, u, pb, d_edge, f_edge, lon_e, lon_o, lev_e, lev_o, sem):
    nj, ni = u.shape[:2]
    q = ni // 4
    pj = plane_at(0, nj)
    copies = [pltpu.make_async_copy(u_in.at[j], u.at[j], sem.at[j]) for j in range(nj)]
    copies += [
        pltpu.make_async_copy(d_in.at[pj], d_edge, sem.at[nj]),
        pltpu.make_async_copy(f_in.at[pj], f_edge, sem.at[nj + 1]),
        pltpu.make_async_copy(u_in.at[pj, pl.ds(0, q)], pb.at[pl.ds(0, q)], sem.at[nj + 2]),
        pltpu.make_async_copy(u_in.at[pj, pl.ds(ni - q, q)], pb.at[pl.ds(q, q)], sem.at[nj + 3]),
    ]
    for copy in copies:
        copy.start()
    for copy in copies:
        copy.wait()
    faces_kernel(u, lon_e, lon_o, lev_e, lev_o)


def lev_rows(lev_e, lev_o, j, base):
    def get(side):
        def row(i):
            at = pl.ds(base + i, 1)
            return side("lev", lev_e[j, at, :], lev_o[j, at, :])

        return row

    return get(lower), get(upper)


def edge_rows(lo, hi, base, mine, below, above, u, lat, lev_e, lev_o, d, f, put):
    nj = u.shape[0]
    pj, pn = plane_at(0, nj), plane_at(1, nj)
    sweep(
        lo,
        hi,
        lambda i: mine[i],
        below,
        above,
        lambda i: u[pn, base + i] + lat[i],
        *lev_rows(lev_e, lev_o, pj, base),
        lambda i: d[base + i],
        lambda i: f[base + i],
        put,
        jnp.int32(0),
    )


def edge_a_kernel(u, pa, pb, lat, lev_e, lev_o, d, f, out):
    def put(i, new, carry):
        out[i] = new
        return carry

    n = pa.shape[0]
    edge_rows(0, n, n // 2, pa, lambda: pb[n // 2 - 1], lambda: pb[n // 2], u, lat, lev_e, lev_o, d, f, put)


def edge_b_kernel(u, pa, pb, lat, lon_e, lon_o, lev_e, lev_o, d, f, *rest):
    nj, ni, nk, _ = u.shape
    q = ni // 4
    pj = plane_at(0, nj)
    out = rest[2] if len(rest) > 1 else rest[0]

    def put(i, new, carry):
        out[i] = new
        return carry

    args = (u, lat, lev_e, lev_o, d, f, put)
    edge_rows(0, q, 0, pb, lambda: lower("lon", lon_e[pj], lon_o[pj]), lambda: pa[0], *args)
    edge_rows(q, 2 * q, 2 * q, pb, lambda: pa[2 * q - 1], lambda: upper("lon", lon_e[pj], lon_o[pj]), *args)
    if len(rest) > 1:
        nu, npa, _, s_lon_e, s_lon_o, s_lev_e, s_lev_o = rest
        faces_kernel(nu, s_lon_e, s_lon_o, s_lev_e, s_lev_o)
        s_lon_e[pj] = lower("lon", out[0], out[2 * q - 1])
        s_lon_o[pj] = upper("lon", out[0], out[2 * q - 1])
        for s_lev, side in ((s_lev_e, lower), (s_lev_o, upper)):
            s_lev[pj, :q] = side("lev", out[:q, 0, :], out[:q, nk - 1, :])
            s_lev[pj, q : 3 * q] = side("lev", npa[:, 0, :], npa[:, nk - 1, :])
            s_lev[pj, 3 * q :] = side("lev", out[q:, 0, :], out[q:, nk - 1, :])


def bulk_planes(u, pa, pb, lon_e, lon_o, lev_e, lev_o, d, f, put, start, finish):
    nj, ni, _, _ = u.shape
    q = ni // 4

    def run(j, lo, hi, nb, carry):
        return sweep(
            lo,
            hi,
            lambda i: u[j, i],
            (lambda: lower("lon", lon_e[j], lon_o[j])) if lo == 0 else None,
            (lambda: upper("lon", lon_e[j], lon_o[j])) if hi == ni else None,
            nb,
            *lev_rows(lev_e, lev_o, j, 0),
            lambda i: d[j, i],
            lambda i: f[j, i],
            functools.partial(put, j),
            carry,
        )

    j, inner = plane_at(1, nj), plane_at(2, nj)
    start(j, 1)
    carry = run(j, 0, q, lambda i: u[inner, i] + pb[i], zero_carry(u))
    carry = run(j, q, 3 * q, lambda i: u[inner, i] + pa[i - q], carry)
    carry = run(j, 3 * q, ni, lambda i: u[inner, i] + pb[i - 2 * q], carry)
    finish(j, 1, carry)

    def body(depth, _):
        j, outer, inner = plane_at(depth, nj), plane_at(depth - 1, nj), plane_at(depth + 1, nj)
        start(j, depth)
        carry = run(j, 0, ni, lambda i: u[outer, i] + u[inner, i], zero_carry(u))
        finish(j, depth, carry)
        return 0

    lax.fori_loop(2, nj - 1, body, 0)
    j, outer = plane_at(nj - 1, nj), plane_at(nj - 2, nj)
    start(j, nj - 1)
    carry = run(j, 0, ni, lambda i: u[outer, i], zero_carry(u))
    finish(j, nj - 1, carry)


def zero_carry(u):
    return jnp.zeros(u.shape[2:], u.dtype)


def nothing(*_):
    pass


def plain_put(out):
    def put(j, i, new, carry):
        out[j, i] = new
        return carry

    return put


def first_bulk_kernel(u, pa, pb, lon_e, lon_o, lev_e, lev_o, d_in, f_in, after, out, d, f, sem):
    del after
    nj = u.shape[0]

    def copies(j, depth):
        return (
            pltpu.make_async_copy(d_in.at[j], d.at[j], sem.at[0, depth]),
            pltpu.make_async_copy(f_in.at[j], f.at[j], sem.at[1, depth]),
        )

    for depth in range(1, nj):
        for copy in copies(plane_at(depth, nj), depth):
            copy.start()

    def start(j, depth):
        for copy in copies(j, depth):
            copy.wait()

    bulk_planes(u, pa, pb, lon_e, lon_o, lev_e, lev_o, d, f, plain_put(out), start, nothing)


def bulk_kernel(u, pa, pb, lon_e, lon_o, lev_e, lev_o, d, f, after, out):
    del after
    bulk_planes(u, pa, pb, lon_e, lon_o, lev_e, lev_o, d, f, plain_put(out), nothing, nothing)


def last_bulk_kernel(u, pa, pb, lon_e, lon_o, lev_e, lev_o, d_in, f_in, after, end, d, f, total, sem):
    del d_in, f_in, after
    nj = u.shape[0]

    def copy_out(j, depth):
        return pltpu.make_async_copy(f.at[j], end.at[j], sem.at[depth])

    def put(j, i, new, carry):
        f[j, i] = new
        carry = carry + new
        d[j, i] = carry
        return carry

    def finish(j, depth, carry):
        total[depth - 1] = carry
        copy_out(j, depth).start()

    bulk_planes(u, pa, pb, lon_e, lon_o, lev_e, lev_o, d, f, put, nothing, finish)
    for depth in range(1, nj):
        copy_out(plane_at(depth, nj), depth).wait()


def last_edge_kernel(u, pa, pb, lat, lon_e, lon_o, lev_e, lev_o, d, f, npa, npb, sums, total):
    edge_b_kernel(u, pa, pb, lat, lon_e, lon_o, lev_e, lev_o, d, f, npb)
    ni = sums.shape[0]
    q = ni // 4
    carry = zero_carry(u)
    for part, lo, n, base in ((npb, 0, q, 0), (npa, 0, 2 * q, q), (npb, q, q, 3 * q)):

        def row(r, carry):
            carry = carry + part[lo + r]
            sums[base + r] = carry
            return carry

        carry = lax.fori_loop(0, n, row, carry, unroll=4)
    total[...] = carry


def earlier(others):
    lon = lax.axis_index("lon")
    before = 0.0
    for bit, other in enumerate(others):
        before += jnp.where(lon & (1 << bit) != 0, other, 0.0)
    return before


def half_kernel(total, other, out):
    n = out.shape[1]
    at = pl.ds(pl.multiple_of(jnp.where(odd("lon"), n, 0), n), n)
    for p in range(out.shape[0]):
        out[p] = total[p, at] + other[p, at]


def total_rows(scale, ni, sums, before, put):
    def row(r, _):
        for q in range(BLOCK):
            i = r * BLOCK + q
            put(i, (sums(i) + before) * scale)
        return 0

    lax.fori_loop(0, ni // BLOCK, row, 0)


def half_totals(scale, upper_half, sums, other, before, out, stage, sem):
    nj, ni, nk = sums.shape[:3]
    n = nk // 2
    at = pl.ds(pl.multiple_of(jnp.where(upper_half, n, 0), n), n)

    def copy_out(depth):
        return pltpu.make_async_copy(stage.at[depth - 1], out.at[plane_at(depth, nj), :, at, :], sem.at[depth - 1])

    def body(depth, _):
        j = plane_at(depth, nj)
        b = before[depth - 1] + earlier([other[depth - 1, at]])

        def put(i, value):
            stage[depth - 1, i] = value

        total_rows(scale, ni, lambda i: sums[j, i, at], b, put)
        copy_out(depth).start()
        return 0

    lax.fori_loop(1, nj, body, 0)
    return [copy_out(depth) for depth in range(1, nj)]


def totals_kernel(scale, sums, other, before, after, out, stage, sem):
    del after
    for copy in half_totals(scale, odd("lon"), sums, other, before, out, stage, sem):
        copy.wait()


def last_totals_kernel(scale, sums, other, before, npa, npb, edge_sums, *rest):
    *others, _, _, end, out, stage, edge_stage, sem, edge_sem = rest
    nj, ni = sums.shape[:2]
    q = ni // 4
    pj = plane_at(0, nj)
    copies = [
        pltpu.make_async_copy(npb.at[pl.ds(0, q)], end.at[pj, pl.ds(0, q)], edge_sem.at[0]),
        pltpu.make_async_copy(npa, end.at[pj, pl.ds(q, 2 * q)], edge_sem.at[1]),
        pltpu.make_async_copy(npb.at[pl.ds(q, q)], end.at[pj, pl.ds(3 * q, q)], edge_sem.at[2]),
        pltpu.make_async_copy(edge_stage, out.at[pj], edge_sem.at[3]),
    ]
    for copy in copies[:3]:
        copy.start()
    copies += half_totals(scale, jnp.logical_not(odd("lon")), sums, other, before, out, stage, sem)

    def put(i, value):
        edge_stage[i] = value

    total_rows(scale, ni, lambda i: edge_sums[i], earlier([other[...] for other in others]), put)
    copies[3].start()
    for copy in copies:
        copy.wait()


def call(kernel, out_shape, out_specs, in_specs, limit=2, scratch=(), aliases=None, flops=0):
    return pl.pallas_call(
        kernel,
        out_shape=out_shape,
        in_specs=in_specs,
        out_specs=out_specs,
        scratch_shapes=scratch,
        input_output_aliases=aliases or {},
        compiler_params=pltpu.CompilerParams(vmem_limit_bytes=limit * 2**20),
        cost_estimate=pl.CostEstimate(flops=flops, transcendentals=0, bytes_accessed=0),
    )


def per_device(lon_size, lev_size, initial_state, scaled_diffusivity, scaled_forcing):
    dtype = initial_state.dtype
    nj, ni, nk, nm = initial_state.shape
    half = ni // 2
    V = lambda *shape: pltpu.VMEM(shape, dtype)
    H = lambda *shape: pltpu.HBM(shape, dtype)

    swap = [(0, 1), (1, 0)]
    faces_out = (V(nj, nk, nm), V(nj, nk, nm), V(nj, ni, nm), V(nj, ni, nm))

    def exchange(axis, size, e, o):
        def swaps(first):
            return [(a, b) for i in range(first, size - 1, 2) for a, b in ((i, i + 1), (i + 1, i))]

        return lax.ppermute(e, axis, swaps(0)), lax.ppermute(o, axis, swaps(1))

    def lon_exchange(e, o):
        return exchange("lon", lon_size, e, o)

    def lev_exchange(e, o):
        return exchange("lev", lev_size, e, o)

    def partner(bit, total):
        pairs = [(i, i ^ (1 << bit)) for i in range(lon_size)]
        if 2 << bit == lon_size:
            pairs = [(a, b) for a, b in pairs if a < b]
        return lax.ppermute(total, "lon", pairs)

    bits = lon_size.bit_length() - 1

    pj = jnp.where(lax.axis_index("lat") == 0, nj - 1, 0)
    pa = lax.dynamic_slice(initial_state, (pj, ni // 4, 0, 0), (1, half, nk, nm))[0]
    lat_a = lax.ppermute(pa, "lat", swap)
    u, pb, d_edge, f_edge, *faces = call(
        load_kernel,
        (V(nj, ni, nk, nm), V(half, nk, nm), V(ni, nk, nm), V(ni, nk, nm)) + faces_out,
        (VMEM,) * 8,
        (HBM,) * 3,
        scratch=(pltpu.SemaphoreType.DMA((nj + 4,)),),
        flops=10**6,
    )(*map(in_hbm, (initial_state, scaled_diffusivity, scaled_forcing)))
    lev = lev_exchange(*faces[2:])
    lon = lon_exchange(*faces[:2])
    lat_b = lax.ppermute(pb, "lat", swap)
    d_edge, f_edge = in_vmem(d_edge), in_vmem(f_edge)
    d, f = in_hbm(scaled_diffusivity), in_hbm(scaled_forcing)

    for step in range(STEPS):
        last = step == STEPS - 1
        u, pa, pb, lat_a, lat_b = map(in_vmem, (u, pa, pb, lat_a, lat_b))
        lon, lev = tuple(map(in_vmem, lon)), tuple(map(in_vmem, lev))
        n_pa = call(edge_a_kernel, V(half, nk, nm), VMEM, (VMEM,) * 8, flops=10**6)(
            u, pa, pb, lat_a, *lev, d_edge, f_edge
        )
        if last:
            break
        lat_a = lax.ppermute(n_pa, "lat", swap)
        if step == 0:
            n_u, d, f = call(
                first_bulk_kernel,
                (V(nj, ni, nk, nm),) * 3,
                (VMEM,) * 3,
                (VMEM,) * 7 + (HBM,) * 2 + (ANY,),
                scratch=(pltpu.SemaphoreType.DMA((2, nj)),),
                flops=2 * 10**7,
            )(u, pa, pb, *lon, *lev, d, f, n_pa)
        else:
            n_u = call(
                bulk_kernel, V(nj, ni, nk, nm), VMEM, (VMEM,) * 9 + (ANY,), flops=2 * 10**7
            )(u, pa, pb, *lon, *lev, in_vmem(d), in_vmem(f), n_pa)
        n_pb, *faces = call(
            edge_b_kernel, (V(half, nk, nm),) + faces_out, (VMEM,) * 5, (VMEM,) * 12, flops=10**6
        )(u, pa, pb, lat_b, *lon, *lev, d_edge, f_edge, in_vmem(n_u), in_vmem(n_pa))
        lon = lon_exchange(*faces[:2])
        lat_b = lax.ppermute(n_pb, "lat", swap)
        lev = lev_exchange(*faces[2:])
        u, pa, pb = n_u, n_pa, n_pb

    scale = 1.0 / (ni * lon_size)
    end, sums, _, total = call(
        last_bulk_kernel,
        (H(nj, ni, nk, nm), V(nj, ni, nk, nm), V(nj, ni, nk, nm), V(nj - 1, nk, nm)),
        (HBM, VMEM, VMEM, VMEM),
        (VMEM,) * 9 + (ANY,),
        scratch=(pltpu.SemaphoreType.DMA((nj,)),),
        aliases={7: 1, 8: 2},
        flops=2 * 10**7,
    )(u, pa, pb, *lon, *lev, in_vmem(d), in_vmem(f), n_pa)
    other = partner(0, total)
    half_total = call(half_kernel, V(nj - 1, nk // 2, nm), VMEM, (VMEM,) * 2, flops=10**5)(
        in_vmem(total), in_vmem(other)
    )
    pairs = lon_size // 2
    mine = []
    for steps in sorted(range(1, pairs), key=lambda steps: (steps % 2 == 0, steps)):
        to = [(2 * a + c, 2 * (a ^ steps) + c) for a in range(pairs) if a < a ^ steps for c in (0, 1)]
        mine.append(lax.ppermute(half_total, "lon", to))
    mine = functools.reduce(jnp.add, mine)
    back = lax.ppermute(mine, "lon", [(i, i ^ 1) for i in range(lon_size)])
    n_pa = in_vmem(n_pa)
    n_pb, edge_sums, edge_total = call(
        last_edge_kernel, (V(half, nk, nm), V(ni, nk, nm), V(nk, nm)), (VMEM,) * 3, (VMEM,) * 11, flops=2 * 10**6
    )(u, pa, pb, lat_b, *lon, *lev, d_edge, f_edge, n_pa)
    others = []
    edge_total_1 = edge_total
    for bit in range(bits):
        others.append(partner(bit, edge_total))
        edge_total = edge_total + others[-1]
    others = tuple(map(in_vmem, others))
    sums, other = in_vmem(sums), in_vmem(other)
    out = call(
        functools.partial(totals_kernel, scale),
        H(nj, ni, nk, nm),
        HBM,
        (VMEM,) * 3 + (ANY,),
        limit=5,
        scratch=(V(nj - 1, ni, nk // 2, nm), pltpu.SemaphoreType.DMA((nj - 1,))),
        flops=10**6,
    )(sums, other, in_vmem(mine), edge_total_1)
    n = 6 + bits
    end, out = call(
        functools.partial(last_totals_kernel, scale),
        (H(nj, ni, nk, nm),) * 2,
        (HBM, HBM),
        (VMEM,) * n + (HBM, HBM),
        scratch=(
            V(nj - 1, ni, nk // 2, nm),
            V(ni, nk, nm),
            pltpu.SemaphoreType.DMA((nj - 1,)),
            pltpu.SemaphoreType.DMA((4,)),
        ),
        limit=6,
        aliases={n: 0, n + 1: 1},
        flops=10**6,
    )(sums, other, in_vmem(back), n_pa, in_vmem(n_pb), in_vmem(edge_sums), *others, in_hbm(end), in_hbm(out))
    return out, end


def solution(mesh):
    spec = P("lat", "lon", "lev", None)
    return jax.shard_map(
        functools.partial(per_device, mesh.shape["lon"], mesh.shape["lev"]),
        mesh=mesh,
        in_specs=(spec, spec, spec),
        out_specs=(spec, spec),
        check_vma=False,
    )
```

```python
import functools

import jax
import jax.numpy as jnp
from jax import lax
from jax.experimental import pallas as pl
from jax.experimental.pallas import tpu as pltpu
from jax.sharding import PartitionSpec as P


STEPS = 4
BLOCK = 4
VMEM = pl.BlockSpec(memory_space=pltpu.VMEM)
HBM = pl.BlockSpec(memory_space=pltpu.HBM)
ANY = pl.BlockSpec(memory_space=pl.ANY)


def in_vmem(x):
    return pltpu.with_memory_space_constraint(x, pltpu.VMEM)


def in_hbm(x):
    return pltpu.with_memory_space_constraint(x, pltpu.HBM)


def new_rows(c, im, ip, nb, klo, khi, d, f):
    km = jnp.concatenate([klo, c[:-1]], axis=0)
    kp = jnp.concatenate([c[1:], khi], axis=0)
    spread = (im + ip) + nb + (km + kp) - 6.0 * c
    return c + d * spread + f


def sweep(lo, hi, row, below, above, nb, klo, khi, d, f, put, carry=None):
    def block(first, bottom, top, carry):
        rows = [bottom() if bottom else row(first - 1)]
        rows += [row(first + r) for r in range(BLOCK)]
        rows += [top() if top else row(first + BLOCK)]
        for r in range(BLOCK):
            i = first + r
            new = new_rows(rows[r + 1], rows[r], rows[r + 2], nb(i), klo(i), khi(i), d(i), f(i))
            carry = put(i, new, carry)
        return carry

    carry = block(lo, below, None, carry)

    def body(b, carry):
        return block(lo + b * BLOCK, None, None, carry)

    n = (hi - lo) // BLOCK
    carry = lax.fori_loop(1, n - 1, body, carry)
    return block(hi - BLOCK, None, above, carry)


def plane_at(depth, n):
    low = lax.axis_index("lat") == 0
    return jnp.where(low, n - 1 - depth, depth)


def odd(axis):
    return lax.axis_index(axis) % 2 == 1


def lower(axis, e, o):
    return jnp.where(odd(axis), e, o)


def upper(axis, e, o):
    return jnp.where(odd(axis), o, e)


def faces_kernel(u, lon_e, lon_o, lev_e, lev_o):
    nj, ni, nk, _ = u.shape
    at_e = jnp.where(odd("lon"), 0, ni - 1)
    for j in range(nj):
        lon_e[j] = u[j, at_e]
        lon_o[j] = u[j, ni - 1 - at_e]
        lo, hi = u[j, :, 0, :], u[j, :, nk - 1, :]
        lev_e[j] = lower("lev", lo, hi)
        lev_o[j] = upper("lev", lo, hi)


def load_kernel(u_in, d_in, f_in, u, pb, d_edge, f_edge, lon_e, lon_o, lev_e, lev_o, sem):
    nj, ni = u.shape[:2]
    q = ni // 4
    pj = plane_at(0, nj)
    copies = [pltpu.make_async_copy(u_in.at[j], u.at[j], sem.at[j]) for j in range(nj)]
    copies += [
        pltpu.make_async_copy(d_in.at[pj], d_edge, sem.at[nj]),
        pltpu.make_async_copy(f_in.at[pj], f_edge, sem.at[nj + 1]),
        pltpu.make_async_copy(u_in.at[pj, pl.ds(0, q)], pb.at[pl.ds(0, q)], sem.at[nj + 2]),
        pltpu.make_async_copy(u_in.at[pj, pl.ds(ni - q, q)], pb.at[pl.ds(q, q)], sem.at[nj + 3]),
    ]
    for copy in copies:
        copy.start()
    for copy in copies:
        copy.wait()
    faces_kernel(u, lon_e, lon_o, lev_e, lev_o)


def lev_rows(lev_e, lev_o, j, base):
    def get(side):
        def row(i):
            at = pl.ds(base + i, 1)
            return side("lev", lev_e[j, at, :], lev_o[j, at, :])

        return row

    return get(lower), get(upper)


def edge_rows(lo, hi, base, mine, below, above, u, lat, lev_e, lev_o, d, f, put):
    nj = u.shape[0]
    pj, pn = plane_at(0, nj), plane_at(1, nj)
    sweep(
        lo,
        hi,
        lambda i: mine[i],
        below,
        above,
        lambda i: u[pn, base + i] + lat[i],
        *lev_rows(lev_e, lev_o, pj, base),
        lambda i: d[base + i],
        lambda i: f[base + i],
        put,
        jnp.int32(0),
    )


def edge_a_kernel(u, pa, pb, lat, lev_e, lev_o, d, f, out):
    def put(i, new, carry):
        out[i] = new
        return carry

    n = pa.shape[0]
    edge_rows(0, n, n // 2, pa, lambda: pb[n // 2 - 1], lambda: pb[n // 2], u, lat, lev_e, lev_o, d, f, put)


def edge_b_kernel(u, pa, pb, lat, lon_e, lon_o, lev_e, lev_o, d, f, *rest):
    nj, ni, nk, _ = u.shape
    q = ni // 4
    pj = plane_at(0, nj)
    out = rest[2] if len(rest) > 1 else rest[0]

    def put(i, new, carry):
        out[i] = new
        return carry

    args = (u, lat, lev_e, lev_o, d, f, put)
    edge_rows(0, q, 0, pb, lambda: lower("lon", lon_e[pj], lon_o[pj]), lambda: pa[0], *args)
    edge_rows(q, 2 * q, 2 * q, pb, lambda: pa[2 * q - 1], lambda: upper("lon", lon_e[pj], lon_o[pj]), *args)
    if len(rest) > 1:
        nu, npa, _, s_lon_e, s_lon_o, s_lev_e, s_lev_o = rest
        faces_kernel(nu, s_lon_e, s_lon_o, s_lev_e, s_lev_o)
        s_lon_e[pj] = lower("lon", out[0], out[2 * q - 1])
        s_lon_o[pj] = upper("lon", out[0], out[2 * q - 1])
        for s_lev, side in ((s_lev_e, lower), (s_lev_o, upper)):
            s_lev[pj, :q] = side("lev", out[:q, 0, :], out[:q, nk - 1, :])
            s_lev[pj, q : 3 * q] = side("lev", npa[:, 0, :], npa[:, nk - 1, :])
            s_lev[pj, 3 * q :] = side("lev", out[q:, 0, :], out[q:, nk - 1, :])


def bulk_planes(u, pa, pb, lon_e, lon_o, lev_e, lev_o, d, f, put, start, finish):
    nj, ni, _, _ = u.shape
    q = ni // 4

    def run(j, lo, hi, nb, carry):
        return sweep(
            lo,
            hi,
            lambda i: u[j, i],
            (lambda: lower("lon", lon_e[j], lon_o[j])) if lo == 0 else None,
            (lambda: upper("lon", lon_e[j], lon_o[j])) if hi == ni else None,
            nb,
            *lev_rows(lev_e, lev_o, j, 0),
            lambda i: d[j, i],
            lambda i: f[j, i],
            functools.partial(put, j),
            carry,
        )

    j, inner = plane_at(1, nj), plane_at(2, nj)
    start(j, 1)
    carry = run(j, 0, q, lambda i: u[inner, i] + pb[i], zero_carry(u))
    carry = run(j, q, 3 * q, lambda i: u[inner, i] + pa[i - q], carry)
    carry = run(j, 3 * q, ni, lambda i: u[inner, i] + pb[i - 2 * q], carry)
    finish(j, 1, carry)

    def body(depth, _):
        j, outer, inner = plane_at(depth, nj), plane_at(depth - 1, nj), plane_at(depth + 1, nj)
        start(j, depth)
        carry = run(j, 0, ni, lambda i: u[outer, i] + u[inner, i], zero_carry(u))
        finish(j, depth, carry)
        return 0

    lax.fori_loop(2, nj - 1, body, 0)
    j, outer = plane_at(nj - 1, nj), plane_at(nj - 2, nj)
    start(j, nj - 1)
    carry = run(j, 0, ni, lambda i: u[outer, i], zero_carry(u))
    finish(j, nj - 1, carry)


def zero_carry(u):
    return jnp.zeros(u.shape[2:], u.dtype)


def nothing(*_):
    pass


def plain_put(out):
    def put(j, i, new, carry):
        out[j, i] = new
        return carry

    return put


def first_bulk_kernel(u, pa, pb, lon_e, lon_o, lev_e, lev_o, d_in, f_in, after, out, d, f, sem):
    del after
    nj = u.shape[0]

    def copies(j, depth):
        return (
            pltpu.make_async_copy(d_in.at[j], d.at[j], sem.at[0, depth]),
            pltpu.make_async_copy(f_in.at[j], f.at[j], sem.at[1, depth]),
        )

    for depth in range(1, nj):
        for copy in copies(plane_at(depth, nj), depth):
            copy.start()

    def start(j, depth):
        for copy in copies(j, depth):
            copy.wait()

    bulk_planes(u, pa, pb, lon_e, lon_o, lev_e, lev_o, d, f, plain_put(out), start, nothing)


def bulk_kernel(u, pa, pb, lon_e, lon_o, lev_e, lev_o, d, f, after, out):
    del after
    bulk_planes(u, pa, pb, lon_e, lon_o, lev_e, lev_o, d, f, plain_put(out), nothing, nothing)


def last_bulk_kernel(u, pa, pb, lon_e, lon_o, lev_e, lev_o, d_in, f_in, after, end, d, f, total, sem):
    del d_in, f_in, after
    nj = u.shape[0]

    def copy_out(j, depth):
        return pltpu.make_async_copy(f.at[j], end.at[j], sem.at[depth])

    def put(j, i, new, carry):
        f[j, i] = new
        carry = carry + new
        d[j, i] = carry
        return carry

    def finish(j, depth, carry):
        total[depth - 1] = carry
        copy_out(j, depth).start()

    bulk_planes(u, pa, pb, lon_e, lon_o, lev_e, lev_o, d, f, put, nothing, finish)
    for depth in range(1, nj):
        copy_out(plane_at(depth, nj), depth).wait()


def last_edge_kernel(u, pa, pb, lat, lon_e, lon_o, lev_e, lev_o, d, f, npa, npb, sums, total):
    edge_b_kernel(u, pa, pb, lat, lon_e, lon_o, lev_e, lev_o, d, f, npb)
    ni = sums.shape[0]
    q = ni // 4
    carry = zero_carry(u)
    for part, lo, n, base in ((npb, 0, q, 0), (npa, 0, 2 * q, q), (npb, q, q, 3 * q)):

        def row(r, carry):
            carry = carry + part[lo + r]
            sums[base + r] = carry
            return carry

        carry = lax.fori_loop(0, n, row, carry, unroll=4)
    total[...] = carry


def earlier(others, first=0):
    lon = lax.axis_index("lon")
    before = 0.0
    for bit, other in enumerate(others):
        before += jnp.where(lon & (1 << (first + bit)) != 0, other, 0.0)
    return before


def half_kernel(total, other, out):
    n = out.shape[1]
    at = pl.ds(pl.multiple_of(jnp.where(odd("lon"), n, 0), n), n)
    for p in range(out.shape[0]):
        out[p] = total[p, at] + other[p, at]


def before_kernel(*refs):
    *others, out = refs
    for p in range(out.shape[0]):
        out[p] = earlier([other[p] for other in others], 1)


def total_rows(scale, ni, sums, before, put):
    def row(r, _):
        for q in range(BLOCK):
            i = r * BLOCK + q
            put(i, (sums(i) + before) * scale)
        return 0

    lax.fori_loop(0, ni // BLOCK, row, 0)


def half_totals(scale, upper_half, sums, other, before, out, stage, sem):
    nj, ni, nk = sums.shape[:3]
    n = nk // 2
    at = pl.ds(pl.multiple_of(jnp.where(upper_half, n, 0), n), n)

    def copy_out(depth):
        return pltpu.make_async_copy(stage.at[depth - 1], out.at[plane_at(depth, nj), :, at, :], sem.at[depth - 1])

    def body(depth, _):
        j = plane_at(depth, nj)
        b = before[depth - 1] + earlier([other[depth - 1, at]])

        def put(i, value):
            stage[depth - 1, i] = value

        total_rows(scale, ni, lambda i: sums[j, i, at], b, put)
        copy_out(depth).start()
        return 0

    lax.fori_loop(1, nj, body, 0)
    return [copy_out(depth) for depth in range(1, nj)]


def totals_kernel(scale, sums, other, before, after, out, stage, sem):
    del after
    for copy in half_totals(scale, odd("lon"), sums, other, before, out, stage, sem):
        copy.wait()


def last_totals_kernel(scale, sums, other, before, npa, npb, edge_sums, *rest):
    *others, _, _, end, out, stage, edge_stage, sem, edge_sem = rest
    nj, ni = sums.shape[:2]
    q = ni // 4
    pj = plane_at(0, nj)
    copies = [
        pltpu.make_async_copy(npb.at[pl.ds(0, q)], end.at[pj, pl.ds(0, q)], edge_sem.at[0]),
        pltpu.make_async_copy(npa, end.at[pj, pl.ds(q, 2 * q)], edge_sem.at[1]),
        pltpu.make_async_copy(npb.at[pl.ds(q, q)], end.at[pj, pl.ds(3 * q, q)], edge_sem.at[2]),
        pltpu.make_async_copy(edge_stage, out.at[pj], edge_sem.at[3]),
    ]
    for copy in copies[:3]:
        copy.start()
    copies += half_totals(scale, jnp.logical_not(odd("lon")), sums, other, before, out, stage, sem)

    def put(i, value):
        edge_stage[i] = value

    total_rows(scale, ni, lambda i: edge_sums[i], earlier([other[...] for other in others]), put)
    copies[3].start()
    for copy in copies:
        copy.wait()


def call(kernel, out_shape, out_specs, in_specs, limit=2, scratch=(), aliases=None, flops=0):
    return pl.pallas_call(
        kernel,
        out_shape=out_shape,
        in_specs=in_specs,
        out_specs=out_specs,
        scratch_shapes=scratch,
        input_output_aliases=aliases or {},
        compiler_params=pltpu.CompilerParams(vmem_limit_bytes=limit * 2**20),
        cost_estimate=pl.CostEstimate(flops=flops, transcendentals=0, bytes_accessed=0),
    )


def per_device(lon_size, lev_size, initial_state, scaled_diffusivity, scaled_forcing):
    dtype = initial_state.dtype
    nj, ni, nk, nm = initial_state.shape
    half = ni // 2
    V = lambda *shape: pltpu.VMEM(shape, dtype)
    H = lambda *shape: pltpu.HBM(shape, dtype)

    swap = [(0, 1), (1, 0)]
    faces_out = (V(nj, nk, nm), V(nj, nk, nm), V(nj, ni, nm), V(nj, ni, nm))

    def exchange(axis, size, e, o):
        def swaps(first):
            return [(a, b) for i in range(first, size - 1, 2) for a, b in ((i, i + 1), (i + 1, i))]

        return lax.ppermute(e, axis, swaps(0)), lax.ppermute(o, axis, swaps(1))

    def lon_exchange(e, o):
        return exchange("lon", lon_size, e, o)

    def lev_exchange(e, o):
        return exchange("lev", lev_size, e, o)

    def partner(bit, total):
        pairs = [(i, i ^ (1 << bit)) for i in range(lon_size)]
        if 2 << bit == lon_size:
            pairs = [(a, b) for a, b in pairs if a < b]
        return lax.ppermute(total, "lon", pairs)

    bits = lon_size.bit_length() - 1

    pj = jnp.where(lax.axis_index("lat") == 0, nj - 1, 0)
    pa = lax.dynamic_slice(initial_state, (pj, ni // 4, 0, 0), (1, half, nk, nm))[0]
    lat_a = lax.ppermute(pa, "lat", swap)
    u, pb, d_edge, f_edge, *faces = call(
        load_kernel,
        (V(nj, ni, nk, nm), V(half, nk, nm), V(ni, nk, nm), V(ni, nk, nm)) + faces_out,
        (VMEM,) * 8,
        (HBM,) * 3,
        scratch=(pltpu.SemaphoreType.DMA((nj + 4,)),),
        flops=10**6,
    )(*map(in_hbm, (initial_state, scaled_diffusivity, scaled_forcing)))
    lev = lev_exchange(*faces[2:])
    lon = lon_exchange(*faces[:2])
    lat_b = lax.ppermute(pb, "lat", swap)
    d_edge, f_edge = in_vmem(d_edge), in_vmem(f_edge)
    d, f = in_hbm(scaled_diffusivity), in_hbm(scaled_forcing)

    for step in range(STEPS):
        last = step == STEPS - 1
        u, pa, pb, lat_a, lat_b = map(in_vmem, (u, pa, pb, lat_a, lat_b))
        lon, lev = tuple(map(in_vmem, lon)), tuple(map(in_vmem, lev))
        n_pa = call(edge_a_kernel, V(half, nk, nm), VMEM, (VMEM,) * 8, flops=10**6)(
            u, pa, pb, lat_a, *lev, d_edge, f_edge
        )
        if last:
            break
        lat_a = lax.ppermute(n_pa, "lat", swap)
        if step == 0:
            n_u, d, f = call(
                first_bulk_kernel,
                (V(nj, ni, nk, nm),) * 3,
                (VMEM,) * 3,
                (VMEM,) * 7 + (HBM,) * 2 + (ANY,),
                scratch=(pltpu.SemaphoreType.DMA((2, nj)),),
                flops=2 * 10**7,
            )(u, pa, pb, *lon, *lev, d, f, n_pa)
        else:
            n_u = call(
                bulk_kernel, V(nj, ni, nk, nm), VMEM, (VMEM,) * 9 + (ANY,), flops=2 * 10**7
            )(u, pa, pb, *lon, *lev, in_vmem(d), in_vmem(f), n_pa)
        n_pb, *faces = call(
            edge_b_kernel, (V(half, nk, nm),) + faces_out, (VMEM,) * 5, (VMEM,) * 12, flops=10**6
        )(u, pa, pb, lat_b, *lon, *lev, d_edge, f_edge, in_vmem(n_u), in_vmem(n_pa))
        lon = lon_exchange(*faces[:2])
        lat_b = lax.ppermute(n_pb, "lat", swap)
        lev = lev_exchange(*faces[2:])
        u, pa, pb = n_u, n_pa, n_pb

    scale = 1.0 / (ni * lon_size)
    end, sums, _, total = call(
        last_bulk_kernel,
        (H(nj, ni, nk, nm), V(nj, ni, nk, nm), V(nj, ni, nk, nm), V(nj - 1, nk, nm)),
        (HBM, VMEM, VMEM, VMEM),
        (VMEM,) * 9 + (ANY,),
        scratch=(pltpu.SemaphoreType.DMA((nj,)),),
        aliases={7: 1, 8: 2},
        flops=2 * 10**7,
    )(u, pa, pb, *lon, *lev, in_vmem(d), in_vmem(f), n_pa)
    other = partner(0, total)
    half_total = call(half_kernel, V(nj - 1, nk // 2, nm), VMEM, (VMEM,) * 2, flops=10**5)(
        in_vmem(total), in_vmem(other)
    )
    later = []
    for bit in range(1, bits):
        later.append(partner(bit, half_total))
        half_total = half_total + later[-1]
    mine = call(before_kernel, V(nj - 1, nk // 2, nm), VMEM, (VMEM,) * (bits - 1), flops=10**5)(*map(in_vmem, later))
    back = lax.ppermute(mine, "lon", [(i, i ^ 1) for i in range(lon_size)])
    n_pa = in_vmem(n_pa)
    n_pb, edge_sums, edge_total = call(
        last_edge_kernel, (V(half, nk, nm), V(ni, nk, nm), V(nk, nm)), (VMEM,) * 3, (VMEM,) * 11, flops=2 * 10**6
    )(u, pa, pb, lat_b, *lon, *lev, d_edge, f_edge, n_pa)
    others = []
    edge_total_1 = edge_total
    for bit in range(bits):
        others.append(partner(bit, edge_total))
        edge_total = edge_total + others[-1]
    others = tuple(map(in_vmem, others))
    sums, other = in_vmem(sums), in_vmem(other)
    out = call(
        functools.partial(totals_kernel, scale),
        H(nj, ni, nk, nm),
        HBM,
        (VMEM,) * 3 + (ANY,),
        limit=5,
        scratch=(V(nj - 1, ni, nk // 2, nm), pltpu.SemaphoreType.DMA((nj - 1,))),
        flops=10**6,
    )(sums, other, in_vmem(mine), edge_total_1)
    n = 6 + bits
    end, out = call(
        functools.partial(last_totals_kernel, scale),
        (H(nj, ni, nk, nm),) * 2,
        (HBM, HBM),
        (VMEM,) * n + (HBM, HBM),
        scratch=(
            V(nj - 1, ni, nk // 2, nm),
            V(ni, nk, nm),
            pltpu.SemaphoreType.DMA((nj - 1,)),
            pltpu.SemaphoreType.DMA((4,)),
        ),
        limit=6,
        aliases={n: 0, n + 1: 1},
        flops=10**6,
    )(sums, other, in_vmem(back), n_pa, in_vmem(n_pb), in_vmem(edge_sums), *others, in_hbm(end), in_hbm(out))
    return out, end


def solution(mesh):
    spec = P("lat", "lon", "lev", None)
    return jax.shard_map(
        functools.partial(per_device, mesh.shape["lon"], mesh.shape["lev"]),
        mesh=mesh,
        in_specs=(spec, spec, spec),
        out_specs=(spec, spec),
        check_vma=False,
    )
```

```python
import functools

import jax
import jax.numpy as jnp
from jax import lax
from jax.experimental import pallas as pl
from jax.experimental.pallas import tpu as pltpu
from jax.sharding import PartitionSpec as P


STEPS = 4
BLOCK = 4
VMEM = pl.BlockSpec(memory_space=pltpu.VMEM)
HBM = pl.BlockSpec(memory_space=pltpu.HBM)
ANY = pl.BlockSpec(memory_space=pl.ANY)


def in_vmem(x):
    return pltpu.with_memory_space_constraint(x, pltpu.VMEM)


def in_hbm(x):
    return pltpu.with_memory_space_constraint(x, pltpu.HBM)


def new_rows(c, im, ip, nb, klo, khi, d, f):
    km = jnp.concatenate([klo, c[:-1]], axis=0)
    kp = jnp.concatenate([c[1:], khi], axis=0)
    spread = (im + ip) + nb + (km + kp) - 6.0 * c
    return c + d * spread + f


def sweep(lo, hi, row, below, above, nb, klo, khi, d, f, put, carry=None):
    def block(first, bottom, top, carry):
        rows = [bottom() if bottom else row(first - 1)]
        rows += [row(first + r) for r in range(BLOCK)]
        rows += [top() if top else row(first + BLOCK)]
        for r in range(BLOCK):
            i = first + r
            new = new_rows(rows[r + 1], rows[r], rows[r + 2], nb(i), klo(i), khi(i), d(i), f(i))
            carry = put(i, new, carry)
        return carry

    carry = block(lo, below, None, carry)

    def body(b, carry):
        return block(lo + b * BLOCK, None, None, carry)

    n = (hi - lo) // BLOCK
    carry = lax.fori_loop(1, n - 1, body, carry)
    return block(hi - BLOCK, None, above, carry)


def plane_at(depth, n):
    low = lax.axis_index("lat") == 0
    return jnp.where(low, n - 1 - depth, depth)


def odd(axis):
    return lax.axis_index(axis) % 2 == 1


def lower(axis, e, o):
    return jnp.where(odd(axis), e, o)


def upper(axis, e, o):
    return jnp.where(odd(axis), o, e)


def faces_kernel(u, lon_e, lon_o, lev_e, lev_o):
    nj, ni, nk, _ = u.shape
    at_e = jnp.where(odd("lon"), 0, ni - 1)
    for j in range(nj):
        lon_e[j] = u[j, at_e]
        lon_o[j] = u[j, ni - 1 - at_e]
        lo, hi = u[j, :, 0, :], u[j, :, nk - 1, :]
        lev_e[j] = lower("lev", lo, hi)
        lev_o[j] = upper("lev", lo, hi)


def load_kernel(u_in, d_in, f_in, u, pb, d_edge, f_edge, lon_e, lon_o, lev_e, lev_o, sem):
    nj, ni = u.shape[:2]
    q = ni // 4
    pj = plane_at(0, nj)
    copies = [pltpu.make_async_copy(u_in.at[j], u.at[j], sem.at[j]) for j in range(nj)]
    copies += [
        pltpu.make_async_copy(d_in.at[pj], d_edge, sem.at[nj]),
        pltpu.make_async_copy(f_in.at[pj], f_edge, sem.at[nj + 1]),
        pltpu.make_async_copy(u_in.at[pj, pl.ds(0, q)], pb.at[pl.ds(0, q)], sem.at[nj + 2]),
        pltpu.make_async_copy(u_in.at[pj, pl.ds(ni - q, q)], pb.at[pl.ds(q, q)], sem.at[nj + 3]),
    ]
    for copy in copies:
        copy.start()
    for copy in copies:
        copy.wait()
    faces_kernel(u, lon_e, lon_o, lev_e, lev_o)


def lev_rows(lev_e, lev_o, j, base):
    def get(side):
        def row(i):
            at = pl.ds(base + i, 1)
            return side("lev", lev_e[j, at, :], lev_o[j, at, :])

        return row

    return get(lower), get(upper)


def edge_rows(lo, hi, base, mine, below, above, u, lat, lev_e, lev_o, d, f, put):
    nj = u.shape[0]
    pj, pn = plane_at(0, nj), plane_at(1, nj)
    sweep(
        lo,
        hi,
        lambda i: mine[i],
        below,
        above,
        lambda i: u[pn, base + i] + lat[i],
        *lev_rows(lev_e, lev_o, pj, base),
        lambda i: d[base + i],
        lambda i: f[base + i],
        put,
        jnp.int32(0),
    )


def edge_a_kernel(u, pa, pb, lat, lev_e, lev_o, d, f, out):
    def put(i, new, carry):
        out[i] = new
        return carry

    n = pa.shape[0]
    edge_rows(0, n, n // 2, pa, lambda: pb[n // 2 - 1], lambda: pb[n // 2], u, lat, lev_e, lev_o, d, f, put)


def edge_b_kernel(u, pa, pb, lat, lon_e, lon_o, lev_e, lev_o, d, f, *rest):
    nj, ni, nk, _ = u.shape
    q = ni // 4
    pj = plane_at(0, nj)
    out = rest[2] if len(rest) > 1 else rest[0]

    def put(i, new, carry):
        out[i] = new
        return carry

    args = (u, lat, lev_e, lev_o, d, f, put)
    edge_rows(0, q, 0, pb, lambda: lower("lon", lon_e[pj], lon_o[pj]), lambda: pa[0], *args)
    edge_rows(q, 2 * q, 2 * q, pb, lambda: pa[2 * q - 1], lambda: upper("lon", lon_e[pj], lon_o[pj]), *args)
    if len(rest) > 1:
        nu, npa, _, s_lon_e, s_lon_o, s_lev_e, s_lev_o = rest
        faces_kernel(nu, s_lon_e, s_lon_o, s_lev_e, s_lev_o)
        s_lon_e[pj] = lower("lon", out[0], out[2 * q - 1])
        s_lon_o[pj] = upper("lon", out[0], out[2 * q - 1])
        for s_lev, side in ((s_lev_e, lower), (s_lev_o, upper)):
            s_lev[pj, :q] = side("lev", out[:q, 0, :], out[:q, nk - 1, :])
            s_lev[pj, q : 3 * q] = side("lev", npa[:, 0, :], npa[:, nk - 1, :])
            s_lev[pj, 3 * q :] = side("lev", out[q:, 0, :], out[q:, nk - 1, :])


def bulk_planes(u, pa, pb, lon_e, lon_o, lev_e, lev_o, d, f, put, start, finish):
    nj, ni, _, _ = u.shape
    q = ni // 4

    def run(j, lo, hi, nb, carry):
        return sweep(
            lo,
            hi,
            lambda i: u[j, i],
            (lambda: lower("lon", lon_e[j], lon_o[j])) if lo == 0 else None,
            (lambda: upper("lon", lon_e[j], lon_o[j])) if hi == ni else None,
            nb,
            *lev_rows(lev_e, lev_o, j, 0),
            lambda i: d[j, i],
            lambda i: f[j, i],
            functools.partial(put, j),
            carry,
        )

    j, inner = plane_at(1, nj), plane_at(2, nj)
    start(j, 1)
    carry = run(j, 0, q, lambda i: u[inner, i] + pb[i], zero_carry(u))
    carry = run(j, q, 3 * q, lambda i: u[inner, i] + pa[i - q], carry)
    carry = run(j, 3 * q, ni, lambda i: u[inner, i] + pb[i - 2 * q], carry)
    finish(j, 1, carry)

    def body(depth, _):
        j, outer, inner = plane_at(depth, nj), plane_at(depth - 1, nj), plane_at(depth + 1, nj)
        start(j, depth)
        carry = run(j, 0, ni, lambda i: u[outer, i] + u[inner, i], zero_carry(u))
        finish(j, depth, carry)
        return 0

    lax.fori_loop(2, nj - 1, body, 0)
    j, outer = plane_at(nj - 1, nj), plane_at(nj - 2, nj)
    start(j, nj - 1)
    carry = run(j, 0, ni, lambda i: u[outer, i], zero_carry(u))
    finish(j, nj - 1, carry)


def zero_carry(u):
    return jnp.zeros(u.shape[2:], u.dtype)


def nothing(*_):
    pass


def plain_put(out):
    def put(j, i, new, carry):
        out[j, i] = new
        return carry

    return put


def first_bulk_kernel(u, pa, pb, lon_e, lon_o, lev_e, lev_o, d_in, f_in, after, out, d, f, sem):
    del after
    nj = u.shape[0]

    def copies(j, depth):
        return (
            pltpu.make_async_copy(d_in.at[j], d.at[j], sem.at[0, depth]),
            pltpu.make_async_copy(f_in.at[j], f.at[j], sem.at[1, depth]),
        )

    for depth in range(1, nj):
        for copy in copies(plane_at(depth, nj), depth):
            copy.start()

    def start(j, depth):
        for copy in copies(j, depth):
            copy.wait()

    bulk_planes(u, pa, pb, lon_e, lon_o, lev_e, lev_o, d, f, plain_put(out), start, nothing)


def bulk_kernel(u, pa, pb, lon_e, lon_o, lev_e, lev_o, d, f, after, out):
    del after
    bulk_planes(u, pa, pb, lon_e, lon_o, lev_e, lev_o, d, f, plain_put(out), nothing, nothing)


def last_bulk_kernel(u, pa, pb, lon_e, lon_o, lev_e, lev_o, d_in, f_in, after, end, d, f, total, sem):
    del d_in, f_in, after
    nj = u.shape[0]

    def copy_out(j, depth):
        return pltpu.make_async_copy(f.at[j], end.at[j], sem.at[depth])

    def put(j, i, new, carry):
        f[j, i] = new
        carry = carry + new
        d[j, i] = carry
        return carry

    def finish(j, depth, carry):
        total[depth - 1] = carry
        copy_out(j, depth).start()

    bulk_planes(u, pa, pb, lon_e, lon_o, lev_e, lev_o, d, f, put, nothing, finish)
    for depth in range(1, nj):
        copy_out(plane_at(depth, nj), depth).wait()


def last_edge_kernel(u, pa, pb, lat, lon_e, lon_o, lev_e, lev_o, d, f, npa, npb, sums, total):
    edge_b_kernel(u, pa, pb, lat, lon_e, lon_o, lev_e, lev_o, d, f, npb)
    ni = sums.shape[0]
    q = ni // 4
    carry = zero_carry(u)
    for part, lo, n, base in ((npb, 0, q, 0), (npa, 0, 2 * q, q), (npb, q, q, 3 * q)):

        def row(r, carry):
            carry = carry + part[lo + r]
            sums[base + r] = carry
            return carry

        carry = lax.fori_loop(0, n, row, carry, unroll=4)
    total[...] = carry


def low_pair():
    return lax.axis_index("lon") & 2 == 0


def half_kernel(total, other, out, low):
    n = out.shape[1]
    at = pl.ds(pl.multiple_of(jnp.where(odd("lon"), n, 0), n), n)
    for p in range(out.shape[0]):
        out[p] = total[p, at] + other[p, at]
        low[p] = jnp.where(low_pair(), out[p], 0.0)


def pair_kernel(total, other, out, low):
    out[...] = total[...] + other[...]
    low[...] = jnp.where(low_pair(), out[...], 0.0)


def total_rows(scale, ni, sums, before, put):
    def row(r, _):
        for q in range(BLOCK):
            i = r * BLOCK + q
            put(i, (sums(i) + before) * scale)
        return 0

    lax.fori_loop(0, ni // BLOCK, row, 0)


def half_totals(scale, upper_half, sums, other, before, out, stage, sem):
    nj, ni, nk = sums.shape[:3]
    n = nk // 2
    at = pl.ds(pl.multiple_of(jnp.where(upper_half, n, 0), n), n)

    def copy_out(depth):
        return pltpu.make_async_copy(stage.at[depth - 1], out.at[plane_at(depth, nj), :, at, :], sem.at[depth - 1])

    def body(depth, _):
        j = plane_at(depth, nj)
        b = before[depth - 1] + jnp.where(odd("lon"), other[depth - 1, at], 0.0)

        def put(i, value):
            stage[depth - 1, i] = value

        total_rows(scale, ni, lambda i: sums[j, i, at], b, put)
        copy_out(depth).start()
        return 0

    lax.fori_loop(1, nj, body, 0)
    return [copy_out(depth) for depth in range(1, nj)]


def totals_kernel(scale, sums, other, before, npa, npb, end_in, end, out, stage, sem, edge_sem):
    del end_in
    nj, ni = sums.shape[:2]
    q = ni // 4
    pj = plane_at(0, nj)
    copies = [
        pltpu.make_async_copy(npb.at[pl.ds(0, q)], end.at[pj, pl.ds(0, q)], edge_sem.at[0]),
        pltpu.make_async_copy(npa, end.at[pj, pl.ds(q, 2 * q)], edge_sem.at[1]),
        pltpu.make_async_copy(npb.at[pl.ds(q, q)], end.at[pj, pl.ds(3 * q, q)], edge_sem.at[2]),
    ]
    for copy in copies:
        copy.start()
    copies += half_totals(scale, odd("lon"), sums, other, before, out, stage, sem)
    for copy in copies:
        copy.wait()


def last_totals_kernel(scale, sums, other, before, edge_sums, edge_other, edge_before, out_in, out, stage, edge_stage, sem, edge_sem):
    del out_in
    nj, ni = sums.shape[:2]
    pj = plane_at(0, nj)

    def put(i, value):
        edge_stage[i] = value

    b = edge_before[...] + jnp.where(odd("lon"), edge_other[...], 0.0)
    total_rows(scale, ni, lambda i: edge_sums[i], b, put)
    copies = [pltpu.make_async_copy(edge_stage, out.at[pj], edge_sem)]
    copies[0].start()
    copies += half_totals(scale, jnp.logical_not(odd("lon")), sums, other, before, out, stage, sem)
    for copy in copies:
        copy.wait()


def call(kernel, out_shape, out_specs, in_specs, limit=2, scratch=(), aliases=None, flops=0):
    return pl.pallas_call(
        kernel,
        out_shape=out_shape,
        in_specs=in_specs,
        out_specs=out_specs,
        scratch_shapes=scratch,
        input_output_aliases=aliases or {},
        compiler_params=pltpu.CompilerParams(vmem_limit_bytes=limit * 2**20),
        cost_estimate=pl.CostEstimate(flops=flops, transcendentals=0, bytes_accessed=0),
    )


def per_device(lon_size, lev_size, initial_state, scaled_diffusivity, scaled_forcing):
    dtype = initial_state.dtype
    nj, ni, nk, nm = initial_state.shape
    half = ni // 2
    V = lambda *shape: pltpu.VMEM(shape, dtype)
    H = lambda *shape: pltpu.HBM(shape, dtype)

    swap = [(0, 1), (1, 0)]
    faces_out = (V(nj, nk, nm), V(nj, nk, nm), V(nj, ni, nm), V(nj, ni, nm))

    def exchange(axis, size, e, o):
        def swaps(first):
            return [(a, b) for i in range(first, size - 1, 2) for a, b in ((i, i + 1), (i + 1, i))]

        return lax.ppermute(e, axis, swaps(0)), lax.ppermute(o, axis, swaps(1))

    def lon_exchange(e, o):
        return exchange("lon", lon_size, e, o)

    def lev_exchange(e, o):
        return exchange("lev", lev_size, e, o)

    core_swap = [(i, i ^ 1) for i in range(lon_size)]

    def earlier(kernel, total, other, shape):
        total, low = call(kernel, (V(*shape),) * 2, (VMEM,) * 2, (VMEM,) * 2, flops=10**5)(
            in_vmem(total), in_vmem(other)
        )
        far = lax.ppermute(total, "lon", [(i, i + 4) for i in range(4)])
        near = lax.ppermute(low + far, "lon", [(i, i ^ 2) for i in range(lon_size) if i & 2 == 0 or i & 4])
        return far + near

    pj = jnp.where(lax.axis_index("lat") == 0, nj - 1, 0)
    pa = lax.dynamic_slice(initial_state, (pj, ni // 4, 0, 0), (1, half, nk, nm))[0]
    lat_a = lax.ppermute(pa, "lat", swap)
    u, pb, d_edge, f_edge, *faces = call(
        load_kernel,
        (V(nj, ni, nk, nm), V(half, nk, nm), V(ni, nk, nm), V(ni, nk, nm)) + faces_out,
        (VMEM,) * 8,
        (HBM,) * 3,
        scratch=(pltpu.SemaphoreType.DMA((nj + 4,)),),
        flops=10**6,
    )(*map(in_hbm, (initial_state, scaled_diffusivity, scaled_forcing)))
    lev = lev_exchange(*faces[2:])
    lon = lon_exchange(*faces[:2])
    lat_b = lax.ppermute(pb, "lat", swap)
    d_edge, f_edge = in_vmem(d_edge), in_vmem(f_edge)
    d, f = in_hbm(scaled_diffusivity), in_hbm(scaled_forcing)

    for step in range(STEPS):
        last = step == STEPS - 1
        u, pa, pb, lat_a, lat_b = map(in_vmem, (u, pa, pb, lat_a, lat_b))
        lon, lev = tuple(map(in_vmem, lon)), tuple(map(in_vmem, lev))
        n_pa = call(edge_a_kernel, V(half, nk, nm), VMEM, (VMEM,) * 8, flops=10**6)(
            u, pa, pb, lat_a, *lev, d_edge, f_edge
        )
        if last:
            break
        lat_a = lax.ppermute(n_pa, "lat", swap)
        if step == 0:
            n_u, d, f = call(
                first_bulk_kernel,
                (V(nj, ni, nk, nm),) * 3,
                (VMEM,) * 3,
                (VMEM,) * 7 + (HBM,) * 2 + (ANY,),
                scratch=(pltpu.SemaphoreType.DMA((2, nj)),),
                flops=2 * 10**7,
            )(u, pa, pb, *lon, *lev, d, f, n_pa)
        else:
            n_u = call(
                bulk_kernel, V(nj, ni, nk, nm), VMEM, (VMEM,) * 9 + (ANY,), flops=2 * 10**7
            )(u, pa, pb, *lon, *lev, in_vmem(d), in_vmem(f), n_pa)
        n_pb, *faces = call(
            edge_b_kernel, (V(half, nk, nm),) + faces_out, (VMEM,) * 5, (VMEM,) * 12, flops=10**6
        )(u, pa, pb, lat_b, *lon, *lev, d_edge, f_edge, in_vmem(n_u), in_vmem(n_pa))
        lon = lon_exchange(*faces[:2])
        lat_b = lax.ppermute(n_pb, "lat", swap)
        lev = lev_exchange(*faces[2:])
        u, pa, pb = n_u, n_pa, n_pb

    scale = 1.0 / (ni * lon_size)
    end, sums, _, total = call(
        last_bulk_kernel,
        (H(nj, ni, nk, nm), V(nj, ni, nk, nm), V(nj, ni, nk, nm), V(nj - 1, nk, nm)),
        (HBM, VMEM, VMEM, VMEM),
        (VMEM,) * 9 + (ANY,),
        scratch=(pltpu.SemaphoreType.DMA((nj,)),),
        aliases={7: 1, 8: 2},
        flops=2 * 10**7,
    )(u, pa, pb, *lon, *lev, in_vmem(d), in_vmem(f), n_pa)
    other = lax.ppermute(total, "lon", core_swap)
    mine = earlier(half_kernel, total, other, (nj - 1, nk // 2, nm))
    back = lax.ppermute(mine, "lon", core_swap)
    n_pa = in_vmem(n_pa)
    n_pb, edge_sums, edge_total = call(
        last_edge_kernel, (V(half, nk, nm), V(ni, nk, nm), V(nk, nm)), (VMEM,) * 3, (VMEM,) * 11, flops=2 * 10**6
    )(u, pa, pb, lat_b, *lon, *lev, d_edge, f_edge, n_pa)
    edge_other = lax.ppermute(edge_total, "lon", core_swap)
    edge_before = earlier(pair_kernel, edge_total, edge_other, (nk, nm))
    sums, other = in_vmem(sums), in_vmem(other)
    end, out = call(
        functools.partial(totals_kernel, scale),
        (H(nj, ni, nk, nm),) * 2,
        (HBM, HBM),
        (VMEM,) * 5 + (HBM,),
        limit=5,
        scratch=(
            V(nj - 1, ni, nk // 2, nm),
            pltpu.SemaphoreType.DMA((nj - 1,)),
            pltpu.SemaphoreType.DMA((3,)),
        ),
        aliases={5: 0},
        flops=10**6,
    )(sums, other, in_vmem(mine), n_pa, in_vmem(n_pb), in_hbm(end))
    out = call(
        functools.partial(last_totals_kernel, scale),
        H(nj, ni, nk, nm),
        HBM,
        (VMEM,) * 6 + (HBM,),
        scratch=(
            V(nj - 1, ni, nk // 2, nm),
            V(ni, nk, nm),
            pltpu.SemaphoreType.DMA((nj - 1,)),
            pltpu.SemaphoreType.DMA,
        ),
        limit=6,
        aliases={6: 0},
        flops=10**6,
    )(sums, other, *map(in_vmem, (back, edge_sums, edge_other, edge_before)), in_hbm(out))
    return out, end


def solution(mesh):
    spec = P("lat", "lon", "lev", None)
    return jax.shard_map(
        functools.partial(per_device, mesh.shape["lon"], mesh.shape["lev"]),
        mesh=mesh,
        in_specs=(spec, spec, spec),
        out_specs=(spec, spec),
        check_vma=False,
    )
```

```python
import functools

import jax
import jax.numpy as jnp
from jax import lax
from jax.experimental import pallas as pl
from jax.experimental.pallas import tpu as pltpu
from jax.sharding import PartitionSpec as P


STEPS = 4
BLOCK = 4
VMEM = pl.BlockSpec(memory_space=pltpu.VMEM)
HBM = pl.BlockSpec(memory_space=pltpu.HBM)
ANY = pl.BlockSpec(memory_space=pl.ANY)


def in_vmem(x):
    return pltpu.with_memory_space_constraint(x, pltpu.VMEM)


def in_hbm(x):
    return pltpu.with_memory_space_constraint(x, pltpu.HBM)


def new_rows(c, im, ip, nb, klo, khi, d, f):
    km = jnp.concatenate([klo, c[:-1]], axis=0)
    kp = jnp.concatenate([c[1:], khi], axis=0)
    spread = (im + ip) + nb + (km + kp) - 6.0 * c
    return c + d * spread + f


def sweep(lo, hi, row, below, above, nb, klo, khi, d, f, put, carry=None):
    def block(first, bottom, top, carry):
        rows = [bottom() if bottom else row(first - 1)]
        rows += [row(first + r) for r in range(BLOCK)]
        rows += [top() if top else row(first + BLOCK)]
        for r in range(BLOCK):
            i = first + r
            new = new_rows(rows[r + 1], rows[r], rows[r + 2], nb(i), klo(i), khi(i), d(i), f(i))
            carry = put(i, new, carry)
        return carry

    carry = block(lo, below, None, carry)

    def body(b, carry):
        return block(lo + b * BLOCK, None, None, carry)

    n = (hi - lo) // BLOCK
    carry = lax.fori_loop(1, n - 1, body, carry)
    return block(hi - BLOCK, None, above, carry)


def plane_at(depth, n):
    low = lax.axis_index("lat") == 0
    return jnp.where(low, n - 1 - depth, depth)


def odd(axis):
    return lax.axis_index(axis) % 2 == 1


def lower(axis, e, o):
    return jnp.where(odd(axis), e, o)


def upper(axis, e, o):
    return jnp.where(odd(axis), o, e)


def across(j, whole, half, relayed):
    return whole[j] + jnp.concatenate([half[j], relayed[j]], axis=0)


def faces_kernel(u, lon_e, lon_o, lon_h, lon_r, lev_e, lev_o):
    nj, ni, nk, _ = u.shape
    at_e = jnp.where(odd("lon"), 0, ni - 1)
    for j in range(nj):
        lon_e[j] = u[j, at_e]
        lon_o[j] = u[j, ni - 1 - at_e]
        lon_h[j] = u[j, ni - 1 - at_e, : nk // 2]
        lon_r[j] = u[j, ni - 1 - at_e, nk // 2 :]
        lo, hi = u[j, :, 0, :], u[j, :, nk - 1, :]
        lev_e[j] = lower("lev", lo, hi)
        lev_o[j] = upper("lev", lo, hi)


def load_kernel(u_in, d_in, f_in, u, pb, d_edge, f_edge, lon_e, lon_o, lon_h, lon_r, lev_e, lev_o, sem):
    nj, ni = u.shape[:2]
    q = ni // 4
    pj = plane_at(0, nj)
    copies = [pltpu.make_async_copy(u_in.at[j], u.at[j], sem.at[j]) for j in range(nj)]
    copies += [
        pltpu.make_async_copy(d_in.at[pj], d_edge, sem.at[nj]),
        pltpu.make_async_copy(f_in.at[pj], f_edge, sem.at[nj + 1]),
        pltpu.make_async_copy(u_in.at[pj, pl.ds(0, q)], pb.at[pl.ds(0, q)], sem.at[nj + 2]),
        pltpu.make_async_copy(u_in.at[pj, pl.ds(ni - q, q)], pb.at[pl.ds(q, q)], sem.at[nj + 3]),
    ]
    for copy in copies:
        copy.start()
    for copy in copies:
        copy.wait()
    faces_kernel(u, lon_e, lon_o, lon_h, lon_r, lev_e, lev_o)


def lev_rows(lev_e, lev_o, j, base):
    def get(side):
        def row(i):
            at = pl.ds(base + i, 1)
            return side("lev", lev_e[j, at, :], lev_o[j, at, :])

        return row

    return get(lower), get(upper)


def edge_rows(lo, hi, base, mine, below, above, u, lat, lev_e, lev_o, d, f, put):
    nj = u.shape[0]
    pj, pn = plane_at(0, nj), plane_at(1, nj)
    sweep(
        lo,
        hi,
        lambda i: mine[i],
        below,
        above,
        lambda i: u[pn, base + i] + lat[i],
        *lev_rows(lev_e, lev_o, pj, base),
        lambda i: d[base + i],
        lambda i: f[base + i],
        put,
        jnp.int32(0),
    )


def edge_a_kernel(u, pa, pb, lat, lev_e, lev_o, d, f, out):
    def put(i, new, carry):
        out[i] = new
        return carry

    n = pa.shape[0]
    edge_rows(0, n, n // 2, pa, lambda: pb[n // 2 - 1], lambda: pb[n // 2], u, lat, lev_e, lev_o, d, f, put)


def edge_b_kernel(u, pa, pb, lat, lon_e, lon_o, lon_h, lon_r, lev_e, lev_o, d, f, *rest):
    nj, ni, nk, _ = u.shape
    q = ni // 4
    pj = plane_at(0, nj)
    out = rest[2] if len(rest) > 1 else rest[0]

    def put(i, new, carry):
        out[i] = new
        return carry

    args = (u, lat, lev_e, lev_o, d, f, put)
    edge_rows(0, q, 0, pb, lambda: lower("lon", lon_e[pj], across(pj, lon_o, lon_h, lon_r)), lambda: pa[0], *args)
    edge_rows(q, 2 * q, 2 * q, pb, lambda: pa[2 * q - 1], lambda: upper("lon", lon_e[pj], across(pj, lon_o, lon_h, lon_r)), *args)
    if len(rest) > 1:
        nu, npa, _, s_lon_e, s_lon_o, s_lon_h, s_lon_r, s_lev_e, s_lev_o = rest
        faces_kernel(nu, s_lon_e, s_lon_o, s_lon_h, s_lon_r, s_lev_e, s_lev_o)
        s_lon_e[pj] = lower("lon", out[0], out[2 * q - 1])
        s_lon_o[pj] = upper("lon", out[0], out[2 * q - 1])
        s_lon_h[pj] = upper("lon", out[0, : nk // 2], out[2 * q - 1, : nk // 2])
        s_lon_r[pj] = upper("lon", out[0, nk // 2 :], out[2 * q - 1, nk // 2 :])
        for s_lev, side in ((s_lev_e, lower), (s_lev_o, upper)):
            s_lev[pj, :q] = side("lev", out[:q, 0, :], out[:q, nk - 1, :])
            s_lev[pj, q : 3 * q] = side("lev", npa[:, 0, :], npa[:, nk - 1, :])
            s_lev[pj, 3 * q :] = side("lev", out[q:, 0, :], out[q:, nk - 1, :])


def bulk_planes(u, pa, pb, lon_e, lon_o, lon_h, lon_r, lev_e, lev_o, d, f, put, start, finish):
    nj, ni, _, _ = u.shape
    q = ni // 4

    def run(j, lo, hi, nb, carry):
        return sweep(
            lo,
            hi,
            lambda i: u[j, i],
            (lambda: lower("lon", lon_e[j], across(j, lon_o, lon_h, lon_r))) if lo == 0 else None,
            (lambda: upper("lon", lon_e[j], across(j, lon_o, lon_h, lon_r))) if hi == ni else None,
            nb,
            *lev_rows(lev_e, lev_o, j, 0),
            lambda i: d[j, i],
            lambda i: f[j, i],
            functools.partial(put, j),
            carry,
        )

    j, inner = plane_at(1, nj), plane_at(2, nj)
    start(j, 1)
    carry = run(j, 0, q, lambda i: u[inner, i] + pb[i], zero_carry(u))
    carry = run(j, q, 3 * q, lambda i: u[inner, i] + pa[i - q], carry)
    carry = run(j, 3 * q, ni, lambda i: u[inner, i] + pb[i - 2 * q], carry)
    finish(j, 1, carry)

    def body(depth, _):
        j, outer, inner = plane_at(depth, nj), plane_at(depth - 1, nj), plane_at(depth + 1, nj)
        start(j, depth)
        carry = run(j, 0, ni, lambda i: u[outer, i] + u[inner, i], zero_carry(u))
        finish(j, depth, carry)
        return 0

    lax.fori_loop(2, nj - 1, body, 0)
    j, outer = plane_at(nj - 1, nj), plane_at(nj - 2, nj)
    start(j, nj - 1)
    carry = run(j, 0, ni, lambda i: u[outer, i], zero_carry(u))
    finish(j, nj - 1, carry)


def zero_carry(u):
    return jnp.zeros(u.shape[2:], u.dtype)


def nothing(*_):
    pass


def plain_put(out):
    def put(j, i, new, carry):
        out[j, i] = new
        return carry

    return put


def first_bulk_kernel(u, pa, pb, lon_e, lon_o, lon_h, lon_r, lev_e, lev_o, d_in, f_in, after, out, d, f, sem):
    del after
    nj = u.shape[0]

    def copies(j, depth):
        return (
            pltpu.make_async_copy(d_in.at[j], d.at[j], sem.at[0, depth]),
            pltpu.make_async_copy(f_in.at[j], f.at[j], sem.at[1, depth]),
        )

    for depth in range(1, nj):
        for copy in copies(plane_at(depth, nj), depth):
            copy.start()

    def start(j, depth):
        for copy in copies(j, depth):
            copy.wait()

    bulk_planes(u, pa, pb, lon_e, lon_o, lon_h, lon_r, lev_e, lev_o, d, f, plain_put(out), start, nothing)


def bulk_kernel(u, pa, pb, lon_e, lon_o, lon_h, lon_r, lev_e, lev_o, d, f, after, out):
    del after
    bulk_planes(u, pa, pb, lon_e, lon_o, lon_h, lon_r, lev_e, lev_o, d, f, plain_put(out), nothing, nothing)


def last_bulk_kernel(u, pa, pb, lon_e, lon_o, lon_h, lon_r, lev_e, lev_o, d_in, f_in, after, end, d, f, total, sem):
    del d_in, f_in, after
    nj = u.shape[0]

    def copy_out(j, depth):
        return pltpu.make_async_copy(f.at[j], end.at[j], sem.at[depth])

    def put(j, i, new, carry):
        f[j, i] = new
        carry = carry + new
        d[j, i] = carry
        return carry

    def finish(j, depth, carry):
        total[depth - 1] = carry
        copy_out(j, depth).start()

    bulk_planes(u, pa, pb, lon_e, lon_o, lon_h, lon_r, lev_e, lev_o, d, f, put, nothing, finish)
    for depth in range(1, nj):
        copy_out(plane_at(depth, nj), depth).wait()


def last_edge_kernel(u, pa, pb, lat, lon_e, lon_o, lon_h, lon_r, lev_e, lev_o, d, f, npa, npb, sums, total):
    edge_b_kernel(u, pa, pb, lat, lon_e, lon_o, lon_h, lon_r, lev_e, lev_o, d, f, npb)
    ni = sums.shape[0]
    q = ni // 4
    carry = zero_carry(u)
    for part, lo, n, base in ((npb, 0, q, 0), (npa, 0, 2 * q, q), (npb, q, q, 3 * q)):

        def row(r, carry):
            carry = carry + part[lo + r]
            sums[base + r] = carry
            return carry

        carry = lax.fori_loop(0, n, row, carry, unroll=4)
    total[...] = carry


def earlier(others, first=0):
    lon = lax.axis_index("lon")
    before = 0.0
    for bit, other in enumerate(others):
        before += jnp.where(lon & (1 << (first + bit)) != 0, other, 0.0)
    return before


def half_kernel(total, other, out):
    n = out.shape[1]
    at = pl.ds(pl.multiple_of(jnp.where(odd("lon"), n, 0), n), n)
    for p in range(out.shape[0]):
        out[p] = total[p, at] + other[p, at]


def before_kernel(*refs):
    *others, out = refs
    for p in range(out.shape[0]):
        out[p] = earlier([other[p] for other in others], 1)


def total_rows(scale, ni, sums, before, put):
    def row(r, _):
        for q in range(BLOCK):
            i = r * BLOCK + q
            put(i, (sums(i) + before) * scale)
        return 0

    lax.fori_loop(0, ni // BLOCK, row, 0)


def half_totals(scale, upper_half, sums, other, before, out, stage, sem):
    nj, ni, nk = sums.shape[:3]
    n = nk // 2
    at = pl.ds(pl.multiple_of(jnp.where(upper_half, n, 0), n), n)

    def copy_out(depth):
        return pltpu.make_async_copy(stage.at[depth - 1], out.at[plane_at(depth, nj), :, at, :], sem.at[depth - 1])

    def body(depth, _):
        j = plane_at(depth, nj)
        b = before[depth - 1] + earlier([other[depth - 1, at]])

        def put(i, value):
            stage[depth - 1, i] = value

        total_rows(scale, ni, lambda i: sums[j, i, at], b, put)
        copy_out(depth).start()
        return 0

    lax.fori_loop(1, nj, body, 0)
    return [copy_out(depth) for depth in range(1, nj)]


def totals_kernel(scale, sums, other, before, after, out, stage, sem):
    del after
    for copy in half_totals(scale, odd("lon"), sums, other, before, out, stage, sem):
        copy.wait()


def last_totals_kernel(scale, sums, other, before, npa, npb, edge_sums, *rest):
    *others, _, _, end, out, stage, edge_stage, sem, edge_sem = rest
    nj, ni = sums.shape[:2]
    q = ni // 4
    pj = plane_at(0, nj)
    copies = [
        pltpu.make_async_copy(npb.at[pl.ds(0, q)], end.at[pj, pl.ds(0, q)], edge_sem.at[0]),
        pltpu.make_async_copy(npa, end.at[pj, pl.ds(q, 2 * q)], edge_sem.at[1]),
        pltpu.make_async_copy(npb.at[pl.ds(q, q)], end.at[pj, pl.ds(3 * q, q)], edge_sem.at[2]),
        pltpu.make_async_copy(edge_stage, out.at[pj], edge_sem.at[3]),
    ]
    for copy in copies[:3]:
        copy.start()
    copies += half_totals(scale, jnp.logical_not(odd("lon")), sums, other, before, out, stage, sem)

    def put(i, value):
        edge_stage[i] = value

    total_rows(scale, ni, lambda i: edge_sums[i], earlier([other[...] for other in others]), put)
    copies[3].start()
    for copy in copies:
        copy.wait()


def call(kernel, out_shape, out_specs, in_specs, limit=2, scratch=(), aliases=None, flops=0):
    return pl.pallas_call(
        kernel,
        out_shape=out_shape,
        in_specs=in_specs,
        out_specs=out_specs,
        scratch_shapes=scratch,
        input_output_aliases=aliases or {},
        compiler_params=pltpu.CompilerParams(vmem_limit_bytes=limit * 2**20),
        cost_estimate=pl.CostEstimate(flops=flops, transcendentals=0, bytes_accessed=0),
    )


def per_device(lon_size, lev_size, initial_state, scaled_diffusivity, scaled_forcing):
    dtype = initial_state.dtype
    nj, ni, nk, nm = initial_state.shape
    half = ni // 2
    V = lambda *shape: pltpu.VMEM(shape, dtype)
    H = lambda *shape: pltpu.HBM(shape, dtype)

    swap = [(0, 1), (1, 0)]
    faces_out = (V(nj, nk, nm),) * 2 + (V(nj, nk // 2, nm),) * 2 + (V(nj, ni, nm),) * 2

    def swaps(*pairs):
        return [(a, b) for p in pairs for a, b in (p, p[::-1])]

    def lon_exchange(e, o, o_half, o_rest):
        e = lax.ppermute(e, "lon", swaps((0, 1), (2, 3), (4, 5), (6, 7)))
        o_rest = lax.ppermute(o_rest, "lon", [(3, 7), (4, 0)])
        o = lax.ppermute(o, "lon", swaps((1, 2), (5, 6)))
        o_half = lax.ppermute(o_half, "lon", swaps((3, 4)))
        o_rest = lax.ppermute(o_rest, "lon", [(7, 4), (0, 3)])
        return e, o, o_half, o_rest

    def lev_exchange(e, o):
        e_pairs, o_pairs = ([(i, i + 1) for i in range(first, lev_size - 1, 2)] for first in (0, 1))
        return lax.ppermute(e, "lev", swaps(*e_pairs)), lax.ppermute(o, "lev", swaps(*o_pairs))

    def partner(bit, total):
        pairs = [(i, i ^ (1 << bit)) for i in range(lon_size)]
        if 2 << bit == lon_size:
            pairs = [(a, b) for a, b in pairs if a < b]
        return lax.ppermute(total, "lon", pairs)

    bits = lon_size.bit_length() - 1

    pj = jnp.where(lax.axis_index("lat") == 0, nj - 1, 0)
    pa = lax.dynamic_slice(initial_state, (pj, ni // 4, 0, 0), (1, half, nk, nm))[0]
    lat_a = lax.ppermute(pa, "lat", swap)
    u, pb, d_edge, f_edge, *faces = call(
        load_kernel,
        (V(nj, ni, nk, nm), V(half, nk, nm), V(ni, nk, nm), V(ni, nk, nm)) + faces_out,
        (VMEM,) * 10,
        (HBM,) * 3,
        scratch=(pltpu.SemaphoreType.DMA((nj + 4,)),),
        flops=10**6,
    )(*map(in_hbm, (initial_state, scaled_diffusivity, scaled_forcing)))
    lon = lon_exchange(*faces[:4])
    lat_b = lax.ppermute(pb, "lat", swap)
    lev = lev_exchange(*faces[4:])
    d_edge, f_edge = in_vmem(d_edge), in_vmem(f_edge)
    d, f = in_hbm(scaled_diffusivity), in_hbm(scaled_forcing)

    for step in range(STEPS):
        last = step == STEPS - 1
        u, pa, pb, lat_a, lat_b = map(in_vmem, (u, pa, pb, lat_a, lat_b))
        lon, lev = tuple(map(in_vmem, lon)), tuple(map(in_vmem, lev))
        n_pa = call(edge_a_kernel, V(half, nk, nm), VMEM, (VMEM,) * 8, flops=10**6)(
            u, pa, pb, lat_a, *lev, d_edge, f_edge
        )
        if last:
            break
        lat_a = lax.ppermute(n_pa, "lat", swap)
        if step == 0:
            n_u, d, f = call(
                first_bulk_kernel,
                (V(nj, ni, nk, nm),) * 3,
                (VMEM,) * 3,
                (VMEM,) * 9 + (HBM,) * 2 + (ANY,),
                scratch=(pltpu.SemaphoreType.DMA((2, nj)),),
                flops=2 * 10**7,
            )(u, pa, pb, *lon, *lev, d, f, n_pa)
        else:
            n_u = call(
                bulk_kernel, V(nj, ni, nk, nm), VMEM, (VMEM,) * 11 + (ANY,), flops=2 * 10**7
            )(u, pa, pb, *lon, *lev, in_vmem(d), in_vmem(f), n_pa)
        n_pb, *faces = call(
            edge_b_kernel, (V(half, nk, nm),) + faces_out, (VMEM,) * 7, (VMEM,) * 14, flops=10**6
        )(u, pa, pb, lat_b, *lon, *lev, d_edge, f_edge, in_vmem(n_u), in_vmem(n_pa))
        lon = lon_exchange(*faces[:4])
        lat_b = lax.ppermute(n_pb, "lat", swap)
        lev = lev_exchange(*faces[4:])
        u, pa, pb = n_u, n_pa, n_pb

    scale = 1.0 / (ni * lon_size)
    end, sums, _, total = call(
        last_bulk_kernel,
        (H(nj, ni, nk, nm), V(nj, ni, nk, nm), V(nj, ni, nk, nm), V(nj - 1, nk, nm)),
        (HBM, VMEM, VMEM, VMEM),
        (VMEM,) * 11 + (ANY,),
        scratch=(pltpu.SemaphoreType.DMA((nj,)),),
        aliases={9: 1, 10: 2},
        flops=2 * 10**7,
    )(u, pa, pb, *lon, *lev, in_vmem(d), in_vmem(f), n_pa)
    other = partner(0, total)
    half_total = call(half_kernel, V(nj - 1, nk // 2, nm), VMEM, (VMEM,) * 2, flops=10**5)(
        in_vmem(total), in_vmem(other)
    )
    later = []
    for bit in range(1, bits):
        later.append(partner(bit, half_total))
        half_total = half_total + later[-1]
    mine = call(before_kernel, V(nj - 1, nk // 2, nm), VMEM, (VMEM,) * (bits - 1), flops=10**5)(*map(in_vmem, later))
    back = lax.ppermute(mine, "lon", [(i, i ^ 1) for i in range(lon_size)])
    n_pa = in_vmem(n_pa)
    n_pb, edge_sums, edge_total = call(
        last_edge_kernel, (V(half, nk, nm), V(ni, nk, nm), V(nk, nm)), (VMEM,) * 3, (VMEM,) * 13, flops=2 * 10**6
    )(u, pa, pb, lat_b, *lon, *lev, d_edge, f_edge, n_pa)
    others = []
    edge_total_1 = edge_total
    for bit in range(bits):
        others.append(partner(bit, edge_total))
        edge_total = edge_total + others[-1]
    others = tuple(map(in_vmem, others))
    sums, other = in_vmem(sums), in_vmem(other)
    out = call(
        functools.partial(totals_kernel, scale),
        H(nj, ni, nk, nm),
        HBM,
        (VMEM,) * 3 + (ANY,),
        limit=5,
        scratch=(V(nj - 1, ni, nk // 2, nm), pltpu.SemaphoreType.DMA((nj - 1,))),
        flops=10**6,
    )(sums, other, in_vmem(mine), edge_total_1)
    n = 6 + bits
    end, out = call(
        functools.partial(last_totals_kernel, scale),
        (H(nj, ni, nk, nm),) * 2,
        (HBM, HBM),
        (VMEM,) * n + (HBM, HBM),
        scratch=(
            V(nj - 1, ni, nk // 2, nm),
            V(ni, nk, nm),
            pltpu.SemaphoreType.DMA((nj - 1,)),
            pltpu.SemaphoreType.DMA((4,)),
        ),
        limit=6,
        aliases={n: 0, n + 1: 1},
        flops=10**6,
    )(sums, other, in_vmem(back), n_pa, in_vmem(n_pb), in_vmem(edge_sums), *others, in_hbm(end), in_hbm(out))
    return out, end


def solution(mesh):
    spec = P("lat", "lon", "lev", None)
    return jax.shard_map(
        functools.partial(per_device, mesh.shape["lon"], mesh.shape["lev"]),
        mesh=mesh,
        in_specs=(spec, spec, spec),
        out_specs=(spec, spec),
        check_vma=False,
    )
```

```python
import functools

import jax
import jax.numpy as jnp
from jax import lax
from jax.experimental import pallas as pl
from jax.experimental.pallas import tpu as pltpu
from jax.sharding import PartitionSpec as P


STEPS = 4
LATE = 2
BLOCK = 4
VMEM = pl.BlockSpec(memory_space=pltpu.VMEM)
HBM = pl.BlockSpec(memory_space=pltpu.HBM)
ANY = pl.BlockSpec(memory_space=pl.ANY)


def in_vmem(x):
    return pltpu.with_memory_space_constraint(x, pltpu.VMEM)


def in_hbm(x):
    return pltpu.with_memory_space_constraint(x, pltpu.HBM)


def new_rows(c, im, ip, nb, klo, khi, d, f):
    km = jnp.concatenate([klo, c[:-1]], axis=0)
    kp = jnp.concatenate([c[1:], khi], axis=0)
    spread = (im + ip) + nb + (km + kp) - 6.0 * c
    return c + d * spread + f


def sweep(lo, hi, row, below, above, nb, klo, khi, d, f, put, carry=None):
    def block(first, bottom, top, carry):
        rows = [bottom() if bottom else row(first - 1)]
        rows += [row(first + r) for r in range(BLOCK)]
        rows += [top() if top else row(first + BLOCK)]
        for r in range(BLOCK):
            i = first + r
            new = new_rows(rows[r + 1], rows[r], rows[r + 2], nb(i), klo(i), khi(i), d(i), f(i))
            carry = put(i, new, carry)
        return carry

    carry = block(lo, below, None, carry)

    def body(b, carry):
        return block(lo + b * BLOCK, None, None, carry)

    n = (hi - lo) // BLOCK
    carry = lax.fori_loop(1, n - 1, body, carry)
    return block(hi - BLOCK, None, above, carry)


def plane_at(depth, n):
    low = lax.axis_index("lat") == 0
    return jnp.where(low, n - 1 - depth, depth)


def odd(axis):
    return lax.axis_index(axis) % 2 == 1


def lower(axis, e, o):
    return jnp.where(odd(axis), e, o)


def upper(axis, e, o):
    return jnp.where(odd(axis), o, e)


def faces_kernel(u, lon_e, lon_o, lev_e, lev_o):
    nj, ni, nk, _ = u.shape
    at_e = jnp.where(odd("lon"), 0, ni - 1)
    for j in range(nj):
        lon_e[j] = u[j, at_e]
        lon_o[j] = u[j, ni - 1 - at_e]
        lo, hi = u[j, :, 0, :], u[j, :, nk - 1, :]
        lev_e[j] = lower("lev", lo, hi)
        lev_o[j] = upper("lev", lo, hi)


def load_a_kernel(u_in, pa, sem):
    n = pa.shape[0]
    copy = pltpu.make_async_copy(u_in.at[plane_at(0, u_in.shape[0]), pl.ds(n // 2, n)], pa, sem)
    copy.start()
    copy.wait()


def load_kernel(u_in, d_in, f_in, u, pb, d_edge, f_edge, lon_e, lon_o, lev_e, lev_o, sem):
    nj, ni = u.shape[:2]
    q = ni // 4
    pj = plane_at(0, nj)
    copies = [pltpu.make_async_copy(u_in.at[j], u.at[j], sem.at[j]) for j in range(nj)]
    copies += [
        pltpu.make_async_copy(d_in.at[pj], d_edge, sem.at[nj]),
        pltpu.make_async_copy(f_in.at[pj], f_edge, sem.at[nj + 1]),
        pltpu.make_async_copy(u_in.at[pj, pl.ds(0, q)], pb.at[pl.ds(0, q)], sem.at[nj + 2]),
        pltpu.make_async_copy(u_in.at[pj, pl.ds(ni - q, q)], pb.at[pl.ds(q, q)], sem.at[nj + 3]),
    ]
    for copy in copies:
        copy.start()
    for copy in copies:
        copy.wait()
    faces_kernel(u, lon_e, lon_o, lev_e, lev_o)


def lev_rows(lev_e, lev_o, j, base):
    def get(side):
        def row(i):
            at = pl.ds(base + i, 1)
            return side("lev", lev_e[j, at, :], lev_o[j, at, :])

        return row

    return get(lower), get(upper)


def edge_rows(lo, hi, base, mine, below, above, u, lat, lev_e, lev_o, d, f, put):
    nj = u.shape[0]
    pj, pn = plane_at(0, nj), plane_at(1, nj)
    sweep(
        lo,
        hi,
        lambda i: mine[i],
        below,
        above,
        lambda i: u[pn, base + i] + lat[i],
        *lev_rows(lev_e, lev_o, pj, base),
        lambda i: d[base + i],
        lambda i: f[base + i],
        put,
        jnp.int32(0),
    )


def edge_a_kernel(u, pa, pb, lat, lev_e, lev_o, d, f, out):
    def put(i, new, carry):
        out[i] = new
        return carry

    n = pa.shape[0]
    edge_rows(0, n, n // 2, pa, lambda: pb[n // 2 - 1], lambda: pb[n // 2], u, lat, lev_e, lev_o, d, f, put)


def edge_b_kernel(u, pa, pb, lat, lon_e, lon_o, lev_e, lev_o, d, f, *rest):
    nj, ni, nk, _ = u.shape
    q = ni // 4
    pj = plane_at(0, nj)
    out = rest[2] if len(rest) > 1 else rest[0]

    def put(i, new, carry):
        out[i] = new
        return carry

    args = (u, lat, lev_e, lev_o, d, f, put)
    edge_rows(0, q, 0, pb, lambda: lower("lon", lon_e[pj], lon_o[pj]), lambda: pa[0], *args)
    edge_rows(q, 2 * q, 2 * q, pb, lambda: pa[2 * q - 1], lambda: upper("lon", lon_e[pj], lon_o[pj]), *args)
    if len(rest) > 1:
        nu, npa, _, s_lon_e, s_lon_o, s_lev_e, s_lev_o = rest
        faces_kernel(nu, s_lon_e, s_lon_o, s_lev_e, s_lev_o)
        s_lon_e[pj] = lower("lon", out[0], out[2 * q - 1])
        s_lon_o[pj] = upper("lon", out[0], out[2 * q - 1])
        for s_lev, side in ((s_lev_e, lower), (s_lev_o, upper)):
            s_lev[pj, :q] = side("lev", out[:q, 0, :], out[:q, nk - 1, :])
            s_lev[pj, q : 3 * q] = side("lev", npa[:, 0, :], npa[:, nk - 1, :])
            s_lev[pj, 3 * q :] = side("lev", out[q:, 0, :], out[q:, nk - 1, :])


def bulk_planes(u, pa, pb, lon_e, lon_o, lev_e, lev_o, d, f, put, start, finish):
    nj, ni, _, _ = u.shape
    q = ni // 4

    def run(j, lo, hi, nb, carry):
        return sweep(
            lo,
            hi,
            lambda i: u[j, i],
            (lambda: lower("lon", lon_e[j], lon_o[j])) if lo == 0 else None,
            (lambda: upper("lon", lon_e[j], lon_o[j])) if hi == ni else None,
            nb,
            *lev_rows(lev_e, lev_o, j, 0),
            lambda i: d[j, i],
            lambda i: f[j, i],
            functools.partial(put, j),
            carry,
        )

    j, inner = plane_at(1, nj), plane_at(2, nj)
    start(j, 1)
    carry = run(j, 0, q, lambda i: u[inner, i] + pb[i], zero_carry(u))
    carry = run(j, q, 3 * q, lambda i: u[inner, i] + pa[i - q], carry)
    carry = run(j, 3 * q, ni, lambda i: u[inner, i] + pb[i - 2 * q], carry)
    finish(j, 1, carry)

    def body(depth, _):
        j, outer, inner = plane_at(depth, nj), plane_at(depth - 1, nj), plane_at(depth + 1, nj)
        start(j, depth)
        carry = run(j, 0, ni, lambda i: u[outer, i] + u[inner, i], zero_carry(u))
        finish(j, depth, carry)
        return 0

    lax.fori_loop(2, nj - 1, body, 0)
    j, outer = plane_at(nj - 1, nj), plane_at(nj - 2, nj)
    start(j, nj - 1)
    carry = run(j, 0, ni, lambda i: u[outer, i], zero_carry(u))
    finish(j, nj - 1, carry)


def zero_carry(u):
    return jnp.zeros(u.shape[2:], u.dtype)


def nothing(*_):
    pass


def plain_put(out):
    def put(j, i, new, carry):
        out[j, i] = new
        return carry

    return put


def first_bulk_kernel(u, pa, pb, lon_e, lon_o, lev_e, lev_o, d_in, f_in, after, out, d, f, sem):
    del after
    nj = u.shape[0]

    def copies(j, depth):
        return (
            pltpu.make_async_copy(d_in.at[j], d.at[j], sem.at[0, depth]),
            pltpu.make_async_copy(f_in.at[j], f.at[j], sem.at[1, depth]),
        )

    for depth in range(1, nj):
        for copy in copies(plane_at(depth, nj), depth):
            copy.start()

    def start(j, depth):
        for copy in copies(j, depth):
            copy.wait()

    bulk_planes(u, pa, pb, lon_e, lon_o, lev_e, lev_o, d, f, plain_put(out), start, nothing)


def bulk_kernel(u, pa, pb, lon_e, lon_o, lev_e, lev_o, d, f, after, out):
    del after
    bulk_planes(u, pa, pb, lon_e, lon_o, lev_e, lev_o, d, f, plain_put(out), nothing, nothing)


def last_bulk_kernel(u, pa, pb, lon_e, lon_o, lev_e, lev_o, d_in, f_in, after, end, d, f, total, sem):
    del d_in, f_in, after
    nj = u.shape[0]

    def copy_out(j, depth):
        return pltpu.make_async_copy(f.at[j], end.at[j], sem.at[depth])

    def put(j, i, new, carry):
        f[j, i] = new
        carry = carry + new
        d[j, i] = carry
        return carry

    def finish(j, depth, carry):
        total[depth - 1] = carry

        @pl.when(depth < nj - LATE)
        def _():
            copy_out(j, depth).start()

    bulk_planes(u, pa, pb, lon_e, lon_o, lev_e, lev_o, d, f, put, nothing, finish)
    for depth in range(1, nj - LATE):
        copy_out(plane_at(depth, nj), depth).wait()


def late_kernel(f, end_in, end, sem):
    del end_in
    nj = f.shape[0]
    copies = []
    for p in range(LATE):
        j = plane_at(nj - LATE + p, nj)
        copies.append(pltpu.make_async_copy(f.at[j], end.at[j], sem.at[p]))
        copies[-1].start()
    for copy in copies:
        copy.wait()


def last_edge_kernel(u, pa, pb, lat, lon_e, lon_o, lev_e, lev_o, d, f, npa, after, npb, sums, total):
    del after
    edge_b_kernel(u, pa, pb, lat, lon_e, lon_o, lev_e, lev_o, d, f, npb)
    ni = sums.shape[0]
    q = ni // 4
    carry = zero_carry(u)
    for part, lo, n, base in ((npb, 0, q, 0), (npa, 0, 2 * q, q), (npb, q, q, 3 * q)):

        def row(r, carry):
            carry = carry + part[lo + r]
            sums[base + r] = carry
            return carry

        carry = lax.fori_loop(0, n, row, carry, unroll=4)
    total[...] = carry


def earlier(others, first=0):
    lon = lax.axis_index("lon")
    before = 0.0
    for bit, other in enumerate(others):
        before += jnp.where(lon & (1 << (first + bit)) != 0, other, 0.0)
    return before


def half_kernel(total, other, out):
    n = out.shape[1]
    at = pl.ds(pl.multiple_of(jnp.where(odd("lon"), n, 0), n), n)
    for p in range(out.shape[0]):
        out[p] = total[p, at] + other[p, at]


def before_kernel(*refs):
    *others, out = refs
    for p in range(out.shape[0]):
        out[p] = earlier([other[p] for other in others], 1)


def total_rows(scale, ni, sums, before, put):
    def row(r, _):
        for q in range(BLOCK):
            i = r * BLOCK + q
            put(i, (sums(i) + before) * scale)
        return 0

    lax.fori_loop(0, ni // BLOCK, row, 0)


def half_totals(scale, upper_half, sums, other, before, out, stage, sem):
    nj, ni, nk = sums.shape[:3]
    n = nk // 2
    at = pl.ds(pl.multiple_of(jnp.where(upper_half, n, 0), n), n)

    def copy_out(depth):
        return pltpu.make_async_copy(stage.at[depth - 1], out.at[plane_at(depth, nj), :, at, :], sem.at[depth - 1])

    def body(depth, _):
        j = plane_at(depth, nj)
        b = before[depth - 1] + earlier([other[depth - 1, at]])

        def put(i, value):
            stage[depth - 1, i] = value

        total_rows(scale, ni, lambda i: sums[j, i, at], b, put)
        copy_out(depth).start()
        return 0

    lax.fori_loop(1, nj, body, 0)
    return [copy_out(depth) for depth in range(1, nj)]


def totals_kernel(scale, sums, other, before, after, out, stage, sem):
    del after
    for copy in half_totals(scale, odd("lon"), sums, other, before, out, stage, sem):
        copy.wait()


def last_totals_kernel(scale, sums, other, before, npa, npb, edge_sums, *rest):
    *others, _, _, end, out, stage, edge_stage, sem, edge_sem = rest
    nj, ni = sums.shape[:2]
    q = ni // 4
    pj = plane_at(0, nj)
    copies = [
        pltpu.make_async_copy(npb.at[pl.ds(0, q)], end.at[pj, pl.ds(0, q)], edge_sem.at[0]),
        pltpu.make_async_copy(npa, end.at[pj, pl.ds(q, 2 * q)], edge_sem.at[1]),
        pltpu.make_async_copy(npb.at[pl.ds(q, q)], end.at[pj, pl.ds(3 * q, q)], edge_sem.at[2]),
        pltpu.make_async_copy(edge_stage, out.at[pj], edge_sem.at[3]),
    ]
    for copy in copies[:3]:
        copy.start()
    copies += half_totals(scale, jnp.logical_not(odd("lon")), sums, other, before, out, stage, sem)

    def put(i, value):
        edge_stage[i] = value

    total_rows(scale, ni, lambda i: edge_sums[i], earlier([other[...] for other in others]), put)
    copies[3].start()
    for copy in copies:
        copy.wait()


def call(kernel, out_shape, out_specs, in_specs, limit=2, scratch=(), aliases=None, flops=0):
    return pl.pallas_call(
        kernel,
        out_shape=out_shape,
        in_specs=in_specs,
        out_specs=out_specs,
        scratch_shapes=scratch,
        input_output_aliases=aliases or {},
        compiler_params=pltpu.CompilerParams(vmem_limit_bytes=limit * 2**20),
        cost_estimate=pl.CostEstimate(flops=flops, transcendentals=0, bytes_accessed=0),
    )


def per_device(lon_size, lev_size, initial_state, scaled_diffusivity, scaled_forcing):
    dtype = initial_state.dtype
    nj, ni, nk, nm = initial_state.shape
    half = ni // 2
    V = lambda *shape: pltpu.VMEM(shape, dtype)
    H = lambda *shape: pltpu.HBM(shape, dtype)

    swap = [(0, 1), (1, 0)]
    faces_out = (V(nj, nk, nm), V(nj, nk, nm), V(nj, ni, nm), V(nj, ni, nm))

    def exchange(axis, size, e, o):
        def swaps(first):
            return [(a, b) for i in range(first, size - 1, 2) for a, b in ((i, i + 1), (i + 1, i))]

        return lax.ppermute(e, axis, swaps(0)), lax.ppermute(o, axis, swaps(1))

    def lon_exchange(e, o):
        return exchange("lon", lon_size, e, o)

    def lev_exchange(e, o):
        return exchange("lev", lev_size, e, o)

    def partner(bit, total):
        pairs = [(i, i ^ (1 << bit)) for i in range(lon_size)]
        if 2 << bit == lon_size:
            pairs = [(a, b) for a, b in pairs if a < b]
        return lax.ppermute(total, "lon", pairs)

    bits = lon_size.bit_length() - 1

    pa = call(
        load_a_kernel, V(half, nk, nm), VMEM, (HBM,), scratch=(pltpu.SemaphoreType.DMA,), flops=10**5
    )(in_hbm(initial_state))
    lat_a = lax.ppermute(pa, "lat", swap)
    u, pb, d_edge, f_edge, *faces = call(
        load_kernel,
        (V(nj, ni, nk, nm), V(half, nk, nm), V(ni, nk, nm), V(ni, nk, nm)) + faces_out,
        (VMEM,) * 8,
        (HBM,) * 3,
        scratch=(pltpu.SemaphoreType.DMA((nj + 4,)),),
        flops=10**6,
    )(*map(in_hbm, (initial_state, scaled_diffusivity, scaled_forcing)))
    lon = lon_exchange(*faces[:2])
    lat_b = lax.ppermute(pb, "lat", swap)
    lev = lev_exchange(*faces[2:])
    d_edge, f_edge = in_vmem(d_edge), in_vmem(f_edge)
    d, f = in_hbm(scaled_diffusivity), in_hbm(scaled_forcing)

    for step in range(STEPS):
        last = step == STEPS - 1
        u, pa, pb, lat_a, lat_b = map(in_vmem, (u, pa, pb, lat_a, lat_b))
        lon, lev = tuple(map(in_vmem, lon)), tuple(map(in_vmem, lev))
        n_pa = call(edge_a_kernel, V(half, nk, nm), VMEM, (VMEM,) * 8, flops=10**6)(
            u, pa, pb, lat_a, *lev, d_edge, f_edge
        )
        if last:
            break
        lat_a = lax.ppermute(n_pa, "lat", swap)
        if step == 0:
            n_u, d, f = call(
                first_bulk_kernel,
                (V(nj, ni, nk, nm),) * 3,
                (VMEM,) * 3,
                (VMEM,) * 7 + (HBM,) * 2 + (ANY,),
                scratch=(pltpu.SemaphoreType.DMA((2, nj)),),
                flops=2 * 10**7,
            )(u, pa, pb, *lon, *lev, d, f, n_pa)
        else:
            n_u = call(
                bulk_kernel, V(nj, ni, nk, nm), VMEM, (VMEM,) * 9 + (ANY,), flops=2 * 10**7
            )(u, pa, pb, *lon, *lev, in_vmem(d), in_vmem(f), n_pa)
        n_pb, *faces = call(
            edge_b_kernel, (V(half, nk, nm),) + faces_out, (VMEM,) * 5, (VMEM,) * 12, flops=10**6
        )(u, pa, pb, lat_b, *lon, *lev, d_edge, f_edge, in_vmem(n_u), in_vmem(n_pa))
        lon = lon_exchange(*faces[:2])
        lat_b = lax.ppermute(n_pb, "lat", swap)
        lev = lev_exchange(*faces[2:])
        u, pa, pb = n_u, n_pa, n_pb

    scale = 1.0 / (ni * lon_size)
    end, sums, values, total = call(
        last_bulk_kernel,
        (H(nj, ni, nk, nm), V(nj, ni, nk, nm), V(nj, ni, nk, nm), V(nj - 1, nk, nm)),
        (HBM, VMEM, VMEM, VMEM),
        (VMEM,) * 9 + (ANY,),
        scratch=(pltpu.SemaphoreType.DMA((nj,)),),
        aliases={7: 1, 8: 2},
        flops=2 * 10**7,
    )(u, pa, pb, *lon, *lev, in_vmem(d), in_vmem(f), n_pa)
    other = partner(0, total)
    end = call(
        late_kernel,
        H(nj, ni, nk, nm),
        HBM,
        (VMEM, HBM),
        scratch=(pltpu.SemaphoreType.DMA((LATE,)),),
        aliases={1: 0},
        flops=10**5,
    )(in_vmem(values), in_hbm(end))
    half_total = call(half_kernel, V(nj - 1, nk // 2, nm), VMEM, (VMEM,) * 2, flops=10**5)(
        in_vmem(total), in_vmem(other)
    )
    later = []
    for bit in range(1, bits):
        later.append(partner(bit, half_total))
        half_total = half_total + later[-1]
    mine = call(before_kernel, V(nj - 1, nk // 2, nm), VMEM, (VMEM,) * (bits - 1), flops=10**5)(*map(in_vmem, later))
    back = lax.ppermute(mine, "lon", [(i, i ^ 1) for i in range(lon_size)])
    n_pa = in_vmem(n_pa)
    n_pb, edge_sums, edge_total = call(
        last_edge_kernel,
        (V(half, nk, nm), V(ni, nk, nm), V(nk, nm)),
        (VMEM,) * 3,
        (VMEM,) * 11 + (ANY,),
        flops=2 * 10**6,
    )(u, pa, pb, lat_b, *lon, *lev, d_edge, f_edge, n_pa, in_hbm(end))
    others = []
    edge_total_1 = edge_total
    for bit in range(bits):
        others.append(partner(bit, edge_total))
        edge_total = edge_total + others[-1]
    others = tuple(map(in_vmem, others))
    sums, other = in_vmem(sums), in_vmem(other)
    out = call(
        functools.partial(totals_kernel, scale),
        H(nj, ni, nk, nm),
        HBM,
        (VMEM,) * 3 + (ANY,),
        limit=5,
        scratch=(V(nj - 1, ni, nk // 2, nm), pltpu.SemaphoreType.DMA((nj - 1,))),
        flops=10**6,
    )(sums, other, in_vmem(mine), edge_total_1)
    n = 6 + bits
    end, out = call(
        functools.partial(last_totals_kernel, scale),
        (H(nj, ni, nk, nm),) * 2,
        (HBM, HBM),
        (VMEM,) * n + (HBM, HBM),
        scratch=(
            V(nj - 1, ni, nk // 2, nm),
            V(ni, nk, nm),
            pltpu.SemaphoreType.DMA((nj - 1,)),
            pltpu.SemaphoreType.DMA((4,)),
        ),
        limit=6,
        aliases={n: 0, n + 1: 1},
        flops=10**6,
    )(sums, other, in_vmem(back), n_pa, in_vmem(n_pb), in_vmem(edge_sums), *others, in_hbm(end), in_hbm(out))
    return out, end


def solution(mesh):
    spec = P("lat", "lon", "lev", None)
    return jax.shard_map(
        functools.partial(per_device, mesh.shape["lon"], mesh.shape["lev"]),
        mesh=mesh,
        in_specs=(spec, spec, spec),
        out_specs=(spec, spec),
        check_vma=False,
    )
```

```python
import functools

import jax
import jax.numpy as jnp
from jax import lax
from jax.experimental import pallas as pl
from jax.experimental.pallas import tpu as pltpu
from jax.sharding import PartitionSpec as P


STEPS = 4
LATE = 2
BLOCK = 4
VMEM = pl.BlockSpec(memory_space=pltpu.VMEM)
HBM = pl.BlockSpec(memory_space=pltpu.HBM)
ANY = pl.BlockSpec(memory_space=pl.ANY)


def in_vmem(x):
    return pltpu.with_memory_space_constraint(x, pltpu.VMEM)


def in_hbm(x):
    return pltpu.with_memory_space_constraint(x, pltpu.HBM)


def new_rows(c, im, ip, nb, klo, khi, d, f):
    km = jnp.concatenate([klo, c[:-1]], axis=0)
    kp = jnp.concatenate([c[1:], khi], axis=0)
    spread = (im + ip) + nb + (km + kp) - 6.0 * c
    return c + d * spread + f


def sweep(lo, hi, row, below, above, nb, klo, khi, d, f, put, carry=None):
    def block(first, bottom, top, carry):
        rows = [bottom() if bottom else row(first - 1)]
        rows += [row(first + r) for r in range(BLOCK)]
        rows += [top() if top else row(first + BLOCK)]
        for r in range(BLOCK):
            i = first + r
            new = new_rows(rows[r + 1], rows[r], rows[r + 2], nb(i), klo(i), khi(i), d(i), f(i))
            carry = put(i, new, carry)
        return carry

    carry = block(lo, below, None, carry)

    def body(b, carry):
        return block(lo + b * BLOCK, None, None, carry)

    n = (hi - lo) // BLOCK
    carry = lax.fori_loop(1, n - 1, body, carry)
    return block(hi - BLOCK, None, above, carry)


def plane_at(depth, n):
    low = lax.axis_index("lat") == 0
    return jnp.where(low, n - 1 - depth, depth)


def odd(axis):
    return lax.axis_index(axis) % 2 == 1


def lower(axis, e, o):
    return jnp.where(odd(axis), e, o)


def upper(axis, e, o):
    return jnp.where(odd(axis), o, e)


def faces_kernel(u, lon_e, lon_o, lev_e, lev_o):
    nj, ni, nk, _ = u.shape
    at_e = jnp.where(odd("lon"), 0, ni - 1)
    for j in range(nj):
        lon_e[j] = u[j, at_e]
        lon_o[j] = u[j, ni - 1 - at_e]
        lo, hi = u[j, :, 0, :], u[j, :, nk - 1, :]
        lev_e[j] = lower("lev", lo, hi)
        lev_o[j] = upper("lev", lo, hi)


def load_a_kernel(u_in, pa, sem):
    n = pa.shape[0]
    copy = pltpu.make_async_copy(u_in.at[plane_at(0, u_in.shape[0]), pl.ds(n // 2, n)], pa, sem)
    copy.start()
    copy.wait()


def load_kernel(u_in, d_in, f_in, u, pb, d_edge, f_edge, lon_e, lon_o, lev_e, lev_o, sem):
    nj, ni = u.shape[:2]
    q = ni // 4
    pj = plane_at(0, nj)
    copies = [pltpu.make_async_copy(u_in.at[j], u.at[j], sem.at[j]) for j in range(nj)]
    copies += [
        pltpu.make_async_copy(d_in.at[pj], d_edge, sem.at[nj]),
        pltpu.make_async_copy(f_in.at[pj], f_edge, sem.at[nj + 1]),
        pltpu.make_async_copy(u_in.at[pj, pl.ds(0, q)], pb.at[pl.ds(0, q)], sem.at[nj + 2]),
        pltpu.make_async_copy(u_in.at[pj, pl.ds(ni - q, q)], pb.at[pl.ds(q, q)], sem.at[nj + 3]),
    ]
    for copy in copies:
        copy.start()
    for copy in copies:
        copy.wait()
    faces_kernel(u, lon_e, lon_o, lev_e, lev_o)


def lev_rows(lev_e, lev_o, j, base):
    def get(side):
        def row(i):
            at = pl.ds(base + i, 1)
            return side("lev", lev_e[j, at, :], lev_o[j, at, :])

        return row

    return get(lower), get(upper)


def edge_rows(lo, hi, base, mine, below, above, u, lat, lev_e, lev_o, d, f, put):
    nj = u.shape[0]
    pj, pn = plane_at(0, nj), plane_at(1, nj)
    sweep(
        lo,
        hi,
        lambda i: mine[i],
        below,
        above,
        lambda i: u[pn, base + i] + lat[i],
        *lev_rows(lev_e, lev_o, pj, base),
        lambda i: d[base + i],
        lambda i: f[base + i],
        put,
        jnp.int32(0),
    )


def edge_a_kernel(u, pa, pb, lat, lev_e, lev_o, d, f, out):
    def put(i, new, carry):
        out[i] = new
        return carry

    n = pa.shape[0]
    edge_rows(0, n, n // 2, pa, lambda: pb[n // 2 - 1], lambda: pb[n // 2], u, lat, lev_e, lev_o, d, f, put)


def edge_b_kernel(u, pa, pb, lat, lon_e, lon_o, lev_e, lev_o, d, f, *rest):
    nj, ni, nk, _ = u.shape
    q = ni // 4
    pj = plane_at(0, nj)
    out = rest[2] if len(rest) > 1 else rest[0]

    def put(i, new, carry):
        out[i] = new
        return carry

    args = (u, lat, lev_e, lev_o, d, f, put)
    edge_rows(0, q, 0, pb, lambda: lower("lon", lon_e[pj], lon_o[pj]), lambda: pa[0], *args)
    edge_rows(q, 2 * q, 2 * q, pb, lambda: pa[2 * q - 1], lambda: upper("lon", lon_e[pj], lon_o[pj]), *args)
    if len(rest) > 1:
        nu, npa, _, s_lon_e, s_lon_o, s_lev_e, s_lev_o = rest
        faces_kernel(nu, s_lon_e, s_lon_o, s_lev_e, s_lev_o)
        s_lon_e[pj] = lower("lon", out[0], out[2 * q - 1])
        s_lon_o[pj] = upper("lon", out[0], out[2 * q - 1])
        for s_lev, side in ((s_lev_e, lower), (s_lev_o, upper)):
            s_lev[pj, :q] = side("lev", out[:q, 0, :], out[:q, nk - 1, :])
            s_lev[pj, q : 3 * q] = side("lev", npa[:, 0, :], npa[:, nk - 1, :])
            s_lev[pj, 3 * q :] = side("lev", out[q:, 0, :], out[q:, nk - 1, :])


def bulk_planes(u, pa, pb, lon_e, lon_o, lev_e, lev_o, d, f, put, start, finish):
    nj, ni, _, _ = u.shape
    q = ni // 4

    def run(j, lo, hi, nb, carry):
        return sweep(
            lo,
            hi,
            lambda i: u[j, i],
            (lambda: lower("lon", lon_e[j], lon_o[j])) if lo == 0 else None,
            (lambda: upper("lon", lon_e[j], lon_o[j])) if hi == ni else None,
            nb,
            *lev_rows(lev_e, lev_o, j, 0),
            lambda i: d[j, i],
            lambda i: f[j, i],
            functools.partial(put, j),
            carry,
        )

    j, inner = plane_at(1, nj), plane_at(2, nj)
    start(j, 1)
    carry = run(j, 0, q, lambda i: u[inner, i] + pb[i], zero_carry(u))
    carry = run(j, q, 3 * q, lambda i: u[inner, i] + pa[i - q], carry)
    carry = run(j, 3 * q, ni, lambda i: u[inner, i] + pb[i - 2 * q], carry)
    finish(j, 1, carry)

    def body(depth, _):
        j, outer, inner = plane_at(depth, nj), plane_at(depth - 1, nj), plane_at(depth + 1, nj)
        start(j, depth)
        carry = run(j, 0, ni, lambda i: u[outer, i] + u[inner, i], zero_carry(u))
        finish(j, depth, carry)
        return 0

    lax.fori_loop(2, nj - 1, body, 0)
    j, outer = plane_at(nj - 1, nj), plane_at(nj - 2, nj)
    start(j, nj - 1)
    carry = run(j, 0, ni, lambda i: u[outer, i], zero_carry(u))
    finish(j, nj - 1, carry)


def zero_carry(u):
    return jnp.zeros(u.shape[2:], u.dtype)


def nothing(*_):
    pass


def plain_put(out):
    def put(j, i, new, carry):
        out[j, i] = new
        return carry

    return put


def first_bulk_kernel(u, pa, pb, lon_e, lon_o, lev_e, lev_o, d_in, f_in, after, out, d, f, sem):
    del after
    nj = u.shape[0]

    def copies(j, depth):
        return (
            pltpu.make_async_copy(d_in.at[j], d.at[j], sem.at[0, depth]),
            pltpu.make_async_copy(f_in.at[j], f.at[j], sem.at[1, depth]),
        )

    for depth in range(1, nj):
        for copy in copies(plane_at(depth, nj), depth):
            copy.start()

    def start(j, depth):
        for copy in copies(j, depth):
            copy.wait()

    bulk_planes(u, pa, pb, lon_e, lon_o, lev_e, lev_o, d, f, plain_put(out), start, nothing)


def bulk_kernel(u, pa, pb, lon_e, lon_o, lev_e, lev_o, d, f, after, out):
    del after
    bulk_planes(u, pa, pb, lon_e, lon_o, lev_e, lev_o, d, f, plain_put(out), nothing, nothing)


def last_bulk_kernel(u, pa, pb, lon_e, lon_o, lev_e, lev_o, d_in, f_in, after, end, d, f, total, sem):
    del d_in, f_in, after
    nj = u.shape[0]

    def copy_out(j, depth):
        return pltpu.make_async_copy(f.at[j], end.at[j], sem.at[depth])

    def put(j, i, new, carry):
        f[j, i] = new
        carry = carry + new
        d[j, i] = carry
        return carry

    def finish(j, depth, carry):
        total[depth - 1] = carry

        @pl.when(depth < nj - LATE)
        def _():
            copy_out(j, depth).start()

    bulk_planes(u, pa, pb, lon_e, lon_o, lev_e, lev_o, d, f, put, nothing, finish)
    for depth in range(1, nj - LATE):
        copy_out(plane_at(depth, nj), depth).wait()


def late_kernel(f, end_in, end, sem):
    del end_in
    nj = f.shape[0]
    copies = []
    for p in range(LATE):
        j = plane_at(nj - LATE + p, nj)
        copies.append(pltpu.make_async_copy(f.at[j], end.at[j], sem.at[p]))
        copies[-1].start()
    for copy in copies:
        copy.wait()


def last_edge_kernel(u, pa, pb, lat, lon_e, lon_o, lev_e, lev_o, d, f, npa, after, npb, sums, total):
    del after
    edge_b_kernel(u, pa, pb, lat, lon_e, lon_o, lev_e, lev_o, d, f, npb)
    ni = sums.shape[0]
    q = ni // 4
    carry = zero_carry(u)
    for part, lo, n, base in ((npb, 0, q, 0), (npa, 0, 2 * q, q), (npb, q, q, 3 * q)):

        def row(r, carry):
            carry = carry + part[lo + r]
            sums[base + r] = carry
            return carry

        carry = lax.fori_loop(0, n, row, carry, unroll=4)
    total[...] = carry


def earlier(others, first=0):
    lon = lax.axis_index("lon")
    before = 0.0
    for bit, other in enumerate(others):
        before += jnp.where(lon & (1 << (first + bit)) != 0, other, 0.0)
    return before


def half_kernel(total, other, out):
    n = out.shape[1]
    at = pl.ds(pl.multiple_of(jnp.where(odd("lon"), n, 0), n), n)
    for p in range(out.shape[0]):
        out[p] = total[p, at] + other[p, at]


def before_kernel(*refs):
    *others, out = refs
    for p in range(out.shape[0]):
        out[p] = earlier([other[p] for other in others], 1)


def total_rows(scale, ni, sums, before, put):
    def row(r, _):
        for q in range(BLOCK):
            i = r * BLOCK + q
            put(i, (sums(i) + before) * scale)
        return 0

    lax.fori_loop(0, ni // BLOCK, row, 0)


def half_totals(scale, upper_half, sums, other, before, out, stage, sem):
    nj, ni, nk = sums.shape[:3]
    n = nk // 2
    at = pl.ds(pl.multiple_of(jnp.where(upper_half, n, 0), n), n)

    def copy_out(depth):
        return pltpu.make_async_copy(stage.at[depth - 1], out.at[plane_at(depth, nj), :, at, :], sem.at[depth - 1])

    def body(depth, _):
        j = plane_at(depth, nj)
        b = before[depth - 1] + earlier([other[depth - 1, at]])

        def put(i, value):
            stage[depth - 1, i] = value

        total_rows(scale, ni, lambda i: sums[j, i, at], b, put)
        copy_out(depth).start()
        return 0

    lax.fori_loop(1, nj, body, 0)
    return [copy_out(depth) for depth in range(1, nj)]


def totals_kernel(scale, sums, other, before, after, out, stage, sem):
    del after
    for copy in half_totals(scale, odd("lon"), sums, other, before, out, stage, sem):
        copy.wait()


def last_totals_kernel(scale, sums, other, before, npa, npb, edge_sums, *rest):
    *others, _, _, end, out, stage, edge_stage, sem, edge_sem = rest
    nj, ni = sums.shape[:2]
    q = ni // 4
    pj = plane_at(0, nj)
    copies = [
        pltpu.make_async_copy(npb.at[pl.ds(0, q)], end.at[pj, pl.ds(0, q)], edge_sem.at[0]),
        pltpu.make_async_copy(npa, end.at[pj, pl.ds(q, 2 * q)], edge_sem.at[1]),
        pltpu.make_async_copy(npb.at[pl.ds(q, q)], end.at[pj, pl.ds(3 * q, q)], edge_sem.at[2]),
        pltpu.make_async_copy(edge_stage, out.at[pj], edge_sem.at[3]),
    ]
    for copy in copies[:3]:
        copy.start()
    copies += half_totals(scale, jnp.logical_not(odd("lon")), sums, other, before, out, stage, sem)

    def put(i, value):
        edge_stage[i] = value

    total_rows(scale, ni, lambda i: edge_sums[i], earlier([other[...] for other in others]), put)
    copies[3].start()
    for copy in copies:
        copy.wait()


def call(kernel, out_shape, out_specs, in_specs, limit=2, scratch=(), aliases=None, flops=0):
    return pl.pallas_call(
        kernel,
        out_shape=out_shape,
        in_specs=in_specs,
        out_specs=out_specs,
        scratch_shapes=scratch,
        input_output_aliases=aliases or {},
        compiler_params=pltpu.CompilerParams(vmem_limit_bytes=limit * 2**20),
        cost_estimate=pl.CostEstimate(flops=flops, transcendentals=0, bytes_accessed=0),
    )


def per_device(lon_size, lev_size, initial_state, scaled_diffusivity, scaled_forcing):
    dtype = initial_state.dtype
    nj, ni, nk, nm = initial_state.shape
    half = ni // 2
    V = lambda *shape: pltpu.VMEM(shape, dtype)
    H = lambda *shape: pltpu.HBM(shape, dtype)

    swap = [(0, 1), (1, 0)]
    faces_out = (V(nj, nk, nm), V(nj, nk, nm), V(nj, ni, nm), V(nj, ni, nm))

    def exchange(axis, size, e, o):
        def swaps(first):
            return [(a, b) for i in range(first, size - 1, 2) for a, b in ((i, i + 1), (i + 1, i))]

        return lax.ppermute(e, axis, swaps(0)), lax.ppermute(o, axis, swaps(1))

    def lon_exchange(e, o, relay):
        if not relay:
            return exchange("lon", lon_size, e, o)
        relayed = lax.ppermute(o, "lon", [(3, 7), (4, 0)])
        e, o = (lax.ppermute(x, "lon", [p for i in a for p in ((i, i + 1), (i + 1, i))]) for x, a in ((e, (0, 2, 4, 6)), (o, (1, 5))))
        return e, o + lax.ppermute(relayed, "lon", [(7, 4), (0, 3)])

    def lev_exchange(e, o):
        return exchange("lev", lev_size, e, o)

    def partner(bit, total):
        pairs = [(i, i ^ (1 << bit)) for i in range(lon_size)]
        if 2 << bit == lon_size:
            pairs = [(a, b) for a, b in pairs if a < b]
        return lax.ppermute(total, "lon", pairs)

    bits = lon_size.bit_length() - 1

    pa = call(
        load_a_kernel, V(half, nk, nm), VMEM, (HBM,), scratch=(pltpu.SemaphoreType.DMA,), flops=10**5
    )(in_hbm(initial_state))
    lat_a = lax.ppermute(pa, "lat", swap)
    u, pb, d_edge, f_edge, *faces = call(
        load_kernel,
        (V(nj, ni, nk, nm), V(half, nk, nm), V(ni, nk, nm), V(ni, nk, nm)) + faces_out,
        (VMEM,) * 8,
        (HBM,) * 3,
        scratch=(pltpu.SemaphoreType.DMA((nj + 4,)),),
        flops=10**6,
    )(*map(in_hbm, (initial_state, scaled_diffusivity, scaled_forcing)))
    lon = lon_exchange(*faces[:2], True)
    lat_b = lax.ppermute(pb, "lat", swap)
    lev = lev_exchange(*faces[2:])
    d_edge, f_edge = in_vmem(d_edge), in_vmem(f_edge)
    d, f = in_hbm(scaled_diffusivity), in_hbm(scaled_forcing)

    for step in range(STEPS):
        last = step == STEPS - 1
        u, pa, pb, lat_a, lat_b = map(in_vmem, (u, pa, pb, lat_a, lat_b))
        lon, lev = tuple(map(in_vmem, lon)), tuple(map(in_vmem, lev))
        n_pa = call(edge_a_kernel, V(half, nk, nm), VMEM, (VMEM,) * 8, flops=10**6)(
            u, pa, pb, lat_a, *lev, d_edge, f_edge
        )
        if last:
            break
        lat_a = lax.ppermute(n_pa, "lat", swap)
        if step == 0:
            n_u, d, f = call(
                first_bulk_kernel,
                (V(nj, ni, nk, nm),) * 3,
                (VMEM,) * 3,
                (VMEM,) * 7 + (HBM,) * 2 + (ANY,),
                scratch=(pltpu.SemaphoreType.DMA((2, nj)),),
                flops=2 * 10**7,
            )(u, pa, pb, *lon, *lev, d, f, n_pa)
        else:
            n_u = call(
                bulk_kernel, V(nj, ni, nk, nm), VMEM, (VMEM,) * 9 + (ANY,), flops=2 * 10**7
            )(u, pa, pb, *lon, *lev, in_vmem(d), in_vmem(f), n_pa)
        n_pb, *faces = call(
            edge_b_kernel, (V(half, nk, nm),) + faces_out, (VMEM,) * 5, (VMEM,) * 12, flops=10**6
        )(u, pa, pb, lat_b, *lon, *lev, d_edge, f_edge, in_vmem(n_u), in_vmem(n_pa))
        lon = lon_exchange(*faces[:2], step % 2 == 1)
        lat_b = lax.ppermute(n_pb, "lat", swap)
        lev = lev_exchange(*faces[2:])
        u, pa, pb = n_u, n_pa, n_pb

    scale = 1.0 / (ni * lon_size)
    end, sums, values, total = call(
        last_bulk_kernel,
        (H(nj, ni, nk, nm), V(nj, ni, nk, nm), V(nj, ni, nk, nm), V(nj - 1, nk, nm)),
        (HBM, VMEM, VMEM, VMEM),
        (VMEM,) * 9 + (ANY,),
        scratch=(pltpu.SemaphoreType.DMA((nj,)),),
        aliases={7: 1, 8: 2},
        flops=2 * 10**7,
    )(u, pa, pb, *lon, *lev, in_vmem(d), in_vmem(f), n_pa)
    other = partner(0, total)
    end = call(
        late_kernel,
        H(nj, ni, nk, nm),
        HBM,
        (VMEM, HBM),
        scratch=(pltpu.SemaphoreType.DMA((LATE,)),),
        aliases={1: 0},
        flops=10**5,
    )(in_vmem(values), in_hbm(end))
    half_total = call(half_kernel, V(nj - 1, nk // 2, nm), VMEM, (VMEM,) * 2, flops=10**5)(
        in_vmem(total), in_vmem(other)
    )
    later = []
    for bit in range(1, bits):
        later.append(partner(bit, half_total))
        half_total = half_total + later[-1]
    mine = call(before_kernel, V(nj - 1, nk // 2, nm), VMEM, (VMEM,) * (bits - 1), flops=10**5)(*map(in_vmem, later))
    back = lax.ppermute(mine, "lon", [(i, i ^ 1) for i in range(lon_size)])
    n_pa = in_vmem(n_pa)
    n_pb, edge_sums, edge_total = call(
        last_edge_kernel,
        (V(half, nk, nm), V(ni, nk, nm), V(nk, nm)),
        (VMEM,) * 3,
        (VMEM,) * 11 + (ANY,),
        flops=2 * 10**6,
    )(u, pa, pb, lat_b, *lon, *lev, d_edge, f_edge, n_pa, in_hbm(end))
    others = []
    edge_total_1 = edge_total
    for bit in range(bits):
        others.append(partner(bit, edge_total))
        edge_total = edge_total + others[-1]
    others = tuple(map(in_vmem, others))
    sums, other = in_vmem(sums), in_vmem(other)
    out = call(
        functools.partial(totals_kernel, scale),
        H(nj, ni, nk, nm),
        HBM,
        (VMEM,) * 3 + (ANY,),
        limit=5,
        scratch=(V(nj - 1, ni, nk // 2, nm), pltpu.SemaphoreType.DMA((nj - 1,))),
        flops=10**6,
    )(sums, other, in_vmem(mine), edge_total_1)
    n = 6 + bits
    end, out = call(
        functools.partial(last_totals_kernel, scale),
        (H(nj, ni, nk, nm),) * 2,
        (HBM, HBM),
        (VMEM,) * n + (HBM, HBM),
        scratch=(
            V(nj - 1, ni, nk // 2, nm),
            V(ni, nk, nm),
            pltpu.SemaphoreType.DMA((nj - 1,)),
            pltpu.SemaphoreType.DMA((4,)),
        ),
        limit=6,
        aliases={n: 0, n + 1: 1},
        flops=10**6,
    )(sums, other, in_vmem(back), n_pa, in_vmem(n_pb), in_vmem(edge_sums), *others, in_hbm(end), in_hbm(out))
    return out, end


def solution(mesh):
    spec = P("lat", "lon", "lev", None)
    return jax.shard_map(
        functools.partial(per_device, mesh.shape["lon"], mesh.shape["lev"]),
        mesh=mesh,
        in_specs=(spec, spec, spec),
        out_specs=(spec, spec),
        check_vma=False,
    )
```

```python
import functools

import jax
import jax.numpy as jnp
from jax import lax
from jax.experimental import pallas as pl
from jax.experimental.pallas import tpu as pltpu
from jax.sharding import PartitionSpec as P


STEPS = 4
LATE = 2
BLOCK = 4
VMEM = pl.BlockSpec(memory_space=pltpu.VMEM)
HBM = pl.BlockSpec(memory_space=pltpu.HBM)
ANY = pl.BlockSpec(memory_space=pl.ANY)


def in_vmem(x):
    return pltpu.with_memory_space_constraint(x, pltpu.VMEM)


def in_hbm(x):
    return pltpu.with_memory_space_constraint(x, pltpu.HBM)


def new_rows(c, im, ip, nb, klo, khi, d, f):
    km = jnp.concatenate([klo, c[:-1]], axis=0)
    kp = jnp.concatenate([c[1:], khi], axis=0)
    spread = (im + ip) + nb + (km + kp) - 6.0 * c
    return c + d * spread + f


def sweep(lo, hi, row, below, above, nb, klo, khi, d, f, put, carry=None):
    def block(first, bottom, top, carry):
        rows = [bottom() if bottom else row(first - 1)]
        rows += [row(first + r) for r in range(BLOCK)]
        rows += [top() if top else row(first + BLOCK)]
        for r in range(BLOCK):
            i = first + r
            new = new_rows(rows[r + 1], rows[r], rows[r + 2], nb(i), klo(i), khi(i), d(i), f(i))
            carry = put(i, new, carry)
        return carry

    carry = block(lo, below, None, carry)

    def body(b, carry):
        return block(lo + b * BLOCK, None, None, carry)

    n = (hi - lo) // BLOCK
    carry = lax.fori_loop(1, n - 1, body, carry)
    return block(hi - BLOCK, None, above, carry)


def plane_at(depth, n):
    low = lax.axis_index("lat") == 0
    return jnp.where(low, n - 1 - depth, depth)


def odd(axis):
    return lax.axis_index(axis) % 2 == 1


def lower(axis, e, o):
    return jnp.where(odd(axis), e, o)


def upper(axis, e, o):
    return jnp.where(odd(axis), o, e)


def faces_kernel(u, lon_e, lon_o, lev_e, lev_o):
    nj, ni, nk, _ = u.shape
    at_e = jnp.where(odd("lon"), 0, ni - 1)
    for j in range(nj):
        lon_e[j] = u[j, at_e]
        lon_o[j] = u[j, ni - 1 - at_e]
        lo, hi = u[j, :, 0, :], u[j, :, nk - 1, :]
        lev_e[j] = lower("lev", lo, hi)
        lev_o[j] = upper("lev", lo, hi)


def load_a_kernel(u_in, pa, sem):
    n = pa.shape[0]
    copy = pltpu.make_async_copy(u_in.at[plane_at(0, u_in.shape[0]), pl.ds(n // 2, n)], pa, sem)
    copy.start()
    copy.wait()


def load_kernel(u_in, d_in, f_in, u, pb, d_edge, f_edge, lon_e, lon_o, lev_e, lev_o, sem):
    nj, ni = u.shape[:2]
    q = ni // 4
    pj = plane_at(0, nj)
    copies = [pltpu.make_async_copy(u_in.at[j], u.at[j], sem.at[j]) for j in range(nj)]
    copies += [
        pltpu.make_async_copy(d_in.at[pj], d_edge, sem.at[nj]),
        pltpu.make_async_copy(f_in.at[pj], f_edge, sem.at[nj + 1]),
        pltpu.make_async_copy(u_in.at[pj, pl.ds(0, q)], pb.at[pl.ds(0, q)], sem.at[nj + 2]),
        pltpu.make_async_copy(u_in.at[pj, pl.ds(ni - q, q)], pb.at[pl.ds(q, q)], sem.at[nj + 3]),
    ]
    for copy in copies:
        copy.start()
    for copy in copies:
        copy.wait()
    faces_kernel(u, lon_e, lon_o, lev_e, lev_o)


def lev_rows(lev_e, lev_o, j, base):
    def get(side):
        def row(i):
            at = pl.ds(base + i, 1)
            return side("lev", lev_e[j, at, :], lev_o[j, at, :])

        return row

    return get(lower), get(upper)


def edge_rows(lo, hi, base, mine, below, above, u, lat, lev_e, lev_o, d, f, put):
    nj = u.shape[0]
    pj, pn = plane_at(0, nj), plane_at(1, nj)
    sweep(
        lo,
        hi,
        lambda i: mine[i],
        below,
        above,
        lambda i: u[pn, base + i] + lat[i],
        *lev_rows(lev_e, lev_o, pj, base),
        lambda i: d[base + i],
        lambda i: f[base + i],
        put,
        jnp.int32(0),
    )


def edge_a_kernel(u, pa, pb, lat, lev_e, lev_o, d, f, out):
    def put(i, new, carry):
        out[i] = new
        return carry

    n = pa.shape[0]
    edge_rows(0, n, n // 2, pa, lambda: pb[n // 2 - 1], lambda: pb[n // 2], u, lat, lev_e, lev_o, d, f, put)


def edge_b_kernel(u, pa, pb, lat, lon_e, lon_o, lev_e, lev_o, d, f, *rest):
    nj, ni, nk, _ = u.shape
    q = ni // 4
    pj = plane_at(0, nj)
    out = rest[2] if len(rest) > 1 else rest[0]

    def put(i, new, carry):
        out[i] = new
        return carry

    args = (u, lat, lev_e, lev_o, d, f, put)
    edge_rows(0, q, 0, pb, lambda: lower("lon", lon_e[pj], lon_o[pj]), lambda: pa[0], *args)
    edge_rows(q, 2 * q, 2 * q, pb, lambda: pa[2 * q - 1], lambda: upper("lon", lon_e[pj], lon_o[pj]), *args)
    if len(rest) > 1:
        nu, npa, _, s_lon_e, s_lon_o, s_lev_e, s_lev_o = rest
        faces_kernel(nu, s_lon_e, s_lon_o, s_lev_e, s_lev_o)
        s_lon_e[pj] = lower("lon", out[0], out[2 * q - 1])
        s_lon_o[pj] = upper("lon", out[0], out[2 * q - 1])
        for s_lev, side in ((s_lev_e, lower), (s_lev_o, upper)):
            s_lev[pj, :q] = side("lev", out[:q, 0, :], out[:q, nk - 1, :])
            s_lev[pj, q : 3 * q] = side("lev", npa[:, 0, :], npa[:, nk - 1, :])
            s_lev[pj, 3 * q :] = side("lev", out[q:, 0, :], out[q:, nk - 1, :])


def bulk_planes(u, pa, pb, lon_e, lon_o, lev_e, lev_o, d, f, put, start, finish):
    nj, ni, _, _ = u.shape
    q = ni // 4

    def run(j, lo, hi, nb, carry):
        return sweep(
            lo,
            hi,
            lambda i: u[j, i],
            (lambda: lower("lon", lon_e[j], lon_o[j])) if lo == 0 else None,
            (lambda: upper("lon", lon_e[j], lon_o[j])) if hi == ni else None,
            nb,
            *lev_rows(lev_e, lev_o, j, 0),
            lambda i: d[j, i],
            lambda i: f[j, i],
            functools.partial(put, j),
            carry,
        )

    j, inner = plane_at(1, nj), plane_at(2, nj)
    start(j, 1)
    carry = run(j, 0, q, lambda i: u[inner, i] + pb[i], zero_carry(u))
    carry = run(j, q, 3 * q, lambda i: u[inner, i] + pa[i - q], carry)
    carry = run(j, 3 * q, ni, lambda i: u[inner, i] + pb[i - 2 * q], carry)
    finish(j, 1, carry)

    def body(depth, _):
        j, outer, inner = plane_at(depth, nj), plane_at(depth - 1, nj), plane_at(depth + 1, nj)
        start(j, depth)
        carry = run(j, 0, ni, lambda i: u[outer, i] + u[inner, i], zero_carry(u))
        finish(j, depth, carry)
        return 0

    lax.fori_loop(2, nj - 1, body, 0)
    j, outer = plane_at(nj - 1, nj), plane_at(nj - 2, nj)
    start(j, nj - 1)
    carry = run(j, 0, ni, lambda i: u[outer, i], zero_carry(u))
    finish(j, nj - 1, carry)


def zero_carry(u):
    return jnp.zeros(u.shape[2:], u.dtype)


def nothing(*_):
    pass


def plain_put(out):
    def put(j, i, new, carry):
        out[j, i] = new
        return carry

    return put


def first_bulk_kernel(u, pa, pb, lon_e, lon_o, lev_e, lev_o, d_in, f_in, after, out, d, f, sem):
    del after
    nj = u.shape[0]

    def copies(j, depth):
        return (
            pltpu.make_async_copy(d_in.at[j], d.at[j], sem.at[0, depth]),
            pltpu.make_async_copy(f_in.at[j], f.at[j], sem.at[1, depth]),
        )

    for depth in range(1, nj):
        for copy in copies(plane_at(depth, nj), depth):
            copy.start()

    def start(j, depth):
        for copy in copies(j, depth):
            copy.wait()

    bulk_planes(u, pa, pb, lon_e, lon_o, lev_e, lev_o, d, f, plain_put(out), start, nothing)


def bulk_kernel(u, pa, pb, lon_e, lon_o, lev_e, lev_o, d, f, after, out):
    del after
    bulk_planes(u, pa, pb, lon_e, lon_o, lev_e, lev_o, d, f, plain_put(out), nothing, nothing)


def last_bulk_kernel(u, pa, pb, lon_e, lon_o, lev_e, lev_o, d_in, f_in, after, end, d, f, total, sem):
    del d_in, f_in, after
    nj = u.shape[0]

    def copy_out(j, depth):
        return pltpu.make_async_copy(f.at[j], end.at[j], sem.at[depth])

    def put(j, i, new, carry):
        f[j, i] = new
        carry = carry + new
        d[j, i] = carry
        return carry

    def finish(j, depth, carry):
        total[depth - 1] = carry

        @pl.when(depth < nj - LATE)
        def _():
            copy_out(j, depth).start()

    bulk_planes(u, pa, pb, lon_e, lon_o, lev_e, lev_o, d, f, put, nothing, finish)
    for depth in range(1, nj - LATE):
        copy_out(plane_at(depth, nj), depth).wait()


def late_kernel(f, end_in, end, sem):
    del end_in
    nj = f.shape[0]
    copies = []
    for p in range(LATE):
        j = plane_at(nj - LATE + p, nj)
        copies.append(pltpu.make_async_copy(f.at[j], end.at[j], sem.at[p]))
        copies[-1].start()
    for copy in copies:
        copy.wait()


def last_edge_kernel(u, pa, pb, lat, lon_e, lon_o, lev_e, lev_o, d, f, npa, npb, sums, total):
    edge_b_kernel(u, pa, pb, lat, lon_e, lon_o, lev_e, lev_o, d, f, npb)
    ni = sums.shape[0]
    q = ni // 4
    carry = zero_carry(u)
    for part, lo, n, base in ((npb, 0, q, 0), (npa, 0, 2 * q, q), (npb, q, q, 3 * q)):

        def row(r, carry):
            carry = carry + part[lo + r]
            sums[base + r] = carry
            return carry

        carry = lax.fori_loop(0, n, row, carry, unroll=4)
    total[...] = carry


def earlier(others, first=0):
    lon = lax.axis_index("lon")
    before = 0.0
    for bit, other in enumerate(others):
        before += jnp.where(lon & (1 << (first + bit)) != 0, other, 0.0)
    return before


def half_kernel(total, other, out):
    n = out.shape[1]
    at = pl.ds(pl.multiple_of(jnp.where(odd("lon"), n, 0), n), n)
    for p in range(out.shape[0]):
        out[p] = total[p, at] + other[p, at]


def before_kernel(*refs):
    *others, out = refs
    for p in range(out.shape[0]):
        out[p] = earlier([other[p] for other in others], 1)


def total_rows(scale, ni, sums, before, put):
    def row(r, _):
        for q in range(BLOCK):
            i = r * BLOCK + q
            put(i, (sums(i) + before) * scale)
        return 0

    lax.fori_loop(0, ni // BLOCK, row, 0)


def half_totals(scale, upper_half, sums, other, before, out, stage, sem):
    nj, ni, nk = sums.shape[:3]
    n = nk // 2
    at = pl.ds(pl.multiple_of(jnp.where(upper_half, n, 0), n), n)

    def copy_out(depth):
        return pltpu.make_async_copy(stage.at[depth - 1], out.at[plane_at(depth, nj), :, at, :], sem.at[depth - 1])

    def body(depth, _):
        j = plane_at(depth, nj)
        b = before[depth - 1] + earlier([other[depth - 1, at]])

        def put(i, value):
            stage[depth - 1, i] = value

        total_rows(scale, ni, lambda i: sums[j, i, at], b, put)
        copy_out(depth).start()
        return 0

    lax.fori_loop(1, nj, body, 0)
    return [copy_out(depth) for depth in range(1, nj)]


def totals_kernel(scale, sums, other, before, after, out, stage, sem):
    del after
    for copy in half_totals(scale, odd("lon"), sums, other, before, out, stage, sem):
        copy.wait()


def last_totals_kernel(scale, sums, other, before, npa, npb, edge_sums, *rest):
    *others, _, _, end, out, stage, edge_stage, sem, edge_sem = rest
    nj, ni = sums.shape[:2]
    q = ni // 4
    pj = plane_at(0, nj)
    copies = [
        pltpu.make_async_copy(npb.at[pl.ds(0, q)], end.at[pj, pl.ds(0, q)], edge_sem.at[0]),
        pltpu.make_async_copy(npa, end.at[pj, pl.ds(q, 2 * q)], edge_sem.at[1]),
        pltpu.make_async_copy(npb.at[pl.ds(q, q)], end.at[pj, pl.ds(3 * q, q)], edge_sem.at[2]),
        pltpu.make_async_copy(edge_stage, out.at[pj], edge_sem.at[3]),
    ]
    for copy in copies[:3]:
        copy.start()
    copies += half_totals(scale, jnp.logical_not(odd("lon")), sums, other, before, out, stage, sem)

    def put(i, value):
        edge_stage[i] = value

    total_rows(scale, ni, lambda i: edge_sums[i], earlier([other[...] for other in others]), put)
    copies[3].start()
    for copy in copies:
        copy.wait()


def call(kernel, out_shape, out_specs, in_specs, limit=2, scratch=(), aliases=None, flops=0):
    return pl.pallas_call(
        kernel,
        out_shape=out_shape,
        in_specs=in_specs,
        out_specs=out_specs,
        scratch_shapes=scratch,
        input_output_aliases=aliases or {},
        compiler_params=pltpu.CompilerParams(vmem_limit_bytes=limit * 2**20),
        cost_estimate=pl.CostEstimate(flops=flops, transcendentals=0, bytes_accessed=0),
    )


def per_device(lon_size, lev_size, initial_state, scaled_diffusivity, scaled_forcing):
    dtype = initial_state.dtype
    nj, ni, nk, nm = initial_state.shape
    half = ni // 2
    V = lambda *shape: pltpu.VMEM(shape, dtype)
    H = lambda *shape: pltpu.HBM(shape, dtype)

    swap = [(0, 1), (1, 0)]
    faces_out = (V(nj, nk, nm), V(nj, nk, nm), V(nj, ni, nm), V(nj, ni, nm))

    def exchange(axis, size, e, o):
        def swaps(first):
            return [(a, b) for i in range(first, size - 1, 2) for a, b in ((i, i + 1), (i + 1, i))]

        return lax.ppermute(e, axis, swaps(0)), lax.ppermute(o, axis, swaps(1))

    def lon_exchange(e, o, relay):
        if not relay:
            return exchange("lon", lon_size, e, o)
        relayed = lax.ppermute(o, "lon", [(3, 7), (4, 0)])
        e, o = (lax.ppermute(x, "lon", [p for i in a for p in ((i, i + 1), (i + 1, i))]) for x, a in ((e, (0, 2, 4, 6)), (o, (1, 5))))
        return e, o + lax.ppermute(relayed, "lon", [(7, 4), (0, 3)])

    def lev_exchange(e, o):
        return exchange("lev", lev_size, e, o)

    def partner(bit, total):
        pairs = [(i, i ^ (1 << bit)) for i in range(lon_size)]
        if 2 << bit == lon_size:
            pairs = [(a, b) for a, b in pairs if a < b]
        return lax.ppermute(total, "lon", pairs)

    bits = lon_size.bit_length() - 1

    pa = call(
        load_a_kernel, V(half, nk, nm), VMEM, (HBM,), scratch=(pltpu.SemaphoreType.DMA,), flops=10**5
    )(in_hbm(initial_state))
    lat_a = lax.ppermute(pa, "lat", swap)
    u, pb, d_edge, f_edge, *faces = call(
        load_kernel,
        (V(nj, ni, nk, nm), V(half, nk, nm), V(ni, nk, nm), V(ni, nk, nm)) + faces_out,
        (VMEM,) * 8,
        (HBM,) * 3,
        scratch=(pltpu.SemaphoreType.DMA((nj + 4,)),),
        flops=10**6,
    )(*map(in_hbm, (initial_state, scaled_diffusivity, scaled_forcing)))
    lon = lon_exchange(*faces[:2], True)
    lat_b = lax.ppermute(pb, "lat", swap)
    lev = lev_exchange(*faces[2:])
    d_edge, f_edge = in_vmem(d_edge), in_vmem(f_edge)
    d, f = in_hbm(scaled_diffusivity), in_hbm(scaled_forcing)

    for step in range(STEPS):
        last = step == STEPS - 1
        u, pa, pb, lat_a, lat_b = map(in_vmem, (u, pa, pb, lat_a, lat_b))
        lon, lev = tuple(map(in_vmem, lon)), tuple(map(in_vmem, lev))
        n_pa = call(edge_a_kernel, V(half, nk, nm), VMEM, (VMEM,) * 8, flops=10**6)(
            u, pa, pb, lat_a, *lev, d_edge, f_edge
        )
        if last:
            break
        lat_a = lax.ppermute(n_pa, "lat", swap)
        if step == 0:
            n_u, d, f = call(
                first_bulk_kernel,
                (V(nj, ni, nk, nm),) * 3,
                (VMEM,) * 3,
                (VMEM,) * 7 + (HBM,) * 2 + (ANY,),
                scratch=(pltpu.SemaphoreType.DMA((2, nj)),),
                flops=2 * 10**7,
            )(u, pa, pb, *lon, *lev, d, f, n_pa)
        else:
            n_u = call(
                bulk_kernel, V(nj, ni, nk, nm), VMEM, (VMEM,) * 9 + (ANY,), flops=2 * 10**7
            )(u, pa, pb, *lon, *lev, in_vmem(d), in_vmem(f), n_pa)
        n_pb, *faces = call(
            edge_b_kernel, (V(half, nk, nm),) + faces_out, (VMEM,) * 5, (VMEM,) * 12, flops=10**6
        )(u, pa, pb, lat_b, *lon, *lev, d_edge, f_edge, in_vmem(n_u), in_vmem(n_pa))
        lon = lon_exchange(*faces[:2], step % 2 == 1)
        lat_b = lax.ppermute(n_pb, "lat", swap)
        lev = lev_exchange(*faces[2:])
        u, pa, pb = n_u, n_pa, n_pb

    scale = 1.0 / (ni * lon_size)
    end, sums, values, total = call(
        last_bulk_kernel,
        (H(nj, ni, nk, nm), V(nj, ni, nk, nm), V(nj, ni, nk, nm), V(nj - 1, nk, nm)),
        (HBM, VMEM, VMEM, VMEM),
        (VMEM,) * 9 + (ANY,),
        scratch=(pltpu.SemaphoreType.DMA((nj,)),),
        aliases={7: 1, 8: 2},
        flops=2 * 10**7,
    )(u, pa, pb, *lon, *lev, in_vmem(d), in_vmem(f), n_pa)
    other = partner(0, total)
    end = call(
        late_kernel,
        H(nj, ni, nk, nm),
        HBM,
        (VMEM, HBM),
        scratch=(pltpu.SemaphoreType.DMA((LATE,)),),
        aliases={1: 0},
        flops=10**5,
    )(in_vmem(values), in_hbm(end))
    half_total = call(half_kernel, V(nj - 1, nk // 2, nm), VMEM, (VMEM,) * 2, flops=10**5)(
        in_vmem(total), in_vmem(other)
    )
    later = []
    for bit in range(1, bits):
        later.append(partner(bit, half_total))
        half_total = half_total + later[-1]
    mine = call(before_kernel, V(nj - 1, nk // 2, nm), VMEM, (VMEM,) * (bits - 1), flops=10**5)(*map(in_vmem, later))
    back = lax.ppermute(mine, "lon", [(i, i ^ 1) for i in range(lon_size)])
    n_pa = in_vmem(n_pa)
    n_pb, edge_sums, edge_total = call(
        last_edge_kernel, (V(half, nk, nm), V(ni, nk, nm), V(nk, nm)), (VMEM,) * 3, (VMEM,) * 11, flops=2 * 10**6
    )(u, pa, pb, lat_b, *lon, *lev, d_edge, f_edge, n_pa)
    others = []
    edge_total_1 = edge_total
    for bit in range(bits):
        others.append(partner(bit, edge_total))
        edge_total = edge_total + others[-1]
    others = tuple(map(in_vmem, others))
    sums, other = in_vmem(sums), in_vmem(other)
    out = call(
        functools.partial(totals_kernel, scale),
        H(nj, ni, nk, nm),
        HBM,
        (VMEM,) * 3 + (ANY,),
        limit=5,
        scratch=(V(nj - 1, ni, nk // 2, nm), pltpu.SemaphoreType.DMA((nj - 1,))),
        flops=10**6,
    )(sums, other, in_vmem(mine), edge_total_1)
    n = 6 + bits
    end, out = call(
        functools.partial(last_totals_kernel, scale),
        (H(nj, ni, nk, nm),) * 2,
        (HBM, HBM),
        (VMEM,) * n + (HBM, HBM),
        scratch=(
            V(nj - 1, ni, nk // 2, nm),
            V(ni, nk, nm),
            pltpu.SemaphoreType.DMA((nj - 1,)),
            pltpu.SemaphoreType.DMA((4,)),
        ),
        limit=6,
        aliases={n: 0, n + 1: 1},
        flops=10**6,
    )(sums, other, in_vmem(back), n_pa, in_vmem(n_pb), in_vmem(edge_sums), *others, in_hbm(end), in_hbm(out))
    return out, end


def solution(mesh):
    spec = P("lat", "lon", "lev", None)
    return jax.shard_map(
        functools.partial(per_device, mesh.shape["lon"], mesh.shape["lev"]),
        mesh=mesh,
        in_specs=(spec, spec, spec),
        out_specs=(spec, spec),
        check_vma=False,
    )
```

```python
import functools

import jax
import jax.numpy as jnp
from jax import lax
from jax.experimental import pallas as pl
from jax.experimental.pallas import tpu as pltpu
from jax.sharding import PartitionSpec as P


STEPS = 4
LATE = 2
BLOCK = 4
VMEM = pl.BlockSpec(memory_space=pltpu.VMEM)
HBM = pl.BlockSpec(memory_space=pltpu.HBM)
ANY = pl.BlockSpec(memory_space=pl.ANY)


def in_vmem(x):
    return pltpu.with_memory_space_constraint(x, pltpu.VMEM)


def in_hbm(x):
    return pltpu.with_memory_space_constraint(x, pltpu.HBM)


def new_rows(c, im, ip, nb, klo, khi, d, f):
    km = jnp.concatenate([klo, c[:-1]], axis=0)
    kp = jnp.concatenate([c[1:], khi], axis=0)
    spread = (im + ip) + nb + (km + kp) - 6.0 * c
    return c + d * spread + f


def sweep(lo, hi, row, below, above, nb, klo, khi, d, f, put, carry=None):
    def block(first, bottom, top, carry):
        rows = [bottom() if bottom else row(first - 1)]
        rows += [row(first + r) for r in range(BLOCK)]
        rows += [top() if top else row(first + BLOCK)]
        for r in range(BLOCK):
            i = first + r
            new = new_rows(rows[r + 1], rows[r], rows[r + 2], nb(i), klo(i), khi(i), d(i), f(i))
            carry = put(i, new, carry)
        return carry

    carry = block(lo, below, None, carry)

    def body(b, carry):
        return block(lo + b * BLOCK, None, None, carry)

    n = (hi - lo) // BLOCK
    carry = lax.fori_loop(1, n - 1, body, carry)
    return block(hi - BLOCK, None, above, carry)


def plane_at(depth, n):
    low = lax.axis_index("lat") == 0
    return jnp.where(low, n - 1 - depth, depth)


def odd(axis):
    return lax.axis_index(axis) % 2 == 1


def lower(axis, e, o):
    return jnp.where(odd(axis), e, o)


def upper(axis, e, o):
    return jnp.where(odd(axis), o, e)


def faces_kernel(u, lon_e, lon_o, lev_e, lev_o):
    nj, ni, nk, _ = u.shape
    at_e = jnp.where(odd("lon"), 0, ni - 1)
    for j in range(nj):
        lon_e[j] = u[j, at_e]
        lon_o[j] = u[j, ni - 1 - at_e]
        lo, hi = u[j, :, 0, :], u[j, :, nk - 1, :]
        lev_e[j] = lower("lev", lo, hi)
        lev_o[j] = upper("lev", lo, hi)


def load_a_kernel(u_in, pa, sem):
    n = pa.shape[0]
    copy = pltpu.make_async_copy(u_in.at[plane_at(0, u_in.shape[0]), pl.ds(n // 2, n)], pa, sem)
    copy.start()
    copy.wait()


def load_kernel(u_in, d_in, f_in, u, pb, d_edge, f_edge, lon_e, lon_o, lev_e, lev_o, sem):
    nj, ni = u.shape[:2]
    q = ni // 4
    pj = plane_at(0, nj)
    copies = [pltpu.make_async_copy(u_in.at[j], u.at[j], sem.at[j]) for j in range(nj)]
    copies += [
        pltpu.make_async_copy(d_in.at[pj], d_edge, sem.at[nj]),
        pltpu.make_async_copy(f_in.at[pj], f_edge, sem.at[nj + 1]),
        pltpu.make_async_copy(u_in.at[pj, pl.ds(0, q)], pb.at[pl.ds(0, q)], sem.at[nj + 2]),
        pltpu.make_async_copy(u_in.at[pj, pl.ds(ni - q, q)], pb.at[pl.ds(q, q)], sem.at[nj + 3]),
    ]
    for copy in copies:
        copy.start()
    for copy in copies:
        copy.wait()
    faces_kernel(u, lon_e, lon_o, lev_e, lev_o)


def lev_rows(lev_e, lev_o, j, base):
    def get(side):
        def row(i):
            at = pl.ds(base + i, 1)
            return side("lev", lev_e[j, at, :], lev_o[j, at, :])

        return row

    return get(lower), get(upper)


def edge_rows(lo, hi, base, mine, below, above, u, lat, lev_e, lev_o, d, f, put):
    nj = u.shape[0]
    pj, pn = plane_at(0, nj), plane_at(1, nj)
    sweep(
        lo,
        hi,
        lambda i: mine[i],
        below,
        above,
        lambda i: u[pn, base + i] + lat[i],
        *lev_rows(lev_e, lev_o, pj, base),
        lambda i: d[base + i],
        lambda i: f[base + i],
        put,
        jnp.int32(0),
    )


def edge_a_kernel(u, pa, pb, lat, lev_e, lev_o, d, f, out):
    def put(i, new, carry):
        out[i] = new
        return carry

    n = pa.shape[0]
    edge_rows(0, n, n // 2, pa, lambda: pb[n // 2 - 1], lambda: pb[n // 2], u, lat, lev_e, lev_o, d, f, put)


def edge_b_kernel(u, pa, pb, lat, lon_e, lon_o, lev_e, lev_o, d, f, *rest):
    nj, ni, nk, _ = u.shape
    q = ni // 4
    pj = plane_at(0, nj)
    out = rest[2] if len(rest) > 1 else rest[0]

    def put(i, new, carry):
        out[i] = new
        return carry

    args = (u, lat, lev_e, lev_o, d, f, put)
    edge_rows(0, q, 0, pb, lambda: lower("lon", lon_e[pj], lon_o[pj]), lambda: pa[0], *args)
    edge_rows(q, 2 * q, 2 * q, pb, lambda: pa[2 * q - 1], lambda: upper("lon", lon_e[pj], lon_o[pj]), *args)
    if len(rest) > 1:
        nu, npa, _, s_lon_e, s_lon_o, s_lev_e, s_lev_o = rest
        faces_kernel(nu, s_lon_e, s_lon_o, s_lev_e, s_lev_o)
        s_lon_e[pj] = lower("lon", out[0], out[2 * q - 1])
        s_lon_o[pj] = upper("lon", out[0], out[2 * q - 1])
        for s_lev, side in ((s_lev_e, lower), (s_lev_o, upper)):
            s_lev[pj, :q] = side("lev", out[:q, 0, :], out[:q, nk - 1, :])
            s_lev[pj, q : 3 * q] = side("lev", npa[:, 0, :], npa[:, nk - 1, :])
            s_lev[pj, 3 * q :] = side("lev", out[q:, 0, :], out[q:, nk - 1, :])


def bulk_planes(u, pa, pb, lon_e, lon_o, lev_e, lev_o, d, f, put, start, finish):
    nj, ni, _, _ = u.shape
    q = ni // 4

    def run(j, lo, hi, nb, carry):
        return sweep(
            lo,
            hi,
            lambda i: u[j, i],
            (lambda: lower("lon", lon_e[j], lon_o[j])) if lo == 0 else None,
            (lambda: upper("lon", lon_e[j], lon_o[j])) if hi == ni else None,
            nb,
            *lev_rows(lev_e, lev_o, j, 0),
            lambda i: d[j, i],
            lambda i: f[j, i],
            functools.partial(put, j),
            carry,
        )

    j, inner = plane_at(1, nj), plane_at(2, nj)
    start(j, 1)
    carry = run(j, 0, q, lambda i: u[inner, i] + pb[i], zero_carry(u))
    carry = run(j, q, 3 * q, lambda i: u[inner, i] + pa[i - q], carry)
    carry = run(j, 3 * q, ni, lambda i: u[inner, i] + pb[i - 2 * q], carry)
    finish(j, 1, carry)

    def body(depth, _):
        j, outer, inner = plane_at(depth, nj), plane_at(depth - 1, nj), plane_at(depth + 1, nj)
        start(j, depth)
        carry = run(j, 0, ni, lambda i: u[outer, i] + u[inner, i], zero_carry(u))
        finish(j, depth, carry)
        return 0

    lax.fori_loop(2, nj - 1, body, 0)
    j, outer = plane_at(nj - 1, nj), plane_at(nj - 2, nj)
    start(j, nj - 1)
    carry = run(j, 0, ni, lambda i: u[outer, i], zero_carry(u))
    finish(j, nj - 1, carry)


def zero_carry(u):
    return jnp.zeros(u.shape[2:], u.dtype)


def nothing(*_):
    pass


def plain_put(out):
    def put(j, i, new, carry):
        out[j, i] = new
        return carry

    return put


def first_bulk_kernel(u, pa, pb, lon_e, lon_o, lev_e, lev_o, d_in, f_in, after, out, d, f, sem):
    del after
    nj = u.shape[0]

    def copies(j, depth):
        return (
            pltpu.make_async_copy(d_in.at[j], d.at[j], sem.at[0, depth]),
            pltpu.make_async_copy(f_in.at[j], f.at[j], sem.at[1, depth]),
        )

    for depth in range(1, nj):
        for copy in copies(plane_at(depth, nj), depth):
            copy.start()

    def start(j, depth):
        for copy in copies(j, depth):
            copy.wait()

    bulk_planes(u, pa, pb, lon_e, lon_o, lev_e, lev_o, d, f, plain_put(out), start, nothing)


def bulk_kernel(u, pa, pb, lon_e, lon_o, lev_e, lev_o, d, f, after, out):
    del after
    bulk_planes(u, pa, pb, lon_e, lon_o, lev_e, lev_o, d, f, plain_put(out), nothing, nothing)


def last_bulk_kernel(u, pa, pb, lon_e, lon_o, lev_e, lev_o, d_in, f_in, after, end, d, f, total, sem):
    del d_in, f_in, after
    nj = u.shape[0]

    def copy_out(j, depth):
        return pltpu.make_async_copy(f.at[j], end.at[j], sem.at[depth])

    def put(j, i, new, carry):
        f[j, i] = new
        carry = carry + new
        d[j, i] = carry
        return carry

    def finish(j, depth, carry):
        total[depth - 1] = carry

        @pl.when(depth < nj - LATE)
        def _():
            copy_out(j, depth).start()

    bulk_planes(u, pa, pb, lon_e, lon_o, lev_e, lev_o, d, f, put, nothing, finish)
    for depth in range(1, nj - LATE):
        copy_out(plane_at(depth, nj), depth).wait()


def late_kernel(f, npa, npb, end_in, end, sem):
    del end_in
    nj, ni = f.shape[:2]
    q = ni // 4
    pj = plane_at(0, nj)
    pairs = [(f.at[j], end.at[j]) for j in (plane_at(nj - LATE + p, nj) for p in range(LATE))]
    pairs += [
        (npb.at[pl.ds(0, q)], end.at[pj, pl.ds(0, q)]),
        (npa, end.at[pj, pl.ds(q, 2 * q)]),
        (npb.at[pl.ds(q, q)], end.at[pj, pl.ds(3 * q, q)]),
    ]
    copies = [pltpu.make_async_copy(source, target, sem.at[p]) for p, (source, target) in enumerate(pairs)]
    for copy in copies:
        copy.start()
    for copy in copies:
        copy.wait()


def last_edge_kernel(u, pa, pb, lat, lon_e, lon_o, lev_e, lev_o, d, f, npa, npb, sums, total):
    edge_b_kernel(u, pa, pb, lat, lon_e, lon_o, lev_e, lev_o, d, f, npb)
    ni = sums.shape[0]
    q = ni // 4
    carry = zero_carry(u)
    for part, lo, n, base in ((npb, 0, q, 0), (npa, 0, 2 * q, q), (npb, q, q, 3 * q)):

        def row(r, carry):
            carry = carry + part[lo + r]
            sums[base + r] = carry
            return carry

        carry = lax.fori_loop(0, n, row, carry, unroll=4)
    total[...] = carry


def earlier(others, first=0):
    lon = lax.axis_index("lon")
    before = 0.0
    for bit, other in enumerate(others):
        before += jnp.where(lon & (1 << (first + bit)) != 0, other, 0.0)
    return before


def half_kernel(total, other, out):
    n = out.shape[1]
    at = pl.ds(pl.multiple_of(jnp.where(odd("lon"), n, 0), n), n)
    for p in range(out.shape[0]):
        out[p] = total[p, at] + other[p, at]


def before_kernel(*refs):
    *others, out = refs
    for p in range(out.shape[0]):
        out[p] = earlier([other[p] for other in others], 1)


def total_rows(scale, ni, sums, before, put):
    def row(r, _):
        for q in range(BLOCK):
            i = r * BLOCK + q
            put(i, (sums(i) + before) * scale)
        return 0

    lax.fori_loop(0, ni // BLOCK, row, 0)


def half_totals(scale, upper_half, sums, other, before, out, stage, sem):
    nj, ni, nk = sums.shape[:3]
    n = nk // 2
    at = pl.ds(pl.multiple_of(jnp.where(upper_half, n, 0), n), n)

    def copy_out(depth):
        return pltpu.make_async_copy(stage.at[depth - 1], out.at[plane_at(depth, nj), :, at, :], sem.at[depth - 1])

    def body(depth, _):
        j = plane_at(depth, nj)
        b = before[depth - 1] + earlier([other[depth - 1, at]])

        def put(i, value):
            stage[depth - 1, i] = value

        total_rows(scale, ni, lambda i: sums[j, i, at], b, put)
        copy_out(depth).start()
        return 0

    lax.fori_loop(1, nj, body, 0)
    return [copy_out(depth) for depth in range(1, nj)]


def totals_kernel(scale, sums, other, before, after, out, stage, sem):
    del after
    for copy in half_totals(scale, odd("lon"), sums, other, before, out, stage, sem):
        copy.wait()


def last_totals_kernel(scale, sums, other, before, edge_sums, *rest):
    *others, _, out, stage, edge_stage, sem, edge_sem = rest
    nj, ni = sums.shape[:2]
    pj = plane_at(0, nj)

    def put(i, value):
        edge_stage[i] = value

    total_rows(scale, ni, lambda i: edge_sums[i], earlier([other[...] for other in others]), put)
    copies = [pltpu.make_async_copy(edge_stage, out.at[pj], edge_sem)]
    copies[0].start()
    copies += half_totals(scale, jnp.logical_not(odd("lon")), sums, other, before, out, stage, sem)
    for copy in copies:
        copy.wait()


def call(kernel, out_shape, out_specs, in_specs, limit=2, scratch=(), aliases=None, flops=0):
    return pl.pallas_call(
        kernel,
        out_shape=out_shape,
        in_specs=in_specs,
        out_specs=out_specs,
        scratch_shapes=scratch,
        input_output_aliases=aliases or {},
        compiler_params=pltpu.CompilerParams(vmem_limit_bytes=limit * 2**20),
        cost_estimate=pl.CostEstimate(flops=flops, transcendentals=0, bytes_accessed=0),
    )


def per_device(lon_size, lev_size, initial_state, scaled_diffusivity, scaled_forcing):
    dtype = initial_state.dtype
    nj, ni, nk, nm = initial_state.shape
    half = ni // 2
    V = lambda *shape: pltpu.VMEM(shape, dtype)
    H = lambda *shape: pltpu.HBM(shape, dtype)

    swap = [(0, 1), (1, 0)]
    faces_out = (V(nj, nk, nm), V(nj, nk, nm), V(nj, ni, nm), V(nj, ni, nm))

    def exchange(axis, size, e, o):
        def swaps(first):
            return [(a, b) for i in range(first, size - 1, 2) for a, b in ((i, i + 1), (i + 1, i))]

        return lax.ppermute(e, axis, swaps(0)), lax.ppermute(o, axis, swaps(1))

    def lon_exchange(e, o, relay):
        if not relay:
            return exchange("lon", lon_size, e, o)
        relayed = lax.ppermute(o, "lon", [(3, 7), (4, 0)])
        e, o = (lax.ppermute(x, "lon", [p for i in a for p in ((i, i + 1), (i + 1, i))]) for x, a in ((e, (0, 2, 4, 6)), (o, (1, 5))))
        return e, o + lax.ppermute(relayed, "lon", [(7, 4), (0, 3)])

    def lev_exchange(e, o):
        return exchange("lev", lev_size, e, o)

    def partner(bit, total):
        pairs = [(i, i ^ (1 << bit)) for i in range(lon_size)]
        if 2 << bit == lon_size:
            pairs = [(a, b) for a, b in pairs if a < b]
        return lax.ppermute(total, "lon", pairs)

    bits = lon_size.bit_length() - 1

    pa = call(
        load_a_kernel, V(half, nk, nm), VMEM, (HBM,), scratch=(pltpu.SemaphoreType.DMA,), flops=10**5
    )(in_hbm(initial_state))
    lat_a = lax.ppermute(pa, "lat", swap)
    u, pb, d_edge, f_edge, *faces = call(
        load_kernel,
        (V(nj, ni, nk, nm), V(half, nk, nm), V(ni, nk, nm), V(ni, nk, nm)) + faces_out,
        (VMEM,) * 8,
        (HBM,) * 3,
        scratch=(pltpu.SemaphoreType.DMA((nj + 4,)),),
        flops=10**6,
    )(*map(in_hbm, (initial_state, scaled_diffusivity, scaled_forcing)))
    lon = lon_exchange(*faces[:2], True)
    lat_b = lax.ppermute(pb, "lat", swap)
    lev = lev_exchange(*faces[2:])
    d_edge, f_edge = in_vmem(d_edge), in_vmem(f_edge)
    d, f = in_hbm(scaled_diffusivity), in_hbm(scaled_forcing)

    for step in range(STEPS):
        last = step == STEPS - 1
        u, pa, pb, lat_a, lat_b = map(in_vmem, (u, pa, pb, lat_a, lat_b))
        lon, lev = tuple(map(in_vmem, lon)), tuple(map(in_vmem, lev))
        n_pa = call(edge_a_kernel, V(half, nk, nm), VMEM, (VMEM,) * 8, flops=10**6)(
            u, pa, pb, lat_a, *lev, d_edge, f_edge
        )
        if last:
            break
        lat_a = lax.ppermute(n_pa, "lat", swap)
        if step == 0:
            n_u, d, f = call(
                first_bulk_kernel,
                (V(nj, ni, nk, nm),) * 3,
                (VMEM,) * 3,
                (VMEM,) * 7 + (HBM,) * 2 + (ANY,),
                scratch=(pltpu.SemaphoreType.DMA((2, nj)),),
                flops=2 * 10**7,
            )(u, pa, pb, *lon, *lev, d, f, n_pa)
        else:
            n_u = call(
                bulk_kernel, V(nj, ni, nk, nm), VMEM, (VMEM,) * 9 + (ANY,), flops=2 * 10**7
            )(u, pa, pb, *lon, *lev, in_vmem(d), in_vmem(f), n_pa)
        n_pb, *faces = call(
            edge_b_kernel, (V(half, nk, nm),) + faces_out, (VMEM,) * 5, (VMEM,) * 12, flops=10**6
        )(u, pa, pb, lat_b, *lon, *lev, d_edge, f_edge, in_vmem(n_u), in_vmem(n_pa))
        lon = lon_exchange(*faces[:2], step % 2 == 1)
        lat_b = lax.ppermute(n_pb, "lat", swap)
        lev = lev_exchange(*faces[2:])
        u, pa, pb = n_u, n_pa, n_pb

    scale = 1.0 / (ni * lon_size)
    end, sums, values, total = call(
        last_bulk_kernel,
        (H(nj, ni, nk, nm), V(nj, ni, nk, nm), V(nj, ni, nk, nm), V(nj - 1, nk, nm)),
        (HBM, VMEM, VMEM, VMEM),
        (VMEM,) * 9 + (ANY,),
        scratch=(pltpu.SemaphoreType.DMA((nj,)),),
        aliases={7: 1, 8: 2},
        flops=2 * 10**7,
    )(u, pa, pb, *lon, *lev, in_vmem(d), in_vmem(f), n_pa)
    other = partner(0, total)
    half_total = call(half_kernel, V(nj - 1, nk // 2, nm), VMEM, (VMEM,) * 2, flops=10**5)(
        in_vmem(total), in_vmem(other)
    )
    later = []
    for bit in range(1, bits):
        later.append(partner(bit, half_total))
        half_total = half_total + later[-1]
    mine = call(before_kernel, V(nj - 1, nk // 2, nm), VMEM, (VMEM,) * (bits - 1), flops=10**5)(*map(in_vmem, later))
    back = lax.ppermute(mine, "lon", [(i, i ^ 1) for i in range(lon_size)])
    n_pa = in_vmem(n_pa)
    n_pb, edge_sums, edge_total = call(
        last_edge_kernel, (V(half, nk, nm), V(ni, nk, nm), V(nk, nm)), (VMEM,) * 3, (VMEM,) * 11, flops=2 * 10**6
    )(u, pa, pb, lat_b, *lon, *lev, d_edge, f_edge, n_pa)
    others = []
    edge_total_1 = edge_total
    for bit in range(bits):
        others.append(partner(bit, edge_total))
        edge_total = edge_total + others[-1]
    others = tuple(map(in_vmem, others))
    n_pb = in_vmem(n_pb)
    end = call(
        late_kernel,
        H(nj, ni, nk, nm),
        HBM,
        (VMEM,) * 3 + (HBM,),
        scratch=(pltpu.SemaphoreType.DMA((LATE + 3,)),),
        aliases={3: 0},
        flops=10**5,
    )(in_vmem(values), n_pa, n_pb, in_hbm(end))
    sums, other = in_vmem(sums), in_vmem(other)
    out = call(
        functools.partial(totals_kernel, scale),
        H(nj, ni, nk, nm),
        HBM,
        (VMEM,) * 3 + (ANY,),
        limit=5,
        scratch=(V(nj - 1, ni, nk // 2, nm), pltpu.SemaphoreType.DMA((nj - 1,))),
        flops=10**6,
    )(sums, other, in_vmem(mine), edge_total_1)
    n = 4 + bits
    out = call(
        functools.partial(last_totals_kernel, scale),
        H(nj, ni, nk, nm),
        HBM,
        (VMEM,) * n + (HBM,),
        scratch=(
            V(nj - 1, ni, nk // 2, nm),
            V(ni, nk, nm),
            pltpu.SemaphoreType.DMA((nj - 1,)),
            pltpu.SemaphoreType.DMA,
        ),
        limit=6,
        aliases={n: 0},
        flops=10**6,
    )(sums, other, in_vmem(back), in_vmem(edge_sums), *others, in_hbm(out))
    return out, end


def solution(mesh):
    spec = P("lat", "lon", "lev", None)
    return jax.shard_map(
        functools.partial(per_device, mesh.shape["lon"], mesh.shape["lev"]),
        mesh=mesh,
        in_specs=(spec, spec, spec),
        out_specs=(spec, spec),
        check_vma=False,
    )
```
